32 devices in a mesh: dp: 2 (over x), cp: 4 (over z), tp: 4 (over y, core).
Axes of the slice: x: 2, y: 2, z: 4, core: 2. Of those that a mesh axis runs over, the one named last changes fastest.
Arguments:
- x: bfloat16 [8192, 3584], P(('dp', 'cp', 'tp')), parts along dimension 0
- idx: int32 [8192, 2], P(('dp', 'cp', 'tp')), parts along dimension 0
- gates: float32 [8192, 2], P(('dp', 'cp', 'tp')), parts along dimension 0
- wq: bfloat16 [3584, 3584], P(None, 'tp')
- wk: bfloat16 [3584, 512], P(None, 'tp')
- wv: bfloat16 [3584, 512], P(None, 'tp')
- wo: bfloat16 [3584, 3584], P('tp')
- w1g: bfloat16 [16, 3584, 2560], P(('cp', 'tp'))
- w1u: bfloat16 [16, 3584, 2560], P(('cp', 'tp'))
- w2: bfloat16 [16, 2560, 3584], P(('cp', 'tp'))
Outputs:
- output: bfloat16 [8192, 3584], P(('dp', 'cp', 'tp')), parts along dimension 0
There are 2 independent parts. The reference program is written for one: setup_inputs(seed, part) draws one part's arguments, and reference() takes and returns one part's arrays. A program takes and returns all parts, laid end to end along the dimension named above; an argument that names none is the same for every part.
All inputs are finite; a program needn't handle non-finite values.
Results may differ from the reference program's by a relative error of at most 0.0100627.
Values are sent between devices in bfloat16 or wider.
A program may use at most 1 GiB of HBM per device.

```python
import math
import jax
import jax.numpy as jnp
from jax import lax

H = 3584
FF = 2560
HEADS = 28
KV_HEADS = 4
HEAD = 128
S = 4096
CP = 4
TP = 4
TOP = 2
QBLK = 512

E = CP * TP
T = S // E
CAP = 4 * T // E
M = 2 * T // E


def seg_positions():
    i = jnp.arange(S, dtype=jnp.int32)
    seg = S // (2 * CP)
    b = i // seg
    r = b // 2
    s_id = jnp.where(b % 2 == 0, r, 2 * CP - 1 - r)
    return s_id * seg + i % seg


def source_routing(key, sigma, counts):
    ends = jnp.cumsum(counts)
    labels = sigma[jnp.searchsorted(ends, jnp.arange(2 * T, dtype=jnp.int32), side='right')]
    perm = jax.random.permutation(key, T)
    return jnp.stack([labels[perm], labels[perm + T]], axis=1).astype(jnp.int32)


def setup_inputs(seed: int = 0, part: int = 0) -> dict:
    key = jax.random.key(seed)
    ks = jax.random.split(key, 7)
    kx = jax.random.split(jax.random.fold_in(key, part), 4)
    a = math.log(S / 16.0) ** 0.25

    def nrm(k, shape, scale):
        return (jax.random.normal(k, shape, jnp.float32) * scale).astype(jnp.bfloat16)

    wq = nrm(ks[0], (H, HEADS * HEAD), a / math.sqrt(H))
    wk = nrm(ks[1], (H, KV_HEADS * HEAD), a / math.sqrt(H))
    wv = nrm(ks[2], (H, KV_HEADS * HEAD), 1.0 / math.sqrt(H))
    wo = nrm(ks[3], (HEADS * HEAD, H), 1.0 / math.sqrt(HEADS * HEAD))
    w1g = nrm(ks[4], (E, H, FF), 1.0 / math.sqrt(H))
    w1u = nrm(ks[5], (E, H, FF), 1.0 / math.sqrt(H))
    w2 = nrm(ks[6], (E, FF, H), 1.5 / math.sqrt(FF))
    x = nrm(kx[0], (S, H), 1.0)
    sigmas = jax.vmap(lambda kk: jax.random.permutation(kk, E))(jax.random.split(kx[1], E))
    counts = jnp.full((E,), M, jnp.int32)
    idx = jax.vmap(lambda kk, sg: source_routing(kk, sg, counts))(jax.random.split(kx[2], E), sigmas)
    idx = idx.reshape(S, TOP)
    gates = jax.random.uniform(kx[3], (S, TOP), jnp.float32, 0.3, 0.7)
    return {'x': x, 'idx': idx, 'gates': gates, 'wq': wq, 'wk': wk, 'wv': wv, 'wo': wo, 'w1g': w1g, 'w1u': w1u, 'w2': w2}


def reference(x, idx, gates, wq, wk, wv, wo, w1g, w1u, w2):
    pos = seg_positions()
    g = HEADS // KV_HEADS
    q = jnp.dot(x, wq, preferred_element_type=jnp.float32).astype(jnp.bfloat16)
    k = jnp.dot(x, wk, preferred_element_type=jnp.float32).astype(jnp.bfloat16)
    v = jnp.dot(x, wv, preferred_element_type=jnp.float32).astype(jnp.bfloat16)
    qh = q.reshape(S, HEADS, HEAD).transpose(1, 0, 2)
    kh = jnp.repeat(k.reshape(S, KV_HEADS, HEAD).transpose(1, 0, 2), g, axis=0)
    vh = jnp.repeat(v.reshape(S, KV_HEADS, HEAD).transpose(1, 0, 2), g, axis=0)
    scale = HEAD ** -0.5
    nb = S // QBLK

    def head(args):
        qa, ka, va = args

        def block(bargs):
            qb, pb = bargs
            s = jnp.dot(qb, ka.T, preferred_element_type=jnp.float32) * scale
            mask = pos[None, :] <= pb[:, None]
            s = jnp.where(mask, s, -1e30)
            m = jnp.max(s, axis=-1, keepdims=True)
            w = jnp.where(mask, jnp.exp(s - m), 0.0)
            l = jnp.sum(w, axis=-1, keepdims=True)
            ob = jnp.dot(w.astype(jnp.bfloat16), va, preferred_element_type=jnp.float32)
            return ob / l

        out = lax.map(block, (qa.reshape(nb, QBLK, HEAD), pos.reshape(nb, QBLK)))
        return out.reshape(S, HEAD)

    o = lax.map(head, (qh, kh, vh))
    o = o.transpose(1, 0, 2).reshape(S, HEADS * HEAD).astype(jnp.bfloat16)
    att = jnp.dot(o, wo, preferred_element_type=jnp.float32)
    h = (x.astype(jnp.float32) + att).astype(jnp.bfloat16)

    ea = idx.reshape(-1)
    tok = jnp.arange(S * TOP) // TOP
    onehot = (ea[:, None] == jnp.arange(E)[None, :]).astype(jnp.int32)
    slot = jnp.take_along_axis(jnp.cumsum(onehot, axis=0), ea[:, None], axis=1)[:, 0] - 1
    ct = E * CAP
    buf = jnp.zeros((E, ct, H), jnp.bfloat16).at[ea, slot].set(h[tok])

    def expert(args):
        rows, wg, wu, wd = args
        gg = jnp.dot(rows, wg, preferred_element_type=jnp.float32)
        uu = jnp.dot(rows, wu, preferred_element_type=jnp.float32)
        act = (jax.nn.silu(gg) * uu).astype(jnp.bfloat16)
        return jnp.dot(act, wd, preferred_element_type=jnp.float32).astype(jnp.bfloat16)

    z = lax.map(expert, (buf, w1g, w1u, w2))
    zt = z[ea, slot].astype(jnp.float32).reshape(S, TOP, H)
    y = h.astype(jnp.float32) + jnp.sum(gates[:, :, None] * zt, axis=1)
    return y.astype(jnp.bfloat16)
```

```python
import functools

import jax
import jax.numpy as jnp
from jax import lax
from jax.experimental import pallas as pl
from jax.experimental.pallas import tpu as pltpu
from jax.sharding import PartitionSpec as P

HD = 128
NEG = -1e30
BF = jnp.bfloat16
F32 = jnp.float32
MESH = pl.DeviceIdType.MESH
VMEM_LIMIT = 67_000_000
CH = 16


def dot(a, b):
    return jnp.dot(a, b, preferred_element_type=F32)


def flash_kernel(q_ref, k_ref, v_ref, o_ref, vt_ref, *, seg, ncp, scale):
    c = lax.axis_index("cp")
    last = 2 * ncp - 1

    @pl.when(pl.program_id(0) == 0)
    def _():
        for b in range(2 * ncp):
            vt_ref[:, b * seg:(b + 1) * seg] = v_ref[b * seg:(b + 1) * seg, :].T

    def place(g):
        r = jnp.minimum(g, last - g)
        return pl.multiple_of((2 * r + jnp.where(g == r, 0, 1)) * seg, seg)

    def step(g, carry, qb, masked):
        m, l, acc = carry
        at = place(g)
        s = lax.dot_general(k_ref[pl.ds(at, seg), :], qb, (((1,), (1,)), ((), ())), preferred_element_type=F32) * scale
        if masked:
            ki = lax.broadcasted_iota(jnp.int32, s.shape, 0)
            qi = lax.broadcasted_iota(jnp.int32, s.shape, 1)
            s = jnp.where(ki <= qi, s, NEG)
        mn = jnp.maximum(m, jnp.max(s, axis=0, keepdims=True))
        w = jnp.exp(s - mn)
        a = jnp.exp(m - mn)
        l = l * a + jnp.sum(w, axis=0, keepdims=True)
        acc = acc * a + dot(vt_ref[:, pl.ds(at, seg)], w.astype(BF))
        return mn, l, acc

    for half in range(2):
        mine = c if half == 0 else last - c
        qb = q_ref[half * seg:(half + 1) * seg, :]
        carry = (jnp.full((1, seg), NEG, F32), jnp.zeros((1, seg), F32), jnp.zeros((HD, seg), F32))
        carry = lax.fori_loop(0, mine, lambda g, cr: step(g, cr, qb, False), carry)
        m, l, acc = step(mine, carry, qb, True)
        o_ref[half * seg:(half + 1) * seg, :] = (acc / l).T.astype(BF)


def flash(q, k, v, ncp):
    n, d = q.shape
    heads = d // HD
    kern = functools.partial(flash_kernel, seg=n // 2, ncp=ncp, scale=HD ** -0.5)
    full = pl.BlockSpec(k.shape, lambda h: (0, 0))
    return pl.pallas_call(
        kern,
        grid=(heads,),
        in_specs=[pl.BlockSpec((n, HD), lambda h: (0, h)), full, full],
        out_specs=pl.BlockSpec((n, HD), lambda h: (0, h)),
        out_shape=jax.ShapeDtypeStruct((n, d), BF),
        scratch_shapes=[pltpu.VMEM((HD, k.shape[0]), BF)],
        compiler_params=pltpu.CompilerParams(vmem_limit_bytes=VMEM_LIMIT, dimension_semantics=("arbitrary",)),
        name="flash",
        cost_estimate=pl.CostEstimate(flops=heads * n * k.shape[0] * HD * 2, bytes_accessed=4 * n * d, transcendentals=heads * n * k.shape[0] // 2),
    )(q, k, v)


def moe_kernel(h_ref, dr_ref, dc_ref, g_ref, wg_hbm, wu_hbm, wd_hbm, y_ref,
               send, recv, zbuf, back, act, w1buf, w2buf,
               ssem, rsem, zsem, bsem, w1sem, w2sem, *, ncp, ntp, nch, f1, f2):
    ne = ncp * ntp
    rows = ne * CH
    t, hd = h_ref.shape
    ff = wg_hbm.shape[1]
    n1, n2 = ff // f1, hd // f2
    r1, r2 = w1buf.shape[0], w2buf.shape[0]
    dp = lax.axis_index("dp")
    c = lax.axis_index("cp")
    p = lax.axis_index("tp")
    me = c * ntp + p

    order = [2, 1, 3, 0]
    peers = [(dc, dt) for dc in order[:ncp] for dt in range(ntp) if (dc, dt) != (0, 0)]

    def peer(dc, dt):
        pc = lax.rem(c + dc, ncp)
        pt = lax.rem(p + dt, ntp)
        return pc, pt, pc * ntp + pt

    def blk(e):
        return pl.ds(pl.multiple_of(e * CH, CH), CH)

    def out_copy(j, dc, dt):
        pc, pt, e = peer(dc, dt)
        return pltpu.make_async_remote_copy(send.at[j, blk(e)], recv.at[j, blk(me)], ssem.at[j, e], rsem.at[j, me],
                                            device_id=(dp, pc, pt), device_id_type=MESH)

    def in_copy(j, dc, dt):
        pc, pt, e = peer(dc, dt)
        return pltpu.make_async_remote_copy(send.at[j, blk(e)], recv.at[j, blk(e)], ssem.at[j, e], rsem.at[j, e],
                                            device_id=(dp, pc, pt), device_id_type=MESH)

    def home_copy(j, dc, dt):
        pc, pt, e = peer(dc, dt)
        return pltpu.make_async_remote_copy(zbuf.at[j, blk(e)], back.at[j, blk(me)], zsem.at[j, e], bsem.at[j, me],
                                            device_id=(dp, pc, pt), device_id_type=MESH)

    def got_copy(j, dc, dt):
        pc, pt, e = peer(dc, dt)
        return pltpu.make_async_remote_copy(zbuf.at[j, blk(e)], back.at[j, blk(e)], zsem.at[j, e], bsem.at[j, e],
                                            device_id=(dp, pc, pt), device_id_type=MESH)

    def w1_copies(s):
        slot = lax.rem(s, r1)
        cols = pl.ds(pl.multiple_of(s * f1, f1), f1)
        return (pltpu.make_async_copy(wg_hbm.at[:, cols], w1buf.at[slot, 0], w1sem.at[slot, 0]),
                pltpu.make_async_copy(wu_hbm.at[:, cols], w1buf.at[slot, 1], w1sem.at[slot, 1]))

    def w2_copy(s):
        slot = lax.rem(s, r2)
        cols = pl.ds(pl.multiple_of(s * f2, f2), f2)
        return pltpu.make_async_copy(wd_hbm.at[:, cols], w2buf.at[slot], w2sem.at[slot])

    def start_w1(s):
        for cp_ in w1_copies(s):
            cp_.start()

    def prefetch_w1():
        for s in range(r1):
            start_w1(jnp.int32(s))

    def prefetch_w2():
        for s in range(r2):
            w2_copy(jnp.int32(s)).start()

    prefetch_w1()
    prefetch_w2()

    barrier = pltpu.get_barrier_semaphore()
    for dc, dt in peers:
        pc, pt, _ = peer(dc, dt)
        pl.semaphore_signal(barrier, inc=1, device_id=(dp, pc, pt), device_id_type=MESH)
    pl.semaphore_wait(barrier, ne - 1)

    for j in range(nch):
        ri = lax.broadcasted_iota(jnp.int32, (rows, t), 0) + j * rows
        sel = jnp.where(ri == dr_ref[0:1, :], 1.0, 0.0) + jnp.where(ri == dr_ref[1:2, :], 1.0, 0.0)
        sel = sel.astype(BF)

        def pick(i, _):
            cols = pl.ds(pl.multiple_of(i * 512, 512), 512)
            send[j, :, cols] = dot(sel, h_ref[:, cols]).astype(BF)
            return 0

        lax.fori_loop(0, hd // 512, pick, 0)
        for dc, dt in peers:
            out_copy(j, dc, dt).start()
        recv[j, blk(me), :] = send[j, blk(me), :]

    for j in range(nch):
        for dc, dt in peers:
            in_copy(j, dc, dt).wait_recv()

        def up(s, _):
            slot = lax.rem(s, r1)
            for cp_ in w1_copies(s):
                cp_.wait()
            xx = recv[j]
            gg = dot(xx, w1buf[slot, 0])
            uu = dot(xx, w1buf[slot, 1])
            act[:, pl.ds(pl.multiple_of(s * f1, f1), f1)] = (gg * jax.nn.sigmoid(gg) * uu).astype(BF)

            @pl.when(s + r1 < n1)
            def _():
                start_w1(s + r1)
            return 0

        lax.fori_loop(0, n1, up, 0)
        if j + 1 < nch:
            prefetch_w1()

        def down(s, _):
            slot = lax.rem(s, r2)
            w2_copy(s).wait()
            zbuf[j, :, pl.ds(pl.multiple_of(s * f2, f2), f2)] = dot(act[...], w2buf[slot]).astype(BF)

            @pl.when(s + r2 < n2)
            def _():
                w2_copy(s + r2).start()
            return 0

        lax.fori_loop(0, n2, down, 0)
        if j + 1 < nch:
            prefetch_w2()
        for dc, dt in peers:
            home_copy(j, dc, dt).start()
        back[j, blk(me), :] = zbuf[j, blk(me), :]

    for j in range(nch):
        for dc, dt in peers:
            got_copy(j, dc, dt).wait_recv()

    ci = lax.broadcasted_iota(jnp.int32, (t, rows), 1)
    sel0 = [jnp.where(ci + j * rows == dc_ref[:, 0:1], 1.0, 0.0).astype(BF) for j in range(nch)]
    sel1 = [jnp.where(ci + j * rows == dc_ref[:, 1:2], 1.0, 0.0).astype(BF) for j in range(nch)]
    g0 = g_ref[:, 0:1]
    g1 = g_ref[:, 1:2]

    def combine(i, _):
        cols = pl.ds(pl.multiple_of(i * 512, 512), 512)
        z0 = sum(dot(sel0[j], back[j, :, cols]) for j in range(nch))
        z1 = sum(dot(sel1[j], back[j, :, cols]) for j in range(nch))
        y_ref[:, cols] = (h_ref[:, cols].astype(F32) + (g0 * z0 + g1 * z1)).astype(BF)
        return 0

    lax.fori_loop(0, hd // 512, combine, 0)

    for j in range(nch):
        for dc, dt in peers:
            out_copy(j, dc, dt).wait_send()
            home_copy(j, dc, dt).wait_send()


def moe(h, drow, dcol, gates, wg, wu, wd, *, ncp, ntp, nch, cid):
    t, hd = h.shape
    ff = wg.shape[1]
    ne = ncp * ntp
    rows = ne * CH
    f1, f2, r1, r2 = 256, 512, 2, 2
    vm = pl.BlockSpec(memory_space=pltpu.VMEM)
    hbm = pl.BlockSpec(memory_space=pl.ANY)
    dma = pltpu.SemaphoreType.DMA
    return pl.pallas_call(
        functools.partial(moe_kernel, ncp=ncp, ntp=ntp, nch=nch, f1=f1, f2=f2),
        in_specs=[vm, vm, vm, vm, hbm, hbm, hbm],
        out_specs=vm,
        out_shape=jax.ShapeDtypeStruct((t, hd), BF),
        scratch_shapes=[
            pltpu.VMEM((nch, rows, hd), BF), pltpu.VMEM((nch, rows, hd), BF),
            pltpu.VMEM((nch, rows, hd), BF), pltpu.VMEM((nch, rows, hd), BF),
            pltpu.VMEM((rows, ff), BF),
            pltpu.VMEM((r1, 2, hd, f1), BF), pltpu.VMEM((r2, ff, f2), BF),
            dma((nch, ne)), dma((nch, ne)), dma((nch, ne)), dma((nch, ne)),
            dma((r1, 2)), dma((r2,)),
        ],
        compiler_params=pltpu.CompilerParams(collective_id=cid, has_side_effects=True, vmem_limit_bytes=VMEM_LIMIT),
        name=f"moe{nch}",
        cost_estimate=pl.CostEstimate(flops=6 * nch * rows * hd * ff, bytes_accessed=6 * nch * hd * ff, transcendentals=0),
    )(h, drow, dcol, gates, wg, wu, wd)


def route(idx, ne):
    t = idx.shape[0]
    e = jnp.arange(ne, dtype=jnp.int32)[None, :]
    oh0 = (idx[:, 0:1] == e).astype(F32)
    oh1 = (idx[:, 1:2] == e).astype(F32)
    both = oh0 + oh1
    i = jnp.arange(t)
    before = dot((i[None, :] < i[:, None]).astype(F32), both)
    s0 = jnp.sum(before * oh0, axis=1).astype(jnp.int32)
    s1 = jnp.sum(before * oh1, axis=1).astype(jnp.int32)
    slot = jnp.stack([s0, s1], axis=1)
    code = (slot // CH) * (ne * CH) + idx * CH + slot % CH
    return code, jnp.max(jnp.sum(both, axis=0)).astype(jnp.int32)


def solution(mesh):
    ncp = mesh.shape["cp"]
    ntp = mesh.shape["tp"]
    ne = ncp * ntp
    rows_spec = P(("dp", "cp", "tp"), None)
    exp_spec = P(("cp", "tp"), None, None)

    def local(x, idx, gates, wq, wk, wv, wo, w1g, w1u, w2):
        code, most = route(idx, ne)
        most = lax.pmax(most, ("dp", "cp", "tp"))
        drow = jnp.pad(code.T, ((0, 6), (0, 0)))
        xs = lax.all_gather(x, "tp", axis=0, tiled=True)
        q = dot(xs, wq).astype(BF)
        kv = dot(xs, jnp.concatenate([wk, wv], axis=1)).astype(BF)
        kvs = lax.all_gather(kv, "cp", axis=0, tiled=True)
        o = flash(q, kvs[:, :HD], kvs[:, HD:], ncp)
        part = dot(o, wo)
        att = lax.psum_scatter(part, "tp", scatter_dimension=0, tiled=True)
        h = (x.astype(F32) + att).astype(BF)

        def few(args):
            return moe(*args, ncp=ncp, ntp=ntp, nch=2, cid=1)

        def many(args):
            return moe(*args, ncp=ncp, ntp=ntp, nch=4, cid=2)

        return lax.cond(most <= 2 * CH, few, many, (h, drow, code, gates, w1g[0], w1u[0], w2[0]))

    return jax.shard_map(local, mesh=mesh, in_specs=(rows_spec, rows_spec, rows_spec, P(None, "tp"), P(None, "tp"), P(None, "tp"), P("tp", None), exp_spec, exp_spec, exp_spec), out_specs=rows_spec, check_vma=False)
```

```python
import functools

import jax
import jax.numpy as jnp
from jax import lax
from jax.experimental import pallas as pl
from jax.experimental.pallas import tpu as pltpu
from jax.sharding import PartitionSpec as P

HD = 128
NEG = -1e30
BF = jnp.bfloat16
F32 = jnp.float32
MESH = pl.DeviceIdType.MESH
VMEM_LIMIT = 67_000_000
CH = 16


def dot(a, b):
    return jnp.dot(a, b, preferred_element_type=F32)


def att_kernel(x_hbm, wq_hbm, wk_hbm, wv_hbm, wo_hbm, most_ref, h_ref, mx_ref,
               xs, wq, wkv, wo_a, wo_b, q_a, q_b, kb, vt, o_a, o_s, o_b, part, pin, cnt,
               lsem, cx_s, cx_r, yx_s, yx_r, fx_s, fx_r, kv_s, kv_r, wy_s, wy_r, wx_s, wx_r,
               wu_s, wu_r, wd_s, wd_r, o_ss, o_rs, p_ss, p_rs, n_s, n_r, *, nd, ncp, ntp, scale):
    d = lax.axis_index("dp")
    c = lax.axis_index("cp")
    t = lax.axis_index("tp")
    y = t // 2
    k = lax.rem(t, 2)
    t_c = 2 * y + 1 - k
    t_y = 2 * (1 - y) + k
    t_z = 2 * (1 - y) + 1 - k
    rb = xs.shape[1]
    hd = xs.shape[2]
    seg = 2 * rb
    hk = rb // 2
    heads = q_a.shape[1] // HD
    pr = wo_a.shape[0] // (nd * ncp)
    last = 2 * ncp - 1
    mine = jnp.where(y == 0, c, last - c)
    other = last - mine
    me = (d * ncp + c) * ntp + t

    def rcopy(src, dst, ss, rs, dd, cc, tt):
        return pltpu.make_async_remote_copy(src, dst, ss, rs, device_id=(dd, cc, tt), device_id_type=MESH)

    loads = [
        pltpu.make_async_copy(wk_hbm, wkv.at[:, 0:HD], lsem.at[0]),
        pltpu.make_async_copy(wv_hbm, wkv.at[:, HD:2 * HD], lsem.at[1]),
        pltpu.make_async_copy(x_hbm, xs.at[t], lsem.at[2]),
        pltpu.make_async_copy(wq_hbm, wq, lsem.at[3]),
        pltpu.make_async_copy(wo_hbm, wo_a, lsem.at[4]),
    ]
    for cp_ in loads:
        cp_.start()

    n_all = nd * ncp * ntp
    others = [(a, b, e) for a in range(nd) for b in range(ncp) for e in range(ntp) if (a, b, e) != (0, 0, 0)]

    def rel(a, b, e):
        return lax.rem(d + a, nd), lax.rem(c + b, ncp), lax.rem(t + e, ntp)

    barrier = pltpu.get_barrier_semaphore()
    for o in others:
        pl.semaphore_signal(barrier, inc=1, device_id=rel(*o), device_id_type=MESH)
    pl.semaphore_wait(barrier, n_all - 1)

    def piece(dd, cc):
        return pl.ds(pl.multiple_of((dd * ncp + cc) * pr, pr), pr)

    def half(i):
        return pl.ds(i * hk, hk)

    wy = rcopy(wo_hbm.at[piece(d, c)], wo_b.at[piece(d, c)], wy_s, wy_r, d, c, t_y)
    wy.start()
    yx = [rcopy(x_hbm.at[half(i)], xs.at[t, half(i)], yx_s.at[i], yx_r.at[i], d, c, t_y) for i in range(2)]
    yx_in = [rcopy(x_hbm.at[half(i)], xs.at[t_y, half(i)], yx_s.at[i], yx_r.at[i], d, c, t_y) for i in range(2)]
    for cp_ in yx:
        cp_.start()
    cx = rcopy(x_hbm, xs.at[t], cx_s, cx_r, d, c, t_c)
    cx_in = rcopy(x_hbm, xs.at[t_c], cx_s, cx_r, d, c, t_c)
    cx.start()
    cnt[me] = most_ref[...]
    for i, o in enumerate(others):
        dd, cc, tt = rel(*o)
        rcopy(most_ref, cnt.at[me], n_s.at[i], n_r.at[me], dd, cc, tt).start()

    zpeers = list(range(1, ncp))

    def kv_copies(g, at, n, i, dc, here):
        cc = lax.rem(c + dc, ncp)
        src = c if here else cc
        rows = pl.ds(at, n)
        return (rcopy(kb.at[g, rows], kb.at[g, rows], kv_s.at[cc, 2 * i], kv_r.at[src, 2 * i], d, cc, t),
                rcopy(vt.at[g, :, rows], vt.at[g, :, rows], kv_s.at[cc, 2 * i + 1], kv_r.at[src, 2 * i + 1], d, cc, t))

    def kv_rows(g, at, n, src):
        r = dot(src, wkv[...])
        kb[g, pl.ds(at, n), :] = r[:, :HD].astype(BF)
        vt[g, :, pl.ds(at, n)] = r[:, HD:].astype(BF).T

    def kv_send(g, at, n, i):
        for dc in zpeers:
            for cp_ in kv_copies(g, at, n, i, dc, True):
                cp_.start()

    at_k = pl.multiple_of(k * rb, rb)
    at_c = pl.multiple_of((1 - k) * rb, rb)

    for i in (0, 1, 2):
        loads[i].wait()
    kv_rows(mine, at_k, rb, xs[t])
    kv_send(mine, at_k, rb, 0)
    cx_in.wait_recv()
    kv_rows(mine, at_c, rb, xs[t_c])
    kv_send(mine, at_c, rb, 1)
    loads[3].wait()

    def q_rows(q_ref, at, src):
        for lo in range(0, heads * HD, 256):
            hi = min(lo + 256, heads * HD)
            q_ref[pl.ds(at, rb), lo:hi] = dot(src, wq[:, lo:hi]).astype(BF)

    q_rows(q_a, at_k, xs[t])
    q_rows(q_a, at_c, xs[t_c])

    def x_copy(cc, there):
        dd = 1 - d if there else d
        return rcopy(wo_b.at[piece(dd, cc)], wo_b.at[piece(dd, cc)], wx_s.at[cc], wx_r.at[cc], 1 - d, c, t)

    def up_copy(cc, to):
        return rcopy(wo_b.at[piece(d, cc)], wo_b.at[piece(d, cc)], wu_s.at[cc], wu_r.at[cc], d, to, t)

    def dn_copy(cc, to):
        return rcopy(wo_b.at[piece(d, cc)], wo_b.at[piece(d, cc)], wd_s.at[cc], wd_r.at[cc], d, to, t)

    c_up = jnp.minimum(c + 1, ncp - 1)
    c_dn = jnp.maximum(c - 1, 0)

    def wo_first():
        rcopy(wo_hbm.at[piece(d, c)], wo_b.at[piece(d, c)], wy_s, wy_r, d, c, t_y).wait_recv()
        x_copy(c, False).start()

        @pl.when(c < ncp - 1)
        def _():
            up_copy(c, c_up).start()

        @pl.when(c > 0)
        def _():
            dn_copy(c, c_dn).start()

    def wo_next(i):
        below = jnp.maximum(c - i, 0)
        above = jnp.minimum(c + i, ncp - 1)

        @pl.when(c - i >= 0)
        def _():
            up_copy(below, c_dn).wait_recv()

            @pl.when(c < ncp - 1)
            def _():
                up_copy(below, c_up).start()
            x_copy(below, False).start()

        @pl.when(c + i <= ncp - 1)
        def _():
            dn_copy(above, c_up).wait_recv()

            @pl.when(c > 0)
            def _():
                dn_copy(above, c_dn).start()
            x_copy(above, False).start()

    wo_first()

    for i in range(2):
        yx_in[i].wait_recv()
        fwd = rcopy(xs.at[t_y, half(i)], xs.at[t_y, half(i)], fx_s.at[i], fx_r.at[i], d, c, t_c)
        fwd.start()
        a0 = pl.multiple_of(at_k + i * hk, hk)
        kv_rows(other, a0, hk, xs[t_y, i * hk:(i + 1) * hk])
        kv_send(other, a0, hk, 2 + i)
        rcopy(xs.at[t_z, half(i)], xs.at[t_z, half(i)], fx_s.at[i], fx_r.at[i], d, c, t_c).wait_recv()
        a1 = pl.multiple_of(at_c + i * hk, hk)
        kv_rows(other, a1, hk, xs[t_z, i * hk:(i + 1) * hk])
        kv_send(other, a1, hk, 4 + i)
        if i == 0:
            wo_next(1)
    q_rows(q_b, at_k, xs[t_y])
    q_rows(q_b, at_c, xs[t_z])

    for dc in zpeers:
        cc = lax.rem(c + dc, ncp)
        gm = jnp.where(y == 0, cc, last - cc)
        go = last - gm
        for i, (g, at, n) in enumerate([(gm, at_k, rb), (gm, at_c, rb),
                                        (go, at_k, hk), (go, pl.multiple_of(at_k + hk, hk), hk),
                                        (go, at_c, hk), (go, pl.multiple_of(at_c + hk, hk), hk)]):
            for cp_ in kv_copies(g, at, n, i, dc, False):
                cp_.wait_recv()

    def step(g, carry, qb, masked):
        m, l, acc = carry
        s = lax.dot_general(kb[g], qb, (((1,), (1,)), ((), ())), preferred_element_type=F32) * scale
        if masked:
            ki = lax.broadcasted_iota(jnp.int32, s.shape, 0)
            qi = lax.broadcasted_iota(jnp.int32, s.shape, 1)
            s = jnp.where(ki <= qi, s, NEG)
        mn = jnp.maximum(m, jnp.max(s, axis=0, keepdims=True))
        w = jnp.exp(s - mn)
        a = jnp.exp(m - mn)
        l = l * a + jnp.sum(w, axis=0, keepdims=True)
        acc = acc * a + dot(vt[g], w.astype(BF))
        return mn, l, acc

    def attend(q_ref, hcols, count):
        qb = q_ref[:, hcols]
        carry = (jnp.full((1, seg), NEG, F32), jnp.zeros((1, seg), F32), jnp.zeros((HD, seg), F32))
        carry = lax.fori_loop(0, count, lambda g, cr: step(g, cr, qb, False), carry)
        m, l, acc = step(count, carry, qb, True)
        return (acc / l).T.astype(BF)

    def o_copy(j):
        cols = pl.ds(pl.multiple_of(j * HD, HD), HD)
        return rcopy(o_s.at[:, cols], o_b.at[:, cols], o_ss.at[j], o_rs.at[j], d, c, t_y)

    def head(j, _):
        hcols = pl.ds(pl.multiple_of(j * HD, HD), HD)
        o_s[:, hcols] = attend(q_b, hcols, other)
        o_copy(j).start()
        o_a[:, hcols] = attend(q_a, hcols, mine)
        return 0

    lax.fori_loop(0, 1, head, 0)
    wo_next(2)
    lax.fori_loop(1, 4, head, 0)
    wo_next(3)
    lax.fori_loop(4, heads, head, 0)

    for cc in range(ncp):
        x_copy(cc, True).wait_recv()
    loads[4].wait()
    for j in range(heads):
        o_copy(j).wait_recv()

    nc = hd // 512

    def p_copy(i):
        cols = pl.ds(pl.multiple_of(i * 512, 512), 512)
        return rcopy(part.at[:, cols], pin.at[:, cols], p_ss.at[i], p_rs.at[i], d, c, t_c)

    def proj(at, cols):
        rows = pl.ds(at, rb)
        return dot(o_a[rows, :], wo_a[:, cols]) + dot(o_b[rows, :], wo_b[:, cols])

    def give(i, _):
        cols = pl.ds(pl.multiple_of(i * 512, 512), 512)
        part[:, cols] = proj(at_c, cols)
        p_copy(i).start()
        return 0

    lax.fori_loop(0, nc, give, 0)

    def keep(i, _):
        cols = pl.ds(pl.multiple_of(i * 512, 512), 512)
        own = proj(at_k, cols)
        p_copy(i).wait_recv()
        h_ref[:, cols] = (xs[t, :, cols].astype(F32) + (own + pin[:, cols])).astype(BF)
        return 0

    lax.fori_loop(0, nc, keep, 0)

    for o in others:
        dd, cc, tt = rel(*o)
        src = (dd * ncp + cc) * ntp + tt
        rcopy(most_ref, cnt.at[src], n_s.at[0], n_r.at[src], dd, cc, tt).wait_recv()
    mx_ref[...] = jnp.max(cnt[...], axis=0)

    wy.wait_send()
    cx.wait_send()
    for i in range(2):
        yx[i].wait_send()
        rcopy(xs.at[t_y, half(i)], xs.at[t_y, half(i)], fx_s.at[i], fx_r.at[i], d, c, t_c).wait_send()
    for i, o in enumerate(others):
        dd, cc, tt = rel(*o)
        rcopy(most_ref, cnt.at[me], n_s.at[i], n_r.at[me], dd, cc, tt).wait_send()
    for dc in zpeers:
        for i, (g, at, n) in enumerate([(mine, at_k, rb), (mine, at_c, rb),
                                        (other, at_k, hk), (other, pl.multiple_of(at_k + hk, hk), hk),
                                        (other, at_c, hk), (other, pl.multiple_of(at_c + hk, hk), hk)]):
            for cp_ in kv_copies(g, at, n, i, dc, True):
                cp_.wait_send()
    for cc in range(ncp):
        x_copy(cc, False).wait_send()

        @pl.when((cc <= c) & (c < ncp - 1))
        def _():
            up_copy(cc, c_up).wait_send()

        @pl.when((cc >= c) & (c > 0))
        def _():
            dn_copy(cc, c_dn).wait_send()
    for j in range(heads):
        o_copy(j).wait_send()
    for i in range(nc):
        p_copy(i).wait_send()


def attention(x, wq, wk, wv, wo, most, *, nd, ncp, ntp, cid):
    rb, hd = x.shape
    ql = wq.shape[1]
    seg = 2 * rb
    heads = ql // HD
    nseg = 2 * ncp
    n_all = nd * ncp * ntp
    hbm = pl.BlockSpec(memory_space=pl.ANY)
    vm = pl.BlockSpec(memory_space=pltpu.VMEM)
    dma = pltpu.SemaphoreType.DMA
    V = pltpu.VMEM
    return pl.pallas_call(
        functools.partial(att_kernel, nd=nd, ncp=ncp, ntp=ntp, scale=HD ** -0.5),
        in_specs=[hbm, hbm, hbm, hbm, hbm, vm],
        out_specs=[vm, vm],
        out_shape=[jax.ShapeDtypeStruct((rb, hd), BF), jax.ShapeDtypeStruct(most.shape, most.dtype)],
        scratch_shapes=[
            V((ntp, rb, hd), BF), V((hd, ql), BF), V((hd, 2 * HD), BF), V((ql, hd), BF), V((ql, hd), BF),
            V((seg, ql), BF), V((seg, ql), BF), V((nseg, seg, HD), BF), V((nseg, HD, seg), BF),
            V((seg, ql), BF), V((seg, ql), BF), V((seg, ql), BF), V((rb, hd), F32), V((rb, hd), F32),
            V((n_all,) + most.shape, most.dtype),
            dma((5,)), dma(()), dma(()), dma((2,)), dma((2,)), dma((2,)), dma((2,)),
            dma((ncp, 12)), dma((ncp, 12)), dma(()), dma(()), dma((ncp,)), dma((ncp,)),
            dma((ncp,)), dma((ncp,)), dma((ncp,)), dma((ncp,)), dma((heads,)), dma((heads,)),
            dma((hd // 512,)), dma((hd // 512,)), dma((n_all - 1,)), dma((n_all,)),
        ],
        compiler_params=pltpu.CompilerParams(collective_id=cid, has_side_effects=True, vmem_limit_bytes=VMEM_LIMIT),
        name="att",
        cost_estimate=pl.CostEstimate(flops=60_000_000_000, bytes_accessed=30_000_000, transcendentals=0),
    )(x, wq, wk, wv, wo, most)


def moe_kernel(h_ref, dr_ref, dc_ref, g_ref, wg_hbm, wu_hbm, wd_hbm, y_ref,
               send, recv, zbuf, back, act, w1buf, w2buf,
               ssem, rsem, zsem, bsem, w1sem, w2sem, *, ncp, ntp, nch, f1, f2):
    ne = ncp * ntp
    rows = ne * CH
    t, hd = h_ref.shape
    ff = wg_hbm.shape[1]
    n1, n2 = ff // f1, hd // f2
    r1, r2 = w1buf.shape[0], w2buf.shape[0]
    dp = lax.axis_index("dp")
    c = lax.axis_index("cp")
    p = lax.axis_index("tp")
    me = c * ntp + p

    order = [2, 1, 3, 0]
    peers = [(dc, dt) for dc in order[:ncp] for dt in range(ntp) if (dc, dt) != (0, 0)]

    def peer(dc, dt):
        pc = lax.rem(c + dc, ncp)
        pt = lax.rem(p + dt, ntp)
        return pc, pt, pc * ntp + pt

    def blk(e):
        return pl.ds(pl.multiple_of(e * CH, CH), CH)

    def out_copy(j, dc, dt):
        pc, pt, e = peer(dc, dt)
        return pltpu.make_async_remote_copy(send.at[j, blk(e)], recv.at[j, blk(me)], ssem.at[j, e], rsem.at[j, me],
                                            device_id=(dp, pc, pt), device_id_type=MESH)

    def in_copy(j, dc, dt):
        pc, pt, e = peer(dc, dt)
        return pltpu.make_async_remote_copy(send.at[j, blk(e)], recv.at[j, blk(e)], ssem.at[j, e], rsem.at[j, e],
                                            device_id=(dp, pc, pt), device_id_type=MESH)

    def home_copy(j, dc, dt):
        pc, pt, e = peer(dc, dt)
        return pltpu.make_async_remote_copy(zbuf.at[j, blk(e)], back.at[j, blk(me)], zsem.at[j, e], bsem.at[j, me],
                                            device_id=(dp, pc, pt), device_id_type=MESH)

    def got_copy(j, dc, dt):
        pc, pt, e = peer(dc, dt)
        return pltpu.make_async_remote_copy(zbuf.at[j, blk(e)], back.at[j, blk(e)], zsem.at[j, e], bsem.at[j, e],
                                            device_id=(dp, pc, pt), device_id_type=MESH)

    def w1_copies(s):
        slot = lax.rem(s, r1)
        cols = pl.ds(pl.multiple_of(s * f1, f1), f1)
        return (pltpu.make_async_copy(wg_hbm.at[:, cols], w1buf.at[slot, 0], w1sem.at[slot, 0]),
                pltpu.make_async_copy(wu_hbm.at[:, cols], w1buf.at[slot, 1], w1sem.at[slot, 1]))

    def w2_copy(s):
        slot = lax.rem(s, r2)
        cols = pl.ds(pl.multiple_of(s * f2, f2), f2)
        return pltpu.make_async_copy(wd_hbm.at[:, cols], w2buf.at[slot], w2sem.at[slot])

    def start_w1(s):
        for cp_ in w1_copies(s):
            cp_.start()

    def prefetch_w1():
        for s in range(r1):
            start_w1(jnp.int32(s))

    def prefetch_w2():
        for s in range(r2):
            w2_copy(jnp.int32(s)).start()

    prefetch_w1()
    prefetch_w2()

    barrier = pltpu.get_barrier_semaphore()
    for dc, dt in peers:
        pc, pt, _ = peer(dc, dt)
        pl.semaphore_signal(barrier, inc=1, device_id=(dp, pc, pt), device_id_type=MESH)
    pl.semaphore_wait(barrier, ne - 1)

    for j in range(nch):
        ri = lax.broadcasted_iota(jnp.int32, (rows, t), 0) + j * rows
        sel = jnp.where(ri == dr_ref[0:1, :], 1.0, 0.0) + jnp.where(ri == dr_ref[1:2, :], 1.0, 0.0)
        sel = sel.astype(BF)

        def pick(i, _):
            cols = pl.ds(pl.multiple_of(i * 512, 512), 512)
            send[j, :, cols] = dot(sel, h_ref[:, cols]).astype(BF)
            return 0

        lax.fori_loop(0, hd // 512, pick, 0)
        for dc, dt in peers:
            out_copy(j, dc, dt).start()
        recv[j, blk(me), :] = send[j, blk(me), :]

    for j in range(nch):
        for dc, dt in peers:
            in_copy(j, dc, dt).wait_recv()

        def up(s, _):
            slot = lax.rem(s, r1)
            for cp_ in w1_copies(s):
                cp_.wait()
            xx = recv[j]
            gg = dot(xx, w1buf[slot, 0])
            uu = dot(xx, w1buf[slot, 1])
            act[:, pl.ds(pl.multiple_of(s * f1, f1), f1)] = (gg * jax.nn.sigmoid(gg) * uu).astype(BF)

            @pl.when(s + r1 < n1)
            def _():
                start_w1(s + r1)
            return 0

        lax.fori_loop(0, n1, up, 0)
        if j + 1 < nch:
            prefetch_w1()

        def down(s, _):
            slot = lax.rem(s, r2)
            w2_copy(s).wait()
            zbuf[j, :, pl.ds(pl.multiple_of(s * f2, f2), f2)] = dot(act[...], w2buf[slot]).astype(BF)

            @pl.when(s + r2 < n2)
            def _():
                w2_copy(s + r2).start()
            return 0

        lax.fori_loop(0, n2, down, 0)
        if j + 1 < nch:
            prefetch_w2()
        for dc, dt in peers:
            home_copy(j, dc, dt).start()
        back[j, blk(me), :] = zbuf[j, blk(me), :]

    for j in range(nch):
        for dc, dt in peers:
            got_copy(j, dc, dt).wait_recv()

    ci = lax.broadcasted_iota(jnp.int32, (t, rows), 1)
    sel0 = [jnp.where(ci + j * rows == dc_ref[:, 0:1], 1.0, 0.0).astype(BF) for j in range(nch)]
    sel1 = [jnp.where(ci + j * rows == dc_ref[:, 1:2], 1.0, 0.0).astype(BF) for j in range(nch)]
    g0 = g_ref[:, 0:1]
    g1 = g_ref[:, 1:2]

    def combine(i, _):
        cols = pl.ds(pl.multiple_of(i * 512, 512), 512)
        z0 = sum(dot(sel0[j], back[j, :, cols]) for j in range(nch))
        z1 = sum(dot(sel1[j], back[j, :, cols]) for j in range(nch))
        y_ref[:, cols] = (h_ref[:, cols].astype(F32) + (g0 * z0 + g1 * z1)).astype(BF)
        return 0

    lax.fori_loop(0, hd // 512, combine, 0)

    for j in range(nch):
        for dc, dt in peers:
            out_copy(j, dc, dt).wait_send()
            home_copy(j, dc, dt).wait_send()


def moe(h, drow, dcol, gates, wg, wu, wd, *, ncp, ntp, nch, cid):
    t, hd = h.shape
    ff = wg.shape[1]
    ne = ncp * ntp
    rows = ne * CH
    f1, f2, r1, r2 = 256, 512, 2, 2
    vm = pl.BlockSpec(memory_space=pltpu.VMEM)
    hbm = pl.BlockSpec(memory_space=pl.ANY)
    dma = pltpu.SemaphoreType.DMA
    return pl.pallas_call(
        functools.partial(moe_kernel, ncp=ncp, ntp=ntp, nch=nch, f1=f1, f2=f2),
        in_specs=[vm, vm, vm, vm, hbm, hbm, hbm],
        out_specs=vm,
        out_shape=jax.ShapeDtypeStruct((t, hd), BF),
        scratch_shapes=[
            pltpu.VMEM((nch, rows, hd), BF), pltpu.VMEM((nch, rows, hd), BF),
            pltpu.VMEM((nch, rows, hd), BF), pltpu.VMEM((nch, rows, hd), BF),
            pltpu.VMEM((rows, ff), BF),
            pltpu.VMEM((r1, 2, hd, f1), BF), pltpu.VMEM((r2, ff, f2), BF),
            dma((nch, ne)), dma((nch, ne)), dma((nch, ne)), dma((nch, ne)),
            dma((r1, 2)), dma((r2,)),
        ],
        compiler_params=pltpu.CompilerParams(collective_id=cid, has_side_effects=True, vmem_limit_bytes=VMEM_LIMIT),
        name=f"moe{nch}",
        cost_estimate=pl.CostEstimate(flops=6 * nch * rows * hd * ff, bytes_accessed=6 * nch * hd * ff, transcendentals=0),
    )(h, drow, dcol, gates, wg, wu, wd)


def route(idx, ne):
    t = idx.shape[0]
    e = jnp.arange(ne, dtype=jnp.int32)[None, :]
    oh0 = (idx[:, 0:1] == e).astype(F32)
    oh1 = (idx[:, 1:2] == e).astype(F32)
    both = oh0 + oh1
    i = jnp.arange(t)
    before = dot((i[None, :] < i[:, None]).astype(F32), both)
    s0 = jnp.sum(before * oh0, axis=1).astype(jnp.int32)
    s1 = jnp.sum(before * oh1, axis=1).astype(jnp.int32)
    slot = jnp.stack([s0, s1], axis=1)
    code = (slot // CH) * (ne * CH) + idx * CH + slot % CH
    return code, jnp.max(jnp.sum(both, axis=0)).astype(jnp.int32)


def solution(mesh):
    ncp = mesh.shape["cp"]
    ntp = mesh.shape["tp"]
    ne = ncp * ntp
    rows_spec = P(("dp", "cp", "tp"), None)
    exp_spec = P(("cp", "tp"), None, None)

    def local(x, idx, gates, wq, wk, wv, wo, w1g, w1u, w2):
        code, most = route(idx, ne)
        drow = jnp.pad(code.T, ((0, 6), (0, 0)))
        h, most = attention(x, wq, wk, wv, wo, jnp.full((8, 128), most), nd=mesh.shape["dp"], ncp=ncp, ntp=ntp, cid=3)

        def few(args):
            return moe(*args, ncp=ncp, ntp=ntp, nch=2, cid=1)

        def many(args):
            return moe(*args, ncp=ncp, ntp=ntp, nch=4, cid=2)

        return lax.cond(most[0, 0] <= 2 * CH, few, many, (h, drow, code, gates, w1g[0], w1u[0], w2[0]))

    return jax.shard_map(local, mesh=mesh, in_specs=(rows_spec, rows_spec, rows_spec, P(None, "tp"), P(None, "tp"), P(None, "tp"), P("tp", None), exp_spec, exp_spec, exp_spec), out_specs=rows_spec, check_vma=False)
```

```python
import functools

import jax
import jax.numpy as jnp
from jax import lax
from jax.experimental import pallas as pl
from jax.experimental.pallas import tpu as pltpu
from jax.sharding import PartitionSpec as P

HD = 128
NEG = -1e30
BF = jnp.bfloat16
F32 = jnp.float32
MESH = pl.DeviceIdType.MESH
VMEM_LIMIT = 67_000_000
CH = 16
NCH = 2


def dot(a, b):
    return jnp.dot(a, b, preferred_element_type=F32)


def layer_kernel(x_hbm, wq_hbm, wk_hbm, wv_hbm, wo_hbm, idx_ref, g_ref, wg_hbm, wu_hbm, wd_hbm,
                 y_ref, h_ref, code_ref, mx_ref,
               xs, wq, wkv, wo_a, wo_b, qq, kb, vt, oo, o_b, part, pin, cnt, top, s0, s1, bias, acc,
               send, recv, act, w2buf,
               lsem, cx_s, cx_r, yx_s, yx_r, fx_s, fx_r, kv_s, kv_r, wy_s, wy_r, wx_s, wx_r,
               wu_s, wu_r, wd_s, wd_r, wf_s, wf_r, o_ss, o_rs, p_ss, p_rs, n_s, n_r, ssem, rsem, zsem, bsem, w1sem, w2sem, *, nd, ncp, ntp, scale):
    d = lax.axis_index("dp")
    c = lax.axis_index("cp")
    t = lax.axis_index("tp")
    y = t // 2
    k = lax.rem(t, 2)
    t_c = 2 * y + 1 - k
    t_y = 2 * (1 - y) + k
    t_z = 2 * (1 - y) + 1 - k
    rb = xs.shape[1]
    hd = xs.shape[2]
    seg = 2 * rb
    hk = rb // 2
    heads = qq.shape[2] // HD
    q_a, q_b, o_a, o_s = qq.at[0], qq.at[1], oo.at[0], oo.at[1]
    pr = wo_a.shape[0] // (nd * ncp)
    last = 2 * ncp - 1
    mine = jnp.where(y == 0, c, last - c)
    other = last - mine
    me = (d * ncp + c) * ntp + t

    def rcopy(src, dst, ss, rs, dd, cc, tt):
        return pltpu.make_async_remote_copy(src, dst, ss, rs, device_id=(dd, cc, tt), device_id_type=MESH)

    loads = [
        pltpu.make_async_copy(wk_hbm, wkv.at[:, 0:HD], lsem.at[0]),
        pltpu.make_async_copy(wv_hbm, wkv.at[:, HD:2 * HD], lsem.at[1]),
        pltpu.make_async_copy(x_hbm, xs.at[t], lsem.at[2]),
        pltpu.make_async_copy(wq_hbm, wq.at[:, 0:wq_hbm.shape[1]], lsem.at[3]),
        pltpu.make_async_copy(wo_hbm, wo_a, lsem.at[4]),
    ]
    for cp_ in loads:
        cp_.start()

    n_all = nd * ncp * ntp
    others = [(a, b, e) for a in range(nd) for b in range(ncp) for e in range(ntp) if (a, b, e) != (0, 0, 0)]

    def rel(a, b, e):
        return lax.rem(d + a, nd), lax.rem(c + b, ncp), lax.rem(t + e, ntp)

    barrier = pltpu.get_barrier_semaphore()
    for o in others:
        pl.semaphore_signal(barrier, inc=1, device_id=rel(*o), device_id_type=MESH)
    pl.semaphore_wait(barrier, n_all - 1)

    def piece(dd, cc):
        return pl.ds(pl.multiple_of((dd * ncp + cc) * pr, pr), pr)

    def half(i):
        return pl.ds(i * hk, hk)

    wy = rcopy(wo_hbm.at[piece(d, c)], wo_b.at[piece(d, c)], wy_s, wy_r, d, c, t_y)
    yx = [rcopy(x_hbm.at[half(i)], xs.at[t, half(i)], yx_s.at[i], yx_r.at[i], d, c, t_y) for i in range(2)]
    yx_in = [rcopy(x_hbm.at[half(i)], xs.at[t_y, half(i)], yx_s.at[i], yx_r.at[i], d, c, t_y) for i in range(2)]
    far = jnp.where(c < ncp // 2, ncp - 1, 0)
    wf = rcopy(wo_hbm.at[piece(d, far)], wo_b.at[piece(d, far)], wf_s, wf_r, d, c, t_y)

    wy.start()
    for cp_ in yx:
        cp_.start()
    wf.start()
    cx = rcopy(x_hbm, xs.at[t], cx_s, cx_r, d, c, t_c)
    cx_in = rcopy(x_hbm, xs.at[t_c], cx_s, cx_r, d, c, t_c)
    cx.start()

    ne = ncp * ntp
    lane = lax.broadcasted_iota(jnp.int32, (rb, 128), 1)
    e0, e1 = idx_ref[:, 0:1], idx_ref[:, 1:2]
    oh0 = jnp.where(lane == e0, 1.0, 0.0)
    oh1 = jnp.where(lane == e1, 1.0, 0.0)
    both = oh0 + oh1
    tri = jnp.where(lax.broadcasted_iota(jnp.int32, (rb, rb), 1) < lax.broadcasted_iota(jnp.int32, (rb, rb), 0), 1.0, 0.0)
    before = dot(tri.astype(BF), both.astype(BF))

    def place(oh, e):
        slot = jnp.sum(before * oh, axis=1, keepdims=True).astype(jnp.int32)
        ch = lax.shift_right_logical(slot, CH.bit_length() - 1)
        return ch * (ne * CH) + e * CH + (slot - ch * CH)

    code_ref[...] = jnp.where(lane == 0, place(oh0, e0), place(oh1, e1))
    top[...] = jnp.zeros(top.shape, F32) + jnp.max(jnp.sum(both, axis=0, keepdims=True), axis=1, keepdims=True)
    cnt[me] = top[...]
    for i, o in enumerate(others):
        dd, cc, tt = rel(*o)
        rcopy(top, cnt.at[me], n_s.at[i], n_r.at[me], dd, cc, tt).start()

    zpeers = list(range(1, ncp))

    def kv_copies(g, at, n, i, dc, here):
        cc = lax.rem(c + dc, ncp)
        src = c if here else cc
        rows = pl.ds(at, n)
        return (rcopy(kb.at[g, rows], kb.at[g, rows], kv_s.at[cc, 2 * i], kv_r.at[src, 2 * i], d, cc, t),
                rcopy(vt.at[g, :, rows], vt.at[g, :, rows], kv_s.at[cc, 2 * i + 1], kv_r.at[src, 2 * i + 1], d, cc, t))

    def kv_rows(g, at, n, src):
        r = dot(src, wkv[...])
        kb[g, pl.ds(at, n), :] = r[:, :HD].astype(BF)
        vt[g, :, pl.ds(at, n)] = r[:, HD:].astype(BF).T

    def kv_send(g, at, n, i):
        for dc in zpeers:
            for cp_ in kv_copies(g, at, n, i, dc, True):
                cp_.start()

    at_k = pl.multiple_of(k * rb, rb)
    at_c = pl.multiple_of((1 - k) * rb, rb)

    ki = lax.broadcasted_iota(jnp.int32, (seg, seg), 0)
    qi = lax.broadcasted_iota(jnp.int32, (seg, seg), 1)
    bias[0] = jnp.zeros((seg, seg), F32)
    bias[1] = jnp.where(ki <= qi, 0.0, NEG)

    for i in (0, 1, 2):
        loads[i].wait()
    kv_rows(mine, at_k, rb, xs[t])
    kv_send(mine, at_k, rb, 0)
    cx_in.wait_recv()
    kv_rows(mine, at_c, rb, xs[t_c])
    kv_send(mine, at_c, rb, 1)
    loads[3].wait()

    def q_rows(q_ref, at, src):
        for lo in range(0, heads * HD, 256):
            hi = min(lo + 256, heads * HD)
            q_ref[pl.ds(at, rb), lo:hi] = dot(src, wq[:, lo:hi]).astype(BF)

    q_rows(q_a, at_k, xs[t])
    q_rows(q_a, at_c, xs[t_c])

    def x_copy(cc, there):
        dd = 1 - d if there else d
        return rcopy(wo_b.at[piece(dd, cc)], wo_b.at[piece(dd, cc)], wx_s.at[cc], wx_r.at[cc], 1 - d, c, t)

    def up_copy(cc, to):
        return rcopy(wo_b.at[piece(d, cc)], wo_b.at[piece(d, cc)], wu_s.at[cc], wu_r.at[cc], d, to, t)

    def dn_copy(cc, to):
        return rcopy(wo_b.at[piece(d, cc)], wo_b.at[piece(d, cc)], wd_s.at[cc], wd_r.at[cc], d, to, t)

    c_up = jnp.minimum(c + 1, ncp - 1)
    c_dn = jnp.maximum(c - 1, 0)

    def wo_first():
        wy.wait_recv()
        x_copy(c, False).start()

        @pl.when(c < ncp - 1)
        def _():
            up_copy(c, c_up).start()

        @pl.when(c > 0)
        def _():
            dn_copy(c, c_dn).start()

    def wo_near():
        @pl.when(c > 0)
        def _():
            up_copy(c_dn, c_dn).wait_recv()

            @pl.when(c == ncp - 2)
            def _():
                up_copy(c_dn, c_up).start()
            x_copy(c_dn, False).start()

        @pl.when(c < ncp - 1)
        def _():
            dn_copy(c_up, c_up).wait_recv()

            @pl.when(c == 1)
            def _():
                dn_copy(c_up, c_dn).start()
            x_copy(c_up, False).start()

    def wo_ends():
        @pl.when(c == ncp - 1)
        def _():
            up_copy(ncp - 3, c_dn).wait_recv()
            x_copy(ncp - 3, False).start()

        @pl.when(c == 0)
        def _():
            dn_copy(2, c_up).wait_recv()
            x_copy(2, False).start()

    def wo_far():
        wf.wait_recv()
        x_copy(far, False).start()


    zb, bk = xs.at[2:4], xs.at[0:2]
    ff = wg_hbm.shape[1]
    f1, f2 = wq.shape[1] // 4, w2buf.shape[2]
    n1, n2 = ff // f1, hd // f2
    self_e = c * ntp + t
    rows = ne * CH
    peers = [(dc, dt) for dc in [2, 1, 3, 0] for dt in range(ntp) if (dc, dt) != (0, 0)]

    def blk(e):
        return pl.ds(pl.multiple_of(e * CH, CH), CH)

    def peer(dc, dt):
        pc = lax.rem(c + dc, ncp)
        pt = lax.rem(t + dt, ntp)
        return pc, pt, pc * ntp + pt

    def out_copy(j, dc, dt):
        pc, pt, e = peer(dc, dt)
        return rcopy(send.at[j, blk(e)], recv.at[j, blk(self_e)], ssem.at[j, e], rsem.at[j, self_e], d, pc, pt)

    def in_copy(j, dc, dt):
        pc, pt, e = peer(dc, dt)
        return rcopy(send.at[j, blk(e)], recv.at[j, blk(e)], ssem.at[j, e], rsem.at[j, e], d, pc, pt)

    def home_copy(j, dc, dt):
        pc, pt, e = peer(dc, dt)
        return rcopy(zb.at[j, blk(e)], bk.at[j, blk(self_e)], zsem.at[j, e], bsem.at[j, self_e], d, pc, pt)

    def got_copy(j, dc, dt):
        pc, pt, e = peer(dc, dt)
        return rcopy(zb.at[j, blk(e)], bk.at[j, blk(e)], zsem.at[j, e], bsem.at[j, e], d, pc, pt)

    def w1_copies(s):
        slot = lax.rem(s, 2)
        cols = pl.ds(pl.multiple_of(s * f1, f1), f1)
        return (pltpu.make_async_copy(wg_hbm.at[:, cols], wq.at[:, pl.ds(pl.multiple_of(slot * 2 * f1, f1), f1)], w1sem.at[slot, 0]),
                pltpu.make_async_copy(wu_hbm.at[:, cols], wq.at[:, pl.ds(pl.multiple_of(slot * 2 * f1 + f1, f1), f1)], w1sem.at[slot, 1]))

    def w2_copy(s):
        slot = lax.rem(s, 2)
        cols = pl.ds(pl.multiple_of(s * f2, f2), f2)
        return pltpu.make_async_copy(wd_hbm.at[:, cols], w2buf.at[slot], w2sem.at[slot])

    def prefetch_w1():
        for s in range(2):
            for cp_ in w1_copies(jnp.int32(s)):
                cp_.start()

    def prefetch_w2():
        for s in range(2):
            w2_copy(jnp.int32(s)).start()

    def dispatch():
        for i in range(2):
            rcopy(xs.at[t_y, half(i)], xs.at[t_y, half(i)], fx_s.at[i], fx_r.at[i], d, c, t_c).wait_send()
        codes = code_ref[...].astype(F32).T.astype(jnp.int32)
        for j in range(NCH):
            ri = lax.broadcasted_iota(jnp.int32, (rows, rb), 0) + j * rows
            sel = (jnp.where(ri == codes[0:1, :], 1.0, 0.0) + jnp.where(ri == codes[1:2, :], 1.0, 0.0)).astype(BF)

            def pick(i, _):
                cols = pl.ds(pl.multiple_of(i * 512, 512), 512)
                send[j, :, cols] = dot(sel, h_ref[:, cols]).astype(BF)
                return 0

            lax.fori_loop(0, nc, pick, 0)
            for dc, dt in peers:
                out_copy(j, dc, dt).start()
            recv[j, blk(self_e), :] = send[j, blk(self_e), :]

    cw = seg // 2

    def o_copy(j):
        cols = pl.ds(pl.multiple_of(j * HD, HD), HD)
        return rcopy(o_s.at[:, cols], o_b.at[:, cols], o_ss.at[j], o_rs.at[j], d, c, t_y)

    def attend(hf, count, points):
        n = count + 1

        def following(j, g):
            wrap = g == n - 1
            return jnp.minimum(j + jnp.where(wrap, 1, 0), heads - 1), jnp.where(wrap, 0, g + 1)

        def score(j, g, s_ref):
            diag = jnp.where(g == n - 1, 1, 0)
            qb = qq[hf, :, pl.ds(pl.multiple_of(j * HD, HD), HD)]
            tops = []
            for lo in range(0, seg, cw):
                v = lax.dot_general(kb[g], qb[lo:lo + cw], (((1,), (1,)), ((), ())), preferred_element_type=F32) * scale
                v = v + bias[diag, :, lo:lo + cw]
                s_ref[:, lo:lo + cw] = v
                tops.append(jnp.max(v, axis=0, keepdims=True))
            return tuple(tops)

        def soft(j, g, s_ref, tops, ms, ls):
            first = g == 0
            nm, nl = [], []
            for n_, lo in enumerate(range(0, seg, cw)):
                m = jnp.where(first, NEG, ms[n_])
                mn = jnp.maximum(m, tops[n_])
                w = jnp.exp(s_ref[:, lo:lo + cw] - mn)
                a = jnp.exp(m - mn)
                nl.append(jnp.where(first, 0.0, ls[n_]) * a + jnp.sum(w, axis=0, keepdims=True))
                acc[:, lo:lo + cw] = acc[:, lo:lo + cw] * a + dot(vt[g], w.astype(BF))
                nm.append(mn)
            return tuple(nm), tuple(nl)

        def finish(j, g, ls):
            hcols = pl.ds(pl.multiple_of(j * HD, HD), HD)

            @pl.when(g == n - 1)
            def _():
                for n_, lo in enumerate(range(0, seg, cw)):
                    oo[hf, lo:lo + cw, hcols] = (acc[:, lo:lo + cw] / ls[n_]).T.astype(BF)

            @pl.when((g == n - 1) & (hf == 1))
            def _():
                o_copy(j).start()

        def pair(u, carry):
            j0, g0, tops, ms, ls = carry
            j1, g1 = following(j0, g0)
            t1 = score(j1, g1, s1)
            ms, ls = soft(j0, g0, s0, tops, ms, ls)
            finish(j0, g0, ls)
            j2, g2 = following(j1, g1)
            t0 = score(j2, g2, s0)
            ms, ls = soft(j1, g1, s1, t1, ms, ls)
            finish(j1, g1, ls)
            return j2, g2, t0, ms, ls

        acc[...] = jnp.zeros(acc.shape, F32)
        z1 = (jnp.zeros((1, cw), F32),) * 2
        zero = jnp.int32(0)
        total = heads * n
        carry = (zero, zero, score(zero, zero, s0), z1, z1)
        at = 0
        for stop, point in points:
            stop = jnp.minimum(stop, total // 2)
            carry = lax.fori_loop(at, stop, pair, carry)
            point()
            at = stop
        j, g, tops, ms, ls = lax.fori_loop(at, total // 2, pair, carry)

        @pl.when(lax.rem(total, 2) == 1)
        def _():
            _, l2 = soft(j, g, s0, tops, ms, ls)
            finish(j, g, l2)

    def kv_wait(which):
        for dc in zpeers:
            cc = lax.rem(c + dc, ncp)
            gm = jnp.where(y == 0, cc, last - cc)
            go = last - gm
            if which == 0:
                parts = [(0, gm, at_k, rb), (1, gm, at_c, rb)]
            else:
                parts = [(2, go, at_k, hk), (3, go, pl.multiple_of(at_k + hk, hk), hk),
                         (4, go, at_c, hk), (5, go, pl.multiple_of(at_c + hk, hk), hk)]
            for i, g, at, n in parts:
                for cp_ in kv_copies(g, at, n, i, dc, False):
                    cp_.wait_recv()

    wo_first()

    for i in range(2):
        yx_in[i].wait_recv()
        fwd = rcopy(xs.at[t_y, half(i)], xs.at[t_y, half(i)], fx_s.at[i], fx_r.at[i], d, c, t_c)
        fwd.start()
        a0 = pl.multiple_of(at_k + i * hk, hk)
        kv_rows(other, a0, hk, xs[t_y, i * hk:(i + 1) * hk])
        kv_send(other, a0, hk, 2 + i)
        rcopy(xs.at[t_z, half(i)], xs.at[t_z, half(i)], fx_s.at[i], fx_r.at[i], d, c, t_c).wait_recv()
        a1 = pl.multiple_of(at_c + i * hk, hk)
        kv_rows(other, a1, hk, xs[t_z, i * hk:(i + 1) * hk])
        kv_send(other, a1, hk, 4 + i)
        if i == 0:
            wo_near()
    q_rows(q_b, at_k, xs[t_y])
    q_rows(q_b, at_c, xs[t_z])

    prefetch_w1()
    prefetch_w2()
    wo_ends()
    kv_wait(0)
    kv_wait(1)
    attend(1, other, [(3, wo_far)])
    attend(0, mine, [])

    def finish_rows():
        for cc in range(ncp):
            x_copy(cc, True).wait_recv()
        loads[4].wait()
        for j in range(heads):
            o_copy(j).wait_recv()
        lax.fori_loop(0, nc, give, 0)
        lax.fori_loop(0, nc, keep, 0)
        dispatch()

    nc = hd // 512
    def p_copy(i):
        cols = pl.ds(pl.multiple_of(i * 512, 512), 512)
        return rcopy(part.at[lax.rem(i, 2)], pin.at[:, cols], p_ss.at[i], p_rs.at[i], d, c, t_c)

    def proj(at, cols):
        rows = pl.ds(at, rb)
        return dot(o_a[rows, :], wo_a[:, cols]) + dot(o_b[rows, :], wo_b[:, cols])

    def give(i, _):
        cols = pl.ds(pl.multiple_of(i * 512, 512), 512)
        v = proj(at_c, cols)

        @pl.when(i >= 2)
        def _():
            p_copy(i - 2).wait_send()
        part[lax.rem(i, 2)] = v
        p_copy(i).start()
        return 0

    def keep(i, _):
        cols = pl.ds(pl.multiple_of(i * 512, 512), 512)
        own = proj(at_k, cols)
        p_copy(i).wait_recv()
        h_ref[:, cols] = (xs[t, :, cols].astype(F32) + (own + pin[:, cols])).astype(BF)
        return 0


    finish_rows()

    for s in range(NCH):
        for dc, dt in peers:
            in_copy(s, dc, dt).wait_recv()

        def up(i, _):
            for cp_ in w1_copies(i):
                cp_.wait()
            at = pl.multiple_of(lax.rem(i, 2) * 2 * f1, f1)
            xx = recv[s]
            gg = dot(xx, wq[:, pl.ds(at, f1)])
            uu = dot(xx, wq[:, pl.ds(pl.multiple_of(at + f1, f1), f1)])
            act[:, pl.ds(pl.multiple_of(i * f1, f1), f1)] = (gg * jax.nn.sigmoid(gg) * uu).astype(BF)

            @pl.when(i + 2 < n1)
            def _():
                for cp_ in w1_copies(i + 2):
                    cp_.start()
            return 0

        lax.fori_loop(0, n1, up, 0)
        if s + 1 < NCH:
            prefetch_w1()

        def down(i, _):
            w2_copy(i).wait()
            zb[s, :, pl.ds(pl.multiple_of(i * f2, f2), f2)] = dot(act[...], w2buf[lax.rem(i, 2)]).astype(BF)

            @pl.when(i + 2 < n2)
            def _():
                w2_copy(i + 2).start()
            return 0

        lax.fori_loop(0, n2, down, 0)
        if s + 1 < NCH:
            prefetch_w2()
        for dc, dt in peers:
            home_copy(s, dc, dt).start()
        bk[s, blk(self_e), :] = zb[s, blk(self_e), :]

    for s in range(NCH):
        for dc, dt in peers:
            got_copy(s, dc, dt).wait_recv()

    ci = lax.broadcasted_iota(jnp.int32, (rb, rows), 1)
    sel0 = [jnp.where(ci + b_ * rows == code_ref[:, 0:1], 1.0, 0.0).astype(BF) for b_ in range(NCH)]
    sel1 = [jnp.where(ci + b_ * rows == code_ref[:, 1:2], 1.0, 0.0).astype(BF) for b_ in range(NCH)]
    g0 = g_ref[:, 0:1]
    g1 = g_ref[:, 1:2]

    def combine(i, _):
        cols = pl.ds(pl.multiple_of(i * 512, 512), 512)
        z0 = dot(sel0[0], bk[0, :, cols]) + dot(sel0[1], bk[1, :, cols])
        z1 = dot(sel1[0], bk[0, :, cols]) + dot(sel1[1], bk[1, :, cols])
        y_ref[:, cols] = (h_ref[:, cols].astype(F32) + (g0 * z0 + g1 * z1)).astype(BF)
        return 0

    lax.fori_loop(0, nc, combine, 0)

    for o in others:
        dd, cc, tt = rel(*o)
        src = (dd * ncp + cc) * ntp + tt
        rcopy(top, cnt.at[src], n_s.at[0], n_r.at[src], dd, cc, tt).wait_recv()
    mx_ref[...] = jnp.max(cnt[...], axis=0)

    wy.wait_send()
    cx.wait_send()
    for i in range(2):
        yx[i].wait_send()
    for i, o in enumerate(others):
        dd, cc, tt = rel(*o)
        rcopy(top, cnt.at[me], n_s.at[i], n_r.at[me], dd, cc, tt).wait_send()
    for dc in zpeers:
        for i, (g, at, n) in enumerate([(mine, at_k, rb), (mine, at_c, rb),
                                        (other, at_k, hk), (other, pl.multiple_of(at_k + hk, hk), hk),
                                        (other, at_c, hk), (other, pl.multiple_of(at_c + hk, hk), hk)]):
            for cp_ in kv_copies(g, at, n, i, dc, True):
                cp_.wait_send()
    for cc in range(ncp):
        x_copy(cc, False).wait_send()


    @pl.when(c < ncp - 1)
    def _():
        up_copy(c, c_up).wait_send()

    @pl.when(c > 0)
    def _():
        dn_copy(c, c_dn).wait_send()

    @pl.when(c == ncp - 2)
    def _():
        up_copy(c_dn, c_up).wait_send()

    @pl.when(c == 1)
    def _():
        dn_copy(c_up, c_dn).wait_send()
    wf.wait_send()
    for j in range(heads):
        o_copy(j).wait_send()
    for i in (nc - 2, nc - 1):
        p_copy(i).wait_send()
    for j in range(NCH):
        for dc, dt in peers:
            out_copy(j, dc, dt).wait_send()
            home_copy(j, dc, dt).wait_send()


def layer(x, wq, wk, wv, wo, idx, gates, wg, wu, wd, *, nd, ncp, ntp, cid):
    rb, hd = x.shape
    ql = wq.shape[1]
    seg = 2 * rb
    heads = ql // HD
    nseg = 2 * ncp
    n_all = nd * ncp * ntp
    ne = ncp * ntp
    ff = wg.shape[1]
    hbm = pl.BlockSpec(memory_space=pl.ANY)
    vm = pl.BlockSpec(memory_space=pltpu.VMEM)
    dma = pltpu.SemaphoreType.DMA
    V = pltpu.VMEM
    return pl.pallas_call(
        functools.partial(layer_kernel, nd=nd, ncp=ncp, ntp=ntp, scale=HD ** -0.5),
        in_specs=[hbm, hbm, hbm, hbm, hbm, vm, vm, hbm, hbm, hbm],
        out_specs=[vm, vm, vm, vm],
        out_shape=[jax.ShapeDtypeStruct((rb, hd), BF), jax.ShapeDtypeStruct((rb, hd), BF), jax.ShapeDtypeStruct((rb, 128), jnp.int32), jax.ShapeDtypeStruct((8, 128), F32)],
        scratch_shapes=[
            V((ntp, rb, hd), BF), V((hd, 1024), BF), V((hd, 2 * HD), BF), V((ql, hd), BF), V((ql, hd), BF),
            V((2, seg, ql), BF), V((nseg, seg, HD), BF), V((nseg, HD, seg), BF),
            V((2, seg, ql), BF), V((seg, ql), BF), V((2, rb, 512), F32), V((rb, hd), F32),
            V((n_all, 8, 128), F32), V((8, 128), F32), V((seg, seg), F32), V((seg, seg), F32), V((2, seg, seg), F32), V((HD, seg), F32),
            V((NCH, ne * CH, hd), BF), V((NCH, ne * CH, hd), BF), V((ne * CH, ff), BF), V((2, ff, 256), BF),
            dma((5,)), dma(()), dma(()), dma((2,)), dma((2,)), dma((2,)), dma((2,)),
            dma((ncp, 12)), dma((ncp, 12)), dma(()), dma(()), dma((ncp,)), dma((ncp,)),
            dma((ncp,)), dma((ncp,)), dma((ncp,)), dma((ncp,)), dma(()), dma(()), dma((heads,)), dma((heads,)),
            dma((hd // 512,)), dma((hd // 512,)), dma((n_all - 1,)), dma((n_all,)),
            dma((NCH, ne)), dma((NCH, ne)), dma((NCH, ne)), dma((NCH, ne)), dma((2, 2)), dma((2,)),
        ],
        compiler_params=pltpu.CompilerParams(collective_id=cid, has_side_effects=True, vmem_limit_bytes=VMEM_LIMIT),
        name="layer",
        cost_estimate=pl.CostEstimate(flops=60_000_000_000, bytes_accessed=30_000_000, transcendentals=0),
    )(x, wq, wk, wv, wo, idx, gates, wg, wu, wd)


def moe_kernel(h_ref, dc_ref, g_ref, wg_hbm, wu_hbm, wd_hbm, y_ref,
               send, recv, zbuf, back, act, w1buf, w2buf,
               ssem, rsem, zsem, bsem, w1sem, w2sem, *, ncp, ntp, nch, f1, f2):
    ne = ncp * ntp
    rows = ne * CH
    t, hd = h_ref.shape
    ff = wg_hbm.shape[1]
    n1, n2 = ff // f1, hd // f2
    r1, r2 = w1buf.shape[0], w2buf.shape[0]
    dp = lax.axis_index("dp")
    c = lax.axis_index("cp")
    p = lax.axis_index("tp")
    me = c * ntp + p

    order = [2, 1, 3, 0]
    peers = [(dc, dt) for dc in order[:ncp] for dt in range(ntp) if (dc, dt) != (0, 0)]

    def peer(dc, dt):
        pc = lax.rem(c + dc, ncp)
        pt = lax.rem(p + dt, ntp)
        return pc, pt, pc * ntp + pt

    def blk(e):
        return pl.ds(pl.multiple_of(e * CH, CH), CH)

    def out_copy(j, dc, dt):
        pc, pt, e = peer(dc, dt)
        return pltpu.make_async_remote_copy(send.at[j, blk(e)], recv.at[j, blk(me)], ssem.at[j, e], rsem.at[j, me],
                                            device_id=(dp, pc, pt), device_id_type=MESH)

    def in_copy(j, dc, dt):
        pc, pt, e = peer(dc, dt)
        return pltpu.make_async_remote_copy(send.at[j, blk(e)], recv.at[j, blk(e)], ssem.at[j, e], rsem.at[j, e],
                                            device_id=(dp, pc, pt), device_id_type=MESH)

    def home_copy(j, dc, dt):
        pc, pt, e = peer(dc, dt)
        return pltpu.make_async_remote_copy(zbuf.at[j, blk(e)], back.at[j, blk(me)], zsem.at[j, e], bsem.at[j, me],
                                            device_id=(dp, pc, pt), device_id_type=MESH)

    def got_copy(j, dc, dt):
        pc, pt, e = peer(dc, dt)
        return pltpu.make_async_remote_copy(zbuf.at[j, blk(e)], back.at[j, blk(e)], zsem.at[j, e], bsem.at[j, e],
                                            device_id=(dp, pc, pt), device_id_type=MESH)

    def w1_copies(s):
        slot = lax.rem(s, r1)
        cols = pl.ds(pl.multiple_of(s * f1, f1), f1)
        return (pltpu.make_async_copy(wg_hbm.at[:, cols], w1buf.at[slot, 0], w1sem.at[slot, 0]),
                pltpu.make_async_copy(wu_hbm.at[:, cols], w1buf.at[slot, 1], w1sem.at[slot, 1]))

    def w2_copy(s):
        slot = lax.rem(s, r2)
        cols = pl.ds(pl.multiple_of(s * f2, f2), f2)
        return pltpu.make_async_copy(wd_hbm.at[:, cols], w2buf.at[slot], w2sem.at[slot])

    def start_w1(s):
        for cp_ in w1_copies(s):
            cp_.start()

    def prefetch_w1():
        for s in range(r1):
            start_w1(jnp.int32(s))

    def prefetch_w2():
        for s in range(r2):
            w2_copy(jnp.int32(s)).start()

    prefetch_w1()
    prefetch_w2()

    barrier = pltpu.get_barrier_semaphore()
    for dc, dt in peers:
        pc, pt, _ = peer(dc, dt)
        pl.semaphore_signal(barrier, inc=1, device_id=(dp, pc, pt), device_id_type=MESH)
    pl.semaphore_wait(barrier, ne - 1)

    codes = dc_ref[...].astype(F32).T.astype(jnp.int32)

    for j in range(nch):
        ri = lax.broadcasted_iota(jnp.int32, (rows, t), 0) + j * rows
        sel = jnp.where(ri == codes[0:1, :], 1.0, 0.0) + jnp.where(ri == codes[1:2, :], 1.0, 0.0)
        sel = sel.astype(BF)

        def pick(i, _):
            cols = pl.ds(pl.multiple_of(i * 512, 512), 512)
            send[j, :, cols] = dot(sel, h_ref[:, cols]).astype(BF)
            return 0

        lax.fori_loop(0, hd // 512, pick, 0)
        for dc, dt in peers:
            out_copy(j, dc, dt).start()
        recv[j, blk(me), :] = send[j, blk(me), :]

    for j in range(nch):
        for dc, dt in peers:
            in_copy(j, dc, dt).wait_recv()

        def up(s, _):
            slot = lax.rem(s, r1)
            for cp_ in w1_copies(s):
                cp_.wait()
            xx = recv[j]
            gg = dot(xx, w1buf[slot, 0])
            uu = dot(xx, w1buf[slot, 1])
            act[:, pl.ds(pl.multiple_of(s * f1, f1), f1)] = (gg * jax.nn.sigmoid(gg) * uu).astype(BF)

            @pl.when(s + r1 < n1)
            def _():
                start_w1(s + r1)
            return 0

        lax.fori_loop(0, n1, up, 0)
        if j + 1 < nch:
            prefetch_w1()

        def down(s, _):
            slot = lax.rem(s, r2)
            w2_copy(s).wait()
            zbuf[j, :, pl.ds(pl.multiple_of(s * f2, f2), f2)] = dot(act[...], w2buf[slot]).astype(BF)

            @pl.when(s + r2 < n2)
            def _():
                w2_copy(s + r2).start()
            return 0

        lax.fori_loop(0, n2, down, 0)
        if j + 1 < nch:
            prefetch_w2()
        for dc, dt in peers:
            home_copy(j, dc, dt).start()
        back[j, blk(me), :] = zbuf[j, blk(me), :]

    for j in range(nch):
        for dc, dt in peers:
            got_copy(j, dc, dt).wait_recv()

    ci = lax.broadcasted_iota(jnp.int32, (t, rows), 1)
    sel0 = [jnp.where(ci + j * rows == dc_ref[:, 0:1], 1.0, 0.0).astype(BF) for j in range(nch)]
    sel1 = [jnp.where(ci + j * rows == dc_ref[:, 1:2], 1.0, 0.0).astype(BF) for j in range(nch)]
    g0 = g_ref[:, 0:1]
    g1 = g_ref[:, 1:2]

    def combine(i, _):
        cols = pl.ds(pl.multiple_of(i * 512, 512), 512)
        z0 = sum(dot(sel0[j], back[j, :, cols]) for j in range(nch))
        z1 = sum(dot(sel1[j], back[j, :, cols]) for j in range(nch))
        y_ref[:, cols] = (h_ref[:, cols].astype(F32) + (g0 * z0 + g1 * z1)).astype(BF)
        return 0

    lax.fori_loop(0, hd // 512, combine, 0)

    for j in range(nch):
        for dc, dt in peers:
            out_copy(j, dc, dt).wait_send()
            home_copy(j, dc, dt).wait_send()


def moe(h, code, gates, wg, wu, wd, *, ncp, ntp, nch, cid):
    t, hd = h.shape
    ff = wg.shape[1]
    ne = ncp * ntp
    rows = ne * CH
    f1, f2, r1, r2 = 256, 512, 2, 2
    vm = pl.BlockSpec(memory_space=pltpu.VMEM)
    hbm = pl.BlockSpec(memory_space=pl.ANY)
    dma = pltpu.SemaphoreType.DMA
    return pl.pallas_call(
        functools.partial(moe_kernel, ncp=ncp, ntp=ntp, nch=nch, f1=f1, f2=f2),
        in_specs=[vm, vm, vm, hbm, hbm, hbm],
        out_specs=vm,
        out_shape=jax.ShapeDtypeStruct((t, hd), BF),
        scratch_shapes=[
            pltpu.VMEM((nch, rows, hd), BF), pltpu.VMEM((nch, rows, hd), BF),
            pltpu.VMEM((nch, rows, hd), BF), pltpu.VMEM((nch, rows, hd), BF),
            pltpu.VMEM((rows, ff), BF),
            pltpu.VMEM((r1, 2, hd, f1), BF), pltpu.VMEM((r2, ff, f2), BF),
            dma((nch, ne)), dma((nch, ne)), dma((nch, ne)), dma((nch, ne)),
            dma((r1, 2)), dma((r2,)),
        ],
        compiler_params=pltpu.CompilerParams(collective_id=cid, has_side_effects=True, vmem_limit_bytes=VMEM_LIMIT),
        name=f"moe{nch}",
        cost_estimate=pl.CostEstimate(flops=6 * nch * rows * hd * ff, bytes_accessed=6 * nch * hd * ff, transcendentals=0),
    )(h, code, gates, wg, wu, wd)


def solution(mesh):
    ncp = mesh.shape["cp"]
    ntp = mesh.shape["tp"]
    rows_spec = P(("dp", "cp", "tp"), None)
    exp_spec = P(("cp", "tp"), None, None)

    def local(x, idx, gates, wq, wk, wv, wo, w1g, w1u, w2):
        y, h, code, most = layer(x, wq, wk, wv, wo, idx, gates, w1g[0], w1u[0], w2[0], nd=mesh.shape["dp"], ncp=ncp, ntp=ntp, cid=3)

        def few(args):
            return y

        def many(args):
            return moe(*args, ncp=ncp, ntp=ntp, nch=4, cid=2)

        return lax.cond(most[0, 0] <= NCH * CH, few, many, (h, code, gates, w1g[0], w1u[0], w2[0]))

    return jax.shard_map(local, mesh=mesh, in_specs=(rows_spec, rows_spec, rows_spec, P(None, "tp"), P(None, "tp"), P(None, "tp"), P("tp", None), exp_spec, exp_spec, exp_spec), out_specs=rows_spec, check_vma=False)
```

```python
import functools

import jax
import jax.numpy as jnp
from jax import lax
from jax.experimental import pallas as pl
from jax.experimental.pallas import tpu as pltpu
from jax.sharding import PartitionSpec as P

HD = 128
NEG = -1e30
BF = jnp.bfloat16
F32 = jnp.float32
MESH = pl.DeviceIdType.MESH
VMEM_LIMIT = 67_000_000
CH = 16
NCH = 2


def dot(a, b):
    return jnp.dot(a, b, preferred_element_type=F32)


def layer_kernel(x_hbm, wq_hbm, wk_hbm, wv_hbm, wo_hbm, idx_ref, g_ref, wg_hbm, wu_hbm, wd_hbm,
                 y_ref, h_ref, code_ref, mx_ref,
               xs, wq, wkv, wo_a, wo_b, qq, kb, vt, oo, o_b, part, pin, cnt, top, s0, s1, bias, acc,
               send, recv, act, w2buf,
               lsem, cx_s, cx_r, yx_s, yx_r, fx_s, fx_r, kv_s, kv_r, wy_s, wy_r, wx_s, wx_r,
               wu_s, wu_r, wd_s, wd_r, wf_s, wf_r, wc_s, wc_r, o_ss, o_rs, p_ss, p_rs, n_s, n_r, ssem, rsem, zsem, bsem, w1sem, w2sem, *, nd, ncp, ntp, scale):
    d = lax.axis_index("dp")
    c = lax.axis_index("cp")
    t = lax.axis_index("tp")
    y = t // 2
    k = lax.rem(t, 2)
    t_c = 2 * y + 1 - k
    t_y = 2 * (1 - y) + k
    t_z = 2 * (1 - y) + 1 - k
    rb = xs.shape[1]
    hd = xs.shape[2]
    seg = 2 * rb
    hk = rb // 2
    heads = qq.shape[2] // HD
    q_a, q_b, o_a, o_s = qq.at[0], qq.at[1], oo.at[0], oo.at[1]
    pr = wo_a.shape[0] // (nd * ncp)
    last = 2 * ncp - 1
    mine = jnp.where(y == 0, c, last - c)
    other = last - mine
    me = (d * ncp + c) * ntp + t

    def rcopy(src, dst, ss, rs, dd, cc, tt):
        return pltpu.make_async_remote_copy(src, dst, ss, rs, device_id=(dd, cc, tt), device_id_type=MESH)

    loads = [
        pltpu.make_async_copy(wk_hbm, wkv.at[:, 0:HD], lsem.at[0]),
        pltpu.make_async_copy(wv_hbm, wkv.at[:, HD:2 * HD], lsem.at[1]),
        pltpu.make_async_copy(x_hbm, xs.at[t], lsem.at[2]),
        pltpu.make_async_copy(wq_hbm, wq.at[:, 0:wq_hbm.shape[1]], lsem.at[3]),
        pltpu.make_async_copy(wo_hbm, wo_a, lsem.at[4]),
    ]
    for cp_ in loads:
        cp_.start()

    n_all = nd * ncp * ntp
    others = [(a, b, e) for a in range(nd) for b in range(ncp) for e in range(ntp) if (a, b, e) != (0, 0, 0)]

    def rel(a, b, e):
        return lax.rem(d + a, nd), lax.rem(c + b, ncp), lax.rem(t + e, ntp)

    barrier = pltpu.get_barrier_semaphore()
    for o in others:
        pl.semaphore_signal(barrier, inc=1, device_id=rel(*o), device_id_type=MESH)
    pl.semaphore_wait(barrier, n_all - 1)

    def piece(dd, cc):
        return pl.ds(pl.multiple_of((dd * ncp + cc) * pr, pr), pr)

    def half(i):
        return pl.ds(i * hk, hk)

    def cols2(v):
        return pl.ds(v * (hd // 2), hd // 2)

    def wo_cut(ref, dd, cc, v):
        return ref.at[piece(dd, cc), cols2(v)]

    wy = [rcopy(wo_cut(wo_hbm, d, c, v), wo_cut(wo_b, d, c, v), wy_s.at[v], wy_r.at[v], d, c, t_y) for v in range(2)]
    yx = [rcopy(x_hbm.at[half(i)], xs.at[t, half(i)], yx_s.at[i], yx_r.at[i], d, c, t_y) for i in range(2)]
    yx_in = [rcopy(x_hbm.at[half(i)], xs.at[t_y, half(i)], yx_s.at[i], yx_r.at[i], d, c, t_y) for i in range(2)]
    far = jnp.where(c < ncp // 2, ncp - 1, 0)
    wf = rcopy(wo_hbm.at[piece(d, far)], wo_b.at[piece(d, far)], wf_s, wf_r, d, c, t_y)

    wy[0].start()
    for cp_ in yx:
        cp_.start()
    wy[1].start()
    wf.start()
    cx = rcopy(x_hbm, xs.at[t], cx_s, cx_r, d, c, t_c)
    cx_in = rcopy(x_hbm, xs.at[t_c], cx_s, cx_r, d, c, t_c)
    cx.start()

    ne = ncp * ntp
    lane = lax.broadcasted_iota(jnp.int32, (rb, 128), 1)

    def column(ref, i):
        return jnp.broadcast_to(ref[i:i + 1, :].astype(F32), (128, rb)).T

    e0, e1 = column(idx_ref, 0).astype(jnp.int32), column(idx_ref, 1).astype(jnp.int32)
    oh0 = jnp.where(lane == e0, 1.0, 0.0)
    oh1 = jnp.where(lane == e1, 1.0, 0.0)
    both = oh0 + oh1
    tri = jnp.where(lax.broadcasted_iota(jnp.int32, (rb, rb), 1) < lax.broadcasted_iota(jnp.int32, (rb, rb), 0), 1.0, 0.0)
    before = dot(tri.astype(BF), both.astype(BF))

    def place(oh, e):
        slot = jnp.sum(before * oh, axis=1, keepdims=True).astype(jnp.int32)
        ch = lax.shift_right_logical(slot, CH.bit_length() - 1)
        return ch * (ne * CH) + e * CH + (slot - ch * CH)

    code_ref[...] = jnp.where(lane == 0, place(oh0, e0), place(oh1, e1))
    top[...] = jnp.zeros(top.shape, F32) + jnp.max(jnp.sum(both, axis=0, keepdims=True), axis=1, keepdims=True)
    cnt[me] = top[...]
    for i, o in enumerate(others):
        dd, cc, tt = rel(*o)
        rcopy(top, cnt.at[me], n_s.at[i], n_r.at[me], dd, cc, tt).start()

    zpeers = list(range(1, ncp))

    def kv_copies(g, at, n, i, dc, here):
        cc = lax.rem(c + dc, ncp)
        src = c if here else cc
        rows = pl.ds(at, n)
        return (rcopy(kb.at[g, rows], kb.at[g, rows], kv_s.at[cc, 2 * i], kv_r.at[src, 2 * i], d, cc, t),
                rcopy(vt.at[g, :, rows], vt.at[g, :, rows], kv_s.at[cc, 2 * i + 1], kv_r.at[src, 2 * i + 1], d, cc, t))

    def kv_rows(g, at, n, src):
        r = dot(src, wkv[...])
        kb[g, pl.ds(at, n), :] = r[:, :HD].astype(BF)
        vt[g, :, pl.ds(at, n)] = r[:, HD:].astype(BF).T

    def kv_send(g, at, n, i):
        for dc in zpeers:
            for cp_ in kv_copies(g, at, n, i, dc, True):
                cp_.start()

    at_k = pl.multiple_of(k * rb, rb)
    at_c = pl.multiple_of((1 - k) * rb, rb)

    ki = lax.broadcasted_iota(jnp.int32, (seg, seg), 0)
    qi = lax.broadcasted_iota(jnp.int32, (seg, seg), 1)
    bias[0] = jnp.zeros((seg, seg), F32)
    bias[1] = jnp.where(ki <= qi, 0.0, NEG)

    for i in (0, 1, 2):
        loads[i].wait()
    kv_rows(mine, at_k, rb, xs[t])
    kv_send(mine, at_k, rb, 0)
    cx_in.wait_recv()
    kv_rows(mine, at_c, rb, xs[t_c])
    kv_send(mine, at_c, rb, 1)
    loads[3].wait()

    def q_rows(q_ref, at, src):
        for lo in range(0, heads * HD, 256):
            hi = min(lo + 256, heads * HD)
            q_ref[pl.ds(at, rb), lo:hi] = dot(src, wq[:, lo:hi]).astype(BF)

    q_rows(q_a, at_k, xs[t])
    q_rows(q_a, at_c, xs[t_c])

    def x_copy(cc, there, v):
        dd = 1 - d if there else d
        return rcopy(wo_cut(wo_b, dd, cc, v), wo_cut(wo_b, dd, cc, v), wx_s.at[cc, v], wx_r.at[cc, v], 1 - d, c, t)

    def up_copy(cc, to, v):
        return rcopy(wo_cut(wo_b, d, cc, v), wo_cut(wo_b, d, cc, v), wu_s.at[cc, v], wu_r.at[cc, v], d, to, t)

    def dn_copy(cc, to, v):
        return rcopy(wo_cut(wo_b, d, cc, v), wo_cut(wo_b, d, cc, v), wd_s.at[cc, v], wd_r.at[cc, v], d, to, t)

    def up2_copy(cc, to):
        return rcopy(wo_cut(wo_b, 1 - d, cc, 1), wo_cut(wo_b, 1 - d, cc, 1), wc_s.at[0], wc_r.at[0], d, to, t)

    def dn2_copy(cc, to):
        return rcopy(wo_cut(wo_b, 1 - d, cc, 1), wo_cut(wo_b, 1 - d, cc, 1), wc_s.at[1], wc_r.at[1], d, to, t)

    c_up = jnp.minimum(c + 1, ncp - 1)
    c_dn = jnp.maximum(c - 1, 0)

    def wo_first(v):
        wy[v].wait_recv()
        x_copy(c, False, v).start()

        @pl.when(c < ncp - 1)
        def _():
            up_copy(c, c_up, v).start()

        @pl.when(c > 0)
        def _():
            dn_copy(c, c_dn, v).start()

    def wo_near(v):
        @pl.when(c > 0)
        def _():
            up_copy(c_dn, c_dn, v).wait_recv()

            @pl.when(c == ncp - 2)
            def _():
                up_copy(c_dn, c_up, v).start()
            if v == 0:
                x_copy(c_dn, False, v).start()

        @pl.when(c < ncp - 1)
        def _():
            dn_copy(c_up, c_up, v).wait_recv()

            @pl.when(c == 1)
            def _():
                dn_copy(c_up, c_dn, v).start()
            if v == 0:
                x_copy(c_up, False, v).start()

    def wo_cross():
        x_copy(c, True, 1).wait_recv()

        @pl.when(c < ncp - 1)
        def _():
            up2_copy(c, c_up).start()

        @pl.when(c > 0)
        def _():
            dn2_copy(c, c_dn).start()

    def wo_ends(v):
        @pl.when(c == ncp - 1)
        def _():
            up_copy(ncp - 3, c_dn, v).wait_recv()
            x_copy(ncp - 3, False, v).start()

        @pl.when(c == 0)
        def _():
            dn_copy(2, c_up, v).wait_recv()
            x_copy(2, False, v).start()

    def wo_far():
        wf.wait_recv()
        for v in range(2):
            x_copy(far, False, v).start()


    zb, bk = xs.at[2:4], xs.at[0:2]
    ff = wg_hbm.shape[1]
    f1, f2 = wq.shape[1] // 4, w2buf.shape[2]
    n1, n2 = ff // f1, hd // f2
    self_e = c * ntp + t
    rows = ne * CH
    peers = [(dc, dt) for dc in [2, 1, 3, 0] for dt in range(ntp) if (dc, dt) != (0, 0)]

    def blk(e):
        return pl.ds(pl.multiple_of(e * CH, CH), CH)

    def peer(dc, dt):
        pc = lax.rem(c + dc, ncp)
        pt = lax.rem(t + dt, ntp)
        return pc, pt, pc * ntp + pt

    def out_copy(j, dc, dt):
        pc, pt, e = peer(dc, dt)
        return rcopy(send.at[j, blk(e)], recv.at[j, blk(self_e)], ssem.at[j, e], rsem.at[j, self_e], d, pc, pt)

    def in_copy(j, dc, dt):
        pc, pt, e = peer(dc, dt)
        return rcopy(send.at[j, blk(e)], recv.at[j, blk(e)], ssem.at[j, e], rsem.at[j, e], d, pc, pt)

    def home_copy(j, dc, dt):
        pc, pt, e = peer(dc, dt)
        return rcopy(zb.at[j, blk(e)], bk.at[j, blk(self_e)], zsem.at[j, e], bsem.at[j, self_e], d, pc, pt)

    def got_copy(j, dc, dt):
        pc, pt, e = peer(dc, dt)
        return rcopy(zb.at[j, blk(e)], bk.at[j, blk(e)], zsem.at[j, e], bsem.at[j, e], d, pc, pt)

    def w1_copies(s):
        slot = lax.rem(s, 2)
        cols = pl.ds(pl.multiple_of(s * f1, f1), f1)
        return (pltpu.make_async_copy(wg_hbm.at[:, cols], wq.at[:, pl.ds(pl.multiple_of(slot * 2 * f1, f1), f1)], w1sem.at[slot, 0]),
                pltpu.make_async_copy(wu_hbm.at[:, cols], wq.at[:, pl.ds(pl.multiple_of(slot * 2 * f1 + f1, f1), f1)], w1sem.at[slot, 1]))

    def w2_copy(s):
        slot = lax.rem(s, 2)
        cols = pl.ds(pl.multiple_of(s * f2, f2), f2)
        return pltpu.make_async_copy(wd_hbm.at[:, cols], w2buf.at[slot], w2sem.at[slot])

    def prefetch_w1():
        for s in range(2):
            for cp_ in w1_copies(jnp.int32(s)):
                cp_.start()

    def prefetch_w2():
        for s in range(2):
            w2_copy(jnp.int32(s)).start()

    def dispatch():
        for i in range(2):
            rcopy(xs.at[t_y, half(i)], xs.at[t_y, half(i)], fx_s.at[i], fx_r.at[i], d, c, t_c).wait_send()
        codes = code_ref[...].astype(F32).T.astype(jnp.int32)
        for j in range(NCH):
            ri = lax.broadcasted_iota(jnp.int32, (rows, rb), 0) + j * rows
            sel = (jnp.where(ri == codes[0:1, :], 1.0, 0.0) + jnp.where(ri == codes[1:2, :], 1.0, 0.0)).astype(BF)

            def pick(i, _):
                cols = pl.ds(pl.multiple_of(i * 512, 512), 512)
                send[j, :, cols] = dot(sel, h_ref[:, cols]).astype(BF)
                return 0

            lax.fori_loop(0, nc, pick, 0)
            for dc, dt in peers:
                out_copy(j, dc, dt).start()
            recv[j, blk(self_e), :] = send[j, blk(self_e), :]

    cw = seg // 2

    def o_copy(j):
        cols = pl.ds(pl.multiple_of(j * HD, HD), HD)
        return rcopy(o_s.at[:, cols], o_b.at[:, cols], o_ss.at[j], o_rs.at[j], d, c, t_y)

    def attend(hf, count, points):
        n = count + 1

        def following(j, g):
            wrap = g == n - 1
            return jnp.minimum(j + jnp.where(wrap, 1, 0), heads - 1), jnp.where(wrap, 0, g + 1)

        def score(j, g, s_ref):
            diag = jnp.where(g == n - 1, 1, 0)
            qb = qq[hf, :, pl.ds(pl.multiple_of(j * HD, HD), HD)]
            tops = []
            for lo in range(0, seg, cw):
                v = lax.dot_general(kb[g], qb[lo:lo + cw], (((1,), (1,)), ((), ())), preferred_element_type=F32) * scale
                v = v + bias[diag, :, lo:lo + cw]
                s_ref[:, lo:lo + cw] = v
                tops.append(jnp.max(v, axis=0, keepdims=True))
            return tuple(tops)

        def soft(j, g, s_ref, tops, ms, ls):
            first = g == 0
            nm, nl = [], []
            for n_, lo in enumerate(range(0, seg, cw)):
                m = jnp.where(first, NEG, ms[n_])
                mn = jnp.maximum(m, tops[n_])
                w = jnp.exp(s_ref[:, lo:lo + cw] - mn)
                a = jnp.exp(m - mn)
                nl.append(jnp.where(first, 0.0, ls[n_]) * a + jnp.sum(w, axis=0, keepdims=True))
                acc[:, lo:lo + cw] = acc[:, lo:lo + cw] * a + dot(vt[g], w.astype(BF))
                nm.append(mn)
            return tuple(nm), tuple(nl)

        def finish(j, g, ls):
            hcols = pl.ds(pl.multiple_of(j * HD, HD), HD)

            @pl.when(g == n - 1)
            def _():
                for n_, lo in enumerate(range(0, seg, cw)):
                    oo[hf, lo:lo + cw, hcols] = (acc[:, lo:lo + cw] / ls[n_]).T.astype(BF)

            @pl.when((g == n - 1) & (hf == 1))
            def _():
                o_copy(j).start()

        def pair(u, carry):
            j0, g0, tops, ms, ls = carry
            j1, g1 = following(j0, g0)
            t1 = score(j1, g1, s1)
            ms, ls = soft(j0, g0, s0, tops, ms, ls)
            finish(j0, g0, ls)
            j2, g2 = following(j1, g1)
            t0 = score(j2, g2, s0)
            ms, ls = soft(j1, g1, s1, t1, ms, ls)
            finish(j1, g1, ls)
            return j2, g2, t0, ms, ls

        acc[...] = jnp.zeros(acc.shape, F32)
        z1 = (jnp.zeros((1, cw), F32),) * 2
        zero = jnp.int32(0)
        total = heads * n
        carry = (zero, zero, score(zero, zero, s0), z1, z1)
        at = 0
        for stop, here, point in points:
            stop = jnp.minimum(stop, total // 2)
            carry = lax.fori_loop(at, stop, pair, carry)
            pl.when(here)(point)
            at = stop
        j, g, tops, ms, ls = lax.fori_loop(at, total // 2, pair, carry)

        @pl.when(lax.rem(total, 2) == 1)
        def _():
            _, l2 = soft(j, g, s0, tops, ms, ls)
            finish(j, g, l2)

    def kv_wait(which):
        for dc in zpeers:
            cc = lax.rem(c + dc, ncp)
            gm = jnp.where(y == 0, cc, last - cc)
            go = last - gm
            if which == 0:
                parts = [(0, gm, at_k, rb), (1, gm, at_c, rb)]
            else:
                parts = [(2, go, at_k, hk), (3, go, pl.multiple_of(at_k + hk, hk), hk),
                         (4, go, at_c, hk), (5, go, pl.multiple_of(at_c + hk, hk), hk)]
            for i, g, at, n in parts:
                for cp_ in kv_copies(g, at, n, i, dc, False):
                    cp_.wait_recv()

    wo_first(0)

    for i in range(2):
        yx_in[i].wait_recv()
        fwd = rcopy(xs.at[t_y, half(i)], xs.at[t_y, half(i)], fx_s.at[i], fx_r.at[i], d, c, t_c)
        fwd.start()
        a0 = pl.multiple_of(at_k + i * hk, hk)
        kv_rows(other, a0, hk, xs[t_y, i * hk:(i + 1) * hk])
        kv_send(other, a0, hk, 2 + i)
        rcopy(xs.at[t_z, half(i)], xs.at[t_z, half(i)], fx_s.at[i], fx_r.at[i], d, c, t_c).wait_recv()
        a1 = pl.multiple_of(at_c + i * hk, hk)
        kv_rows(other, a1, hk, xs[t_z, i * hk:(i + 1) * hk])
        kv_send(other, a1, hk, 4 + i)
        if i == 0:
            wo_near(0)
    q_rows(q_b, at_k, xs[t_y])
    q_rows(q_b, at_c, xs[t_z])

    prefetch_w1()
    prefetch_w2()
    wo_ends(0)
    kv_wait(0)
    wo_first(1)
    kv_wait(1)
    points = [(4, wo_cross), (5, lambda: wo_near(1)), (13, wo_far), (20, lambda: wo_ends(1))]
    done = heads * (other + 1) // 2
    attend(1, other, [(stop, stop <= done, point) for stop, point in points])
    attend(0, mine, [(jnp.maximum(stop - done, 0), stop > done, point) for stop, point in points])

    def finish_rows():
        for cc in range(ncp):
            x_copy(cc, True, 0).wait_recv()
        x_copy(far, True, 1).wait_recv()

        @pl.when(c == 0)
        def _():
            x_copy(2, True, 1).wait_recv()

        @pl.when(c == ncp - 1)
        def _():
            x_copy(ncp - 3, True, 1).wait_recv()

        @pl.when(c > 0)
        def _():
            up2_copy(c_dn, c_dn).wait_recv()

        @pl.when(c < ncp - 1)
        def _():
            dn2_copy(c_up, c_up).wait_recv()
        loads[4].wait()
        for j in range(heads):
            o_copy(j).wait_recv()
        lax.fori_loop(0, nc, give, 0)
        lax.fori_loop(0, nc, keep, 0)
        dispatch()

    nc = hd // 512
    def p_copy(i):
        cols = pl.ds(pl.multiple_of(i * 512, 512), 512)
        return rcopy(part.at[lax.rem(i, 2)], pin.at[:, cols], p_ss.at[i], p_rs.at[i], d, c, t_c)

    def proj(at, cols):
        rows = pl.ds(at, rb)
        return dot(o_a[rows, :], wo_a[:, cols]) + dot(o_b[rows, :], wo_b[:, cols])

    def give(i, _):
        cols = pl.ds(pl.multiple_of(i * 512, 512), 512)
        v = proj(at_c, cols)

        @pl.when(i >= 2)
        def _():
            p_copy(i - 2).wait_send()
        part[lax.rem(i, 2)] = v
        p_copy(i).start()
        return 0

    def keep(i, _):
        cols = pl.ds(pl.multiple_of(i * 512, 512), 512)
        own = proj(at_k, cols)
        p_copy(i).wait_recv()
        h_ref[:, cols] = (xs[t, :, cols].astype(F32) + (own + pin[:, cols])).astype(BF)
        return 0


    finish_rows()

    for s in range(NCH):
        for dc, dt in peers:
            in_copy(s, dc, dt).wait_recv()

        def up(i, _):
            for cp_ in w1_copies(i):
                cp_.wait()
            at = pl.multiple_of(lax.rem(i, 2) * 2 * f1, f1)
            xx = recv[s]
            gg = dot(xx, wq[:, pl.ds(at, f1)])
            uu = dot(xx, wq[:, pl.ds(pl.multiple_of(at + f1, f1), f1)])
            act[:, pl.ds(pl.multiple_of(i * f1, f1), f1)] = (gg * jax.nn.sigmoid(gg) * uu).astype(BF)

            @pl.when(i + 2 < n1)
            def _():
                for cp_ in w1_copies(i + 2):
                    cp_.start()
            return 0

        lax.fori_loop(0, n1, up, 0)
        if s + 1 < NCH:
            prefetch_w1()

        def down(i, _):
            w2_copy(i).wait()
            zb[s, :, pl.ds(pl.multiple_of(i * f2, f2), f2)] = dot(act[...], w2buf[lax.rem(i, 2)]).astype(BF)

            @pl.when(i + 2 < n2)
            def _():
                w2_copy(i + 2).start()
            return 0

        lax.fori_loop(0, n2, down, 0)
        if s + 1 < NCH:
            prefetch_w2()
        for dc, dt in peers:
            home_copy(s, dc, dt).start()
        bk[s, blk(self_e), :] = zb[s, blk(self_e), :]

    ci = lax.broadcasted_iota(jnp.int32, (rb, rows), 1)
    g0 = column(g_ref, 0)[:, 0:1]
    g1 = column(g_ref, 1)[:, 0:1]
    for s in range(NCH):
        sel0 = jnp.where(ci + s * rows == code_ref[:, 0:1], 1.0, 0.0).astype(BF)
        sel1 = jnp.where(ci + s * rows == code_ref[:, 1:2], 1.0, 0.0).astype(BF)
        for dc, dt in peers:
            got_copy(s, dc, dt).wait_recv()

        def combine(i, _):
            cols = pl.ds(pl.multiple_of(i * 512, 512), 512)
            v = g0 * dot(sel0, bk[s, :, cols]) + g1 * dot(sel1, bk[s, :, cols])
            if s > 0:
                v = pin[:, cols] + v
            if s + 1 < NCH:
                pin[:, cols] = v
            else:
                y_ref[:, cols] = (h_ref[:, cols].astype(F32) + v).astype(BF)
            return 0

        lax.fori_loop(0, nc, combine, 0)

    for o in others:
        dd, cc, tt = rel(*o)
        src = (dd * ncp + cc) * ntp + tt
        rcopy(top, cnt.at[src], n_s.at[0], n_r.at[src], dd, cc, tt).wait_recv()
    mx_ref[...] = jnp.max(cnt[...], axis=0)

    for v in range(2):
        wy[v].wait_send()
    cx.wait_send()
    for i in range(2):
        yx[i].wait_send()
    for i, o in enumerate(others):
        dd, cc, tt = rel(*o)
        rcopy(top, cnt.at[me], n_s.at[i], n_r.at[me], dd, cc, tt).wait_send()
    for dc in zpeers:
        for i, (g, at, n) in enumerate([(mine, at_k, rb), (mine, at_c, rb),
                                        (other, at_k, hk), (other, pl.multiple_of(at_k + hk, hk), hk),
                                        (other, at_c, hk), (other, pl.multiple_of(at_c + hk, hk), hk)]):
            for cp_ in kv_copies(g, at, n, i, dc, True):
                cp_.wait_send()
    for cc in range(ncp):
        x_copy(cc, False, 0).wait_send()
    x_copy(c, False, 1).wait_send()
    x_copy(far, False, 1).wait_send()

    @pl.when(c == 0)
    def _():
        x_copy(2, False, 1).wait_send()

    @pl.when(c == ncp - 1)
    def _():
        x_copy(ncp - 3, False, 1).wait_send()

    @pl.when(c < ncp - 1)
    def _():
        up2_copy(c, c_up).wait_send()

    @pl.when(c > 0)
    def _():
        dn2_copy(c, c_dn).wait_send()

    for v in range(2):

        @pl.when(c < ncp - 1)
        def _():
            up_copy(c, c_up, v).wait_send()

        @pl.when(c > 0)
        def _():
            dn_copy(c, c_dn, v).wait_send()

        @pl.when(c == ncp - 2)
        def _():
            up_copy(c_dn, c_up, v).wait_send()

        @pl.when(c == 1)
        def _():
            dn_copy(c_up, c_dn, v).wait_send()
    wf.wait_send()
    for j in range(heads):
        o_copy(j).wait_send()
    for i in (nc - 2, nc - 1):
        p_copy(i).wait_send()
    for j in range(NCH):
        for dc, dt in peers:
            out_copy(j, dc, dt).wait_send()
            home_copy(j, dc, dt).wait_send()


def layer(x, wq, wk, wv, wo, idx, gates, wg, wu, wd, *, nd, ncp, ntp, cid):
    rb, hd = x.shape
    ql = wq.shape[1]
    seg = 2 * rb
    heads = ql // HD
    nseg = 2 * ncp
    n_all = nd * ncp * ntp
    ne = ncp * ntp
    ff = wg.shape[1]
    hbm = pl.BlockSpec(memory_space=pl.ANY)
    vm = pl.BlockSpec(memory_space=pltpu.VMEM)
    dma = pltpu.SemaphoreType.DMA
    V = pltpu.VMEM
    return pl.pallas_call(
        functools.partial(layer_kernel, nd=nd, ncp=ncp, ntp=ntp, scale=HD ** -0.5),
        in_specs=[hbm, hbm, hbm, hbm, hbm, vm, vm, hbm, hbm, hbm],
        out_specs=[vm, vm, vm, vm],
        out_shape=[jax.ShapeDtypeStruct((rb, hd), BF), jax.ShapeDtypeStruct((rb, hd), BF), jax.ShapeDtypeStruct((rb, 128), jnp.int32), jax.ShapeDtypeStruct((8, 128), F32)],
        scratch_shapes=[
            V((ntp, rb, hd), BF), V((hd, 1024), BF), V((hd, 2 * HD), BF), V((ql, hd), BF), V((ql, hd), BF),
            V((2, seg, ql), BF), V((nseg, seg, HD), BF), V((nseg, HD, seg), BF),
            V((2, seg, ql), BF), V((seg, ql), BF), V((2, rb, 512), F32), V((rb, hd), F32),
            V((n_all, 8, 128), F32), V((8, 128), F32), V((seg, seg), F32), V((seg, seg), F32), V((2, seg, seg), F32), V((HD, seg), F32),
            V((NCH, ne * CH, hd), BF), V((NCH, ne * CH, hd), BF), V((ne * CH, ff), BF), V((2, ff, 256), BF),
            dma((5,)), dma(()), dma(()), dma((2,)), dma((2,)), dma((2,)), dma((2,)),
            dma((ncp, 12)), dma((ncp, 12)), dma((2,)), dma((2,)), dma((ncp, 2)), dma((ncp, 2)),
            dma((ncp, 2)), dma((ncp, 2)), dma((ncp, 2)), dma((ncp, 2)), dma(()), dma(()), dma((2,)), dma((2,)), dma((heads,)), dma((heads,)),
            dma((hd // 512,)), dma((hd // 512,)), dma((n_all - 1,)), dma((n_all,)),
            dma((NCH, ne)), dma((NCH, ne)), dma((NCH, ne)), dma((NCH, ne)), dma((2, 2)), dma((2,)),
        ],
        compiler_params=pltpu.CompilerParams(collective_id=cid, has_side_effects=True, vmem_limit_bytes=VMEM_LIMIT),
        name="layer",
        cost_estimate=pl.CostEstimate(flops=60_000_000_000, bytes_accessed=30_000_000, transcendentals=0),
    )(x, wq, wk, wv, wo, idx.T, gates.T, wg, wu, wd)


def moe_kernel(h_ref, dc_ref, g_ref, wg_hbm, wu_hbm, wd_hbm, y_ref,
               send, recv, zbuf, back, act, w1buf, w2buf,
               ssem, rsem, zsem, bsem, w1sem, w2sem, *, ncp, ntp, nch, f1, f2):
    ne = ncp * ntp
    rows = ne * CH
    t, hd = h_ref.shape
    ff = wg_hbm.shape[1]
    n1, n2 = ff // f1, hd // f2
    r1, r2 = w1buf.shape[0], w2buf.shape[0]
    dp = lax.axis_index("dp")
    c = lax.axis_index("cp")
    p = lax.axis_index("tp")
    me = c * ntp + p

    order = [2, 1, 3, 0]
    peers = [(dc, dt) for dc in order[:ncp] for dt in range(ntp) if (dc, dt) != (0, 0)]

    def peer(dc, dt):
        pc = lax.rem(c + dc, ncp)
        pt = lax.rem(p + dt, ntp)
        return pc, pt, pc * ntp + pt

    def blk(e):
        return pl.ds(pl.multiple_of(e * CH, CH), CH)

    def out_copy(j, dc, dt):
        pc, pt, e = peer(dc, dt)
        return pltpu.make_async_remote_copy(send.at[j, blk(e)], recv.at[j, blk(me)], ssem.at[j, e], rsem.at[j, me],
                                            device_id=(dp, pc, pt), device_id_type=MESH)

    def in_copy(j, dc, dt):
        pc, pt, e = peer(dc, dt)
        return pltpu.make_async_remote_copy(send.at[j, blk(e)], recv.at[j, blk(e)], ssem.at[j, e], rsem.at[j, e],
                                            device_id=(dp, pc, pt), device_id_type=MESH)

    def home_copy(j, dc, dt):
        pc, pt, e = peer(dc, dt)
        return pltpu.make_async_remote_copy(zbuf.at[j, blk(e)], back.at[j, blk(me)], zsem.at[j, e], bsem.at[j, me],
                                            device_id=(dp, pc, pt), device_id_type=MESH)

    def got_copy(j, dc, dt):
        pc, pt, e = peer(dc, dt)
        return pltpu.make_async_remote_copy(zbuf.at[j, blk(e)], back.at[j, blk(e)], zsem.at[j, e], bsem.at[j, e],
                                            device_id=(dp, pc, pt), device_id_type=MESH)

    def w1_copies(s):
        slot = lax.rem(s, r1)
        cols = pl.ds(pl.multiple_of(s * f1, f1), f1)
        return (pltpu.make_async_copy(wg_hbm.at[:, cols], w1buf.at[slot, 0], w1sem.at[slot, 0]),
                pltpu.make_async_copy(wu_hbm.at[:, cols], w1buf.at[slot, 1], w1sem.at[slot, 1]))

    def w2_copy(s):
        slot = lax.rem(s, r2)
        cols = pl.ds(pl.multiple_of(s * f2, f2), f2)
        return pltpu.make_async_copy(wd_hbm.at[:, cols], w2buf.at[slot], w2sem.at[slot])

    def start_w1(s):
        for cp_ in w1_copies(s):
            cp_.start()

    def prefetch_w1():
        for s in range(r1):
            start_w1(jnp.int32(s))

    def prefetch_w2():
        for s in range(r2):
            w2_copy(jnp.int32(s)).start()

    prefetch_w1()
    prefetch_w2()

    barrier = pltpu.get_barrier_semaphore()
    for dc, dt in peers:
        pc, pt, _ = peer(dc, dt)
        pl.semaphore_signal(barrier, inc=1, device_id=(dp, pc, pt), device_id_type=MESH)
    pl.semaphore_wait(barrier, ne - 1)

    codes = dc_ref[...].astype(F32).T.astype(jnp.int32)

    for j in range(nch):
        ri = lax.broadcasted_iota(jnp.int32, (rows, t), 0) + j * rows
        sel = jnp.where(ri == codes[0:1, :], 1.0, 0.0) + jnp.where(ri == codes[1:2, :], 1.0, 0.0)
        sel = sel.astype(BF)

        def pick(i, _):
            cols = pl.ds(pl.multiple_of(i * 512, 512), 512)
            send[j, :, cols] = dot(sel, h_ref[:, cols]).astype(BF)
            return 0

        lax.fori_loop(0, hd // 512, pick, 0)
        for dc, dt in peers:
            out_copy(j, dc, dt).start()
        recv[j, blk(me), :] = send[j, blk(me), :]

    for j in range(nch):
        for dc, dt in peers:
            in_copy(j, dc, dt).wait_recv()

        def up(s, _):
            slot = lax.rem(s, r1)
            for cp_ in w1_copies(s):
                cp_.wait()
            xx = recv[j]
            gg = dot(xx, w1buf[slot, 0])
            uu = dot(xx, w1buf[slot, 1])
            act[:, pl.ds(pl.multiple_of(s * f1, f1), f1)] = (gg * jax.nn.sigmoid(gg) * uu).astype(BF)

            @pl.when(s + r1 < n1)
            def _():
                start_w1(s + r1)
            return 0

        lax.fori_loop(0, n1, up, 0)
        if j + 1 < nch:
            prefetch_w1()

        def down(s, _):
            slot = lax.rem(s, r2)
            w2_copy(s).wait()
            zbuf[j, :, pl.ds(pl.multiple_of(s * f2, f2), f2)] = dot(act[...], w2buf[slot]).astype(BF)

            @pl.when(s + r2 < n2)
            def _():
                w2_copy(s + r2).start()
            return 0

        lax.fori_loop(0, n2, down, 0)
        if j + 1 < nch:
            prefetch_w2()
        for dc, dt in peers:
            home_copy(j, dc, dt).start()
        back[j, blk(me), :] = zbuf[j, blk(me), :]

    for j in range(nch):
        for dc, dt in peers:
            got_copy(j, dc, dt).wait_recv()

    ci = lax.broadcasted_iota(jnp.int32, (t, rows), 1)
    sel0 = [jnp.where(ci + j * rows == dc_ref[:, 0:1], 1.0, 0.0).astype(BF) for j in range(nch)]
    sel1 = [jnp.where(ci + j * rows == dc_ref[:, 1:2], 1.0, 0.0).astype(BF) for j in range(nch)]
    g0 = g_ref[:, 0:1]
    g1 = g_ref[:, 1:2]

    def combine(i, _):
        cols = pl.ds(pl.multiple_of(i * 512, 512), 512)
        z0 = sum(dot(sel0[j], back[j, :, cols]) for j in range(nch))
        z1 = sum(dot(sel1[j], back[j, :, cols]) for j in range(nch))
        y_ref[:, cols] = (h_ref[:, cols].astype(F32) + (g0 * z0 + g1 * z1)).astype(BF)
        return 0

    lax.fori_loop(0, hd // 512, combine, 0)

    for j in range(nch):
        for dc, dt in peers:
            out_copy(j, dc, dt).wait_send()
            home_copy(j, dc, dt).wait_send()


def moe(h, code, gates, wg, wu, wd, *, ncp, ntp, nch, cid):
    t, hd = h.shape
    ff = wg.shape[1]
    ne = ncp * ntp
    rows = ne * CH
    f1, f2, r1, r2 = 256, 512, 2, 2
    vm = pl.BlockSpec(memory_space=pltpu.VMEM)
    hbm = pl.BlockSpec(memory_space=pl.ANY)
    dma = pltpu.SemaphoreType.DMA
    return pl.pallas_call(
        functools.partial(moe_kernel, ncp=ncp, ntp=ntp, nch=nch, f1=f1, f2=f2),
        in_specs=[vm, vm, vm, hbm, hbm, hbm],
        out_specs=vm,
        out_shape=jax.ShapeDtypeStruct((t, hd), BF),
        scratch_shapes=[
            pltpu.VMEM((nch, rows, hd), BF), pltpu.VMEM((nch, rows, hd), BF),
            pltpu.VMEM((nch, rows, hd), BF), pltpu.VMEM((nch, rows, hd), BF),
            pltpu.VMEM((rows, ff), BF),
            pltpu.VMEM((r1, 2, hd, f1), BF), pltpu.VMEM((r2, ff, f2), BF),
            dma((nch, ne)), dma((nch, ne)), dma((nch, ne)), dma((nch, ne)),
            dma((r1, 2)), dma((r2,)),
        ],
        compiler_params=pltpu.CompilerParams(collective_id=cid, has_side_effects=True, vmem_limit_bytes=VMEM_LIMIT),
        name=f"moe{nch}",
        cost_estimate=pl.CostEstimate(flops=6 * nch * rows * hd * ff, bytes_accessed=6 * nch * hd * ff, transcendentals=0),
    )(h, code, gates, wg, wu, wd)


def solution(mesh):
    ncp = mesh.shape["cp"]
    ntp = mesh.shape["tp"]
    rows_spec = P(("dp", "cp", "tp"), None)
    exp_spec = P(("cp", "tp"), None, None)

    def local(x, idx, gates, wq, wk, wv, wo, w1g, w1u, w2):
        y, h, code, most = layer(x, wq, wk, wv, wo, idx, gates, w1g[0], w1u[0], w2[0], nd=mesh.shape["dp"], ncp=ncp, ntp=ntp, cid=3)

        def few(args):
            return y

        def many(args):
            return moe(*args, ncp=ncp, ntp=ntp, nch=4, cid=2)

        return lax.cond(most[0, 0] <= NCH * CH, few, many, (h, code, gates, w1g[0], w1u[0], w2[0]))

    return jax.shard_map(local, mesh=mesh, in_specs=(rows_spec, rows_spec, rows_spec, P(None, "tp"), P(None, "tp"), P(None, "tp"), P("tp", None), exp_spec, exp_spec, exp_spec), out_specs=rows_spec, check_vma=False)
```

```python
import functools

import jax
import jax.numpy as jnp
from jax import lax
from jax.experimental import pallas as pl
from jax.experimental.pallas import tpu as pltpu
from jax.sharding import PartitionSpec as P

HD = 128
NEG = -1e30
BF = jnp.bfloat16
F32 = jnp.float32
MESH = pl.DeviceIdType.MESH
VMEM_LIMIT = 67_000_000
CH = 16
NCH = 2


def dot(a, b):
    return jnp.dot(a, b, preferred_element_type=F32)


def layer_kernel(x_hbm, wq_hbm, wk_hbm, wv_hbm, wo_hbm, idx_ref, g_ref, wg_hbm, wu_hbm, wd_hbm,
                 y_ref, h_ref, code_ref, mx_ref,
               xs, wq, wkv, wo_a, wo_b, qq, kb, vt, oo, o_b, part, pin, cnt, top, s0, s1, bias, acc,
               send, recv, act, w2buf,
               lsem, cx_s, cx_r, yx_s, yx_r, fx_s, fx_r, kv_s, kv_r, wy_s, wy_r, wx_s, wx_r,
               wu_s, wu_r, wd_s, wd_r, wf_s, wf_r, wc_s, wc_r, o_ss, o_rs, p_ss, p_rs, n_s, n_r, ssem, rsem, zsem, bsem, w1sem, w2sem, *, nd, ncp, ntp, scale):
    d = lax.axis_index("dp")
    c = lax.axis_index("cp")
    t = lax.axis_index("tp")
    y = t // 2
    k = lax.rem(t, 2)
    t_c = 2 * y + 1 - k
    t_y = 2 * (1 - y) + k
    t_z = 2 * (1 - y) + 1 - k
    rb = xs.shape[1]
    hd = xs.shape[2]
    seg = 2 * rb
    hk = rb // 2
    heads = qq.shape[2] // HD
    q_a, q_b, o_a, o_s = qq.at[0], qq.at[1], oo.at[0], oo.at[1]
    pr = wo_a.shape[0] // (nd * ncp)
    last = 2 * ncp - 1
    mine = jnp.where(y == 0, c, last - c)
    other = last - mine
    me = (d * ncp + c) * ntp + t

    def rcopy(src, dst, ss, rs, dd, cc, tt):
        return pltpu.make_async_remote_copy(src, dst, ss, rs, device_id=(dd, cc, tt), device_id_type=MESH)

    loads = [
        pltpu.make_async_copy(wk_hbm, wkv.at[:, 0:HD], lsem.at[0]),
        pltpu.make_async_copy(wv_hbm, wkv.at[:, HD:2 * HD], lsem.at[1]),
        pltpu.make_async_copy(x_hbm, xs.at[t], lsem.at[2]),
        pltpu.make_async_copy(wq_hbm, wq.at[:, 0:wq_hbm.shape[1]], lsem.at[3]),
        pltpu.make_async_copy(wo_hbm, wo_a, lsem.at[4]),
    ]
    for cp_ in loads:
        cp_.start()

    n_all = nd * ncp * ntp
    others = [(a, b, e) for a in range(nd) for b in range(ncp) for e in range(ntp) if (a, b, e) != (0, 0, 0)]

    def rel(a, b, e):
        return lax.rem(d + a, nd), lax.rem(c + b, ncp), lax.rem(t + e, ntp)

    barrier = pltpu.get_barrier_semaphore()
    for o in others:
        pl.semaphore_signal(barrier, inc=1, device_id=rel(*o), device_id_type=MESH)
    pl.semaphore_wait(barrier, n_all - 1)

    def piece(dd, cc):
        return pl.ds(pl.multiple_of((dd * ncp + cc) * pr, pr), pr)

    def half(i):
        return pl.ds(i * hk, hk)

    def cols2(v):
        return pl.ds(v * (hd // 2), hd // 2)

    def wo_cut(ref, dd, cc, v):
        return ref.at[piece(dd, cc), cols2(v)]

    wy = [rcopy(wo_cut(wo_hbm, d, c, v), wo_cut(wo_b, d, c, v), wy_s.at[v], wy_r.at[v], d, c, t_y) for v in range(2)]
    yx = [rcopy(x_hbm.at[half(i)], xs.at[t, half(i)], yx_s.at[i], yx_r.at[i], d, c, t_y) for i in range(2)]
    yx_in = [rcopy(x_hbm.at[half(i)], xs.at[t_y, half(i)], yx_s.at[i], yx_r.at[i], d, c, t_y) for i in range(2)]
    far = jnp.where(c < ncp // 2, ncp - 1, 0)
    wf = rcopy(wo_hbm.at[piece(d, far)], wo_b.at[piece(d, far)], wf_s, wf_r, d, c, t_y)

    wy[0].start()
    for cp_ in yx:
        cp_.start()
    wy[1].start()
    wf.start()
    cx = rcopy(x_hbm, xs.at[t], cx_s, cx_r, d, c, t_c)
    cx_in = rcopy(x_hbm, xs.at[t_c], cx_s, cx_r, d, c, t_c)
    cx.start()

    ne = ncp * ntp
    lane = lax.broadcasted_iota(jnp.int32, (rb, 128), 1)

    def column(ref, i):
        return jnp.broadcast_to(ref[i:i + 1, :].astype(F32), (128, rb)).T

    e0, e1 = column(idx_ref, 0).astype(jnp.int32), column(idx_ref, 1).astype(jnp.int32)
    oh0 = jnp.where(lane == e0, 1.0, 0.0)
    oh1 = jnp.where(lane == e1, 1.0, 0.0)
    both = oh0 + oh1
    tri = jnp.where(lax.broadcasted_iota(jnp.int32, (rb, rb), 1) < lax.broadcasted_iota(jnp.int32, (rb, rb), 0), 1.0, 0.0)
    before = dot(tri.astype(BF), both.astype(BF))

    def place(oh, e):
        slot = jnp.sum(before * oh, axis=1, keepdims=True).astype(jnp.int32)
        ch = lax.shift_right_logical(slot, CH.bit_length() - 1)
        return ch * (ne * CH) + e * CH + (slot - ch * CH)

    code_ref[...] = jnp.where(lane == 0, place(oh0, e0), place(oh1, e1))
    top[...] = jnp.zeros(top.shape, F32) + jnp.max(jnp.sum(both, axis=0, keepdims=True), axis=1, keepdims=True)
    cnt[me] = top[...]
    for i, o in enumerate(others):
        dd, cc, tt = rel(*o)
        rcopy(top, cnt.at[me], n_s.at[i], n_r.at[me], dd, cc, tt).start()

    zpeers = list(range(1, ncp))

    def kv_copies(g, at, n, i, dc, here):
        cc = lax.rem(c + dc, ncp)
        src = c if here else cc
        rows = pl.ds(at, n)
        return (rcopy(kb.at[g, rows], kb.at[g, rows], kv_s.at[cc, 2 * i], kv_r.at[src, 2 * i], d, cc, t),
                rcopy(vt.at[g, :, rows], vt.at[g, :, rows], kv_s.at[cc, 2 * i + 1], kv_r.at[src, 2 * i + 1], d, cc, t))

    def kv_rows(g, at, n, src):
        r = dot(src, wkv[...])
        kb[g, pl.ds(at, n), :] = r[:, :HD].astype(BF)
        vt[g, :, pl.ds(at, n)] = r[:, HD:].astype(BF).T

    def kv_send(g, at, n, i):
        for dc in zpeers:
            for cp_ in kv_copies(g, at, n, i, dc, True):
                cp_.start()

    at_k = pl.multiple_of(k * rb, rb)
    at_c = pl.multiple_of((1 - k) * rb, rb)

    ki = lax.broadcasted_iota(jnp.int32, (seg, seg), 0)
    qi = lax.broadcasted_iota(jnp.int32, (seg, seg), 1)
    bias[0] = jnp.zeros((seg, seg), F32)
    bias[1] = jnp.where(ki <= qi, 0.0, NEG)

    for i in (0, 1, 2):
        loads[i].wait()
    kv_rows(mine, at_k, rb, xs[t])
    kv_send(mine, at_k, rb, 0)
    cx_in.wait_recv()
    kv_rows(mine, at_c, rb, xs[t_c])
    kv_send(mine, at_c, rb, 1)
    loads[3].wait()

    def q_rows(q_ref, at, src):
        for lo in range(0, heads * HD, 256):
            hi = min(lo + 256, heads * HD)
            q_ref[pl.ds(at, rb), lo:hi] = dot(src, wq[:, lo:hi]).astype(BF)

    q_rows(q_a, at_k, xs[t])
    q_rows(q_a, at_c, xs[t_c])

    def x_copy(cc, there, v):
        dd = 1 - d if there else d
        return rcopy(wo_cut(wo_b, dd, cc, v), wo_cut(wo_b, dd, cc, v), wx_s.at[cc, v], wx_r.at[cc, v], 1 - d, c, t)

    def up_copy(cc, to, v):
        return rcopy(wo_cut(wo_b, d, cc, v), wo_cut(wo_b, d, cc, v), wu_s.at[cc, v], wu_r.at[cc, v], d, to, t)

    def dn_copy(cc, to, v):
        return rcopy(wo_cut(wo_b, d, cc, v), wo_cut(wo_b, d, cc, v), wd_s.at[cc, v], wd_r.at[cc, v], d, to, t)

    def up2_copy(cc, to):
        return rcopy(wo_cut(wo_b, 1 - d, cc, 1), wo_cut(wo_b, 1 - d, cc, 1), wc_s.at[0], wc_r.at[0], d, to, t)

    def dn2_copy(cc, to):
        return rcopy(wo_cut(wo_b, 1 - d, cc, 1), wo_cut(wo_b, 1 - d, cc, 1), wc_s.at[1], wc_r.at[1], d, to, t)

    c_up = jnp.minimum(c + 1, ncp - 1)
    c_dn = jnp.maximum(c - 1, 0)

    def wo_first(v):
        wy[v].wait_recv()
        x_copy(c, False, v).start()

        @pl.when(c < ncp - 1)
        def _():
            up_copy(c, c_up, v).start()

        @pl.when(c > 0)
        def _():
            dn_copy(c, c_dn, v).start()

    def wo_near(v):
        @pl.when(c > 0)
        def _():
            up_copy(c_dn, c_dn, v).wait_recv()

            @pl.when(c == ncp - 2)
            def _():
                up_copy(c_dn, c_up, v).start()
            if v == 0:
                x_copy(c_dn, False, v).start()

        @pl.when(c < ncp - 1)
        def _():
            dn_copy(c_up, c_up, v).wait_recv()

            @pl.when(c == 1)
            def _():
                dn_copy(c_up, c_dn, v).start()
            if v == 0:
                x_copy(c_up, False, v).start()

    def wo_cross():
        x_copy(c, True, 1).wait_recv()

        @pl.when(c < ncp - 1)
        def _():
            up2_copy(c, c_up).start()

        @pl.when(c > 0)
        def _():
            dn2_copy(c, c_dn).start()

    def wo_ends(v):
        @pl.when(c == ncp - 1)
        def _():
            up_copy(ncp - 3, c_dn, v).wait_recv()
            x_copy(ncp - 3, False, v).start()

        @pl.when(c == 0)
        def _():
            dn_copy(2, c_up, v).wait_recv()
            x_copy(2, False, v).start()

    def wo_far():
        wf.wait_recv()
        for v in range(2):
            x_copy(far, False, v).start()


    zb, bk = xs.at[2:4], xs.at[0:2]
    ff = wg_hbm.shape[1]
    f1, f2 = wq.shape[1] // 4, w2buf.shape[2]
    n1, n2 = ff // f1, hd // f2
    self_e = c * ntp + t
    rows = ne * CH
    peers = [(dc, dt) for dc in [2, 1, 3, 0] for dt in range(ntp) if (dc, dt) != (0, 0)]

    def blk(e):
        return pl.ds(pl.multiple_of(e * CH, CH), CH)

    def peer(dc, dt):
        pc = lax.rem(c + dc, ncp)
        pt = lax.rem(t + dt, ntp)
        return pc, pt, pc * ntp + pt

    early = 1024
    cuts = [(0, 0, early), (0, early, hd)] + [(j, 0, hd) for j in range(1, NCH)]

    def out_copy(n, dc, dt):
        pc, pt, e = peer(dc, dt)
        j, lo, hi = cuts[n]
        return rcopy(send.at[j, blk(e), lo:hi], recv.at[j, blk(self_e), lo:hi], ssem.at[n, e], rsem.at[n, self_e], d, pc, pt)

    def in_copy(n, dc, dt):
        pc, pt, e = peer(dc, dt)
        j, lo, hi = cuts[n]
        return rcopy(send.at[j, blk(e), lo:hi], recv.at[j, blk(e), lo:hi], ssem.at[n, e], rsem.at[n, e], d, pc, pt)

    def home_copy(j, dc, dt):
        pc, pt, e = peer(dc, dt)
        return rcopy(zb.at[j, blk(e)], bk.at[j, blk(self_e)], zsem.at[j, e], bsem.at[j, self_e], d, pc, pt)

    def got_copy(j, dc, dt):
        pc, pt, e = peer(dc, dt)
        return rcopy(zb.at[j, blk(e)], bk.at[j, blk(e)], zsem.at[j, e], bsem.at[j, e], d, pc, pt)

    def w1_copies(s):
        slot = lax.rem(s, 2)
        cols = pl.ds(pl.multiple_of(s * f1, f1), f1)
        return (pltpu.make_async_copy(wg_hbm.at[:, cols], wq.at[:, pl.ds(pl.multiple_of(slot * 2 * f1, f1), f1)], w1sem.at[slot, 0]),
                pltpu.make_async_copy(wu_hbm.at[:, cols], wq.at[:, pl.ds(pl.multiple_of(slot * 2 * f1 + f1, f1), f1)], w1sem.at[slot, 1]))

    def w2_copy(s):
        slot = lax.rem(s, 2)
        cols = pl.ds(pl.multiple_of(s * f2, f2), f2)
        return pltpu.make_async_copy(wd_hbm.at[:, cols], w2buf.at[slot], w2sem.at[slot])

    def prefetch_w1():
        for s in range(2):
            for cp_ in w1_copies(jnp.int32(s)):
                cp_.start()

    def prefetch_w2():
        for s in range(2):
            w2_copy(jnp.int32(s)).start()

    def dispatch(ns):
        codes = code_ref[...].astype(F32).T.astype(jnp.int32)
        for n in ns:
            j, lo, hi = cuts[n]
            ri = lax.broadcasted_iota(jnp.int32, (rows, rb), 0) + j * rows
            sel = (jnp.where(ri == codes[0:1, :], 1.0, 0.0) + jnp.where(ri == codes[1:2, :], 1.0, 0.0)).astype(BF)

            def pick(i, _):
                cols = pl.ds(pl.multiple_of(i * 512, 512), 512)
                send[j, :, cols] = dot(sel, h_ref[:, cols]).astype(BF)
                return 0

            lax.fori_loop(lo // 512, hi // 512, pick, 0)
            for dc, dt in peers:
                out_copy(n, dc, dt).start()
            recv[j, blk(self_e), lo:hi] = send[j, blk(self_e), lo:hi]

    cw = seg // 2

    def o_copy(j):
        cols = pl.ds(pl.multiple_of(j * HD, HD), HD)
        return rcopy(o_s.at[:, cols], o_b.at[:, cols], o_ss.at[j], o_rs.at[j], d, c, t_y)

    def attend(hf, count, points):
        n = count + 1

        def following(j, g):
            wrap = g == n - 1
            return jnp.minimum(j + jnp.where(wrap, 1, 0), heads - 1), jnp.where(wrap, 0, g + 1)

        def score(j, g, s_ref):
            diag = jnp.where(g == n - 1, 1, 0)
            qb = qq[hf, :, pl.ds(pl.multiple_of(j * HD, HD), HD)]
            tops = []
            for lo in range(0, seg, cw):
                v = lax.dot_general(kb[g], qb[lo:lo + cw], (((1,), (1,)), ((), ())), preferred_element_type=F32) * scale
                v = v + bias[diag, :, lo:lo + cw]
                s_ref[:, lo:lo + cw] = v
                tops.append(jnp.max(v, axis=0, keepdims=True))
            return tuple(tops)

        def soft(j, g, s_ref, tops, ms, ls):
            first = g == 0
            nm, nl = [], []
            for n_, lo in enumerate(range(0, seg, cw)):
                m = jnp.where(first, NEG, ms[n_])
                mn = jnp.maximum(m, tops[n_])
                w = jnp.exp(s_ref[:, lo:lo + cw] - mn)
                a = jnp.exp(m - mn)
                nl.append(jnp.where(first, 0.0, ls[n_]) * a + jnp.sum(w, axis=0, keepdims=True))
                acc[:, lo:lo + cw] = acc[:, lo:lo + cw] * a + dot(vt[g], w.astype(BF))
                nm.append(mn)
            return tuple(nm), tuple(nl)

        def finish(j, g, ls):
            hcols = pl.ds(pl.multiple_of(j * HD, HD), HD)

            @pl.when(g == n - 1)
            def _():
                for n_, lo in enumerate(range(0, seg, cw)):
                    oo[hf, lo:lo + cw, hcols] = (acc[:, lo:lo + cw] / ls[n_]).T.astype(BF)

            @pl.when((g == n - 1) & (hf == 1))
            def _():
                o_copy(j).start()

        def pair(u, carry):
            j0, g0, tops, ms, ls = carry
            j1, g1 = following(j0, g0)
            t1 = score(j1, g1, s1)
            ms, ls = soft(j0, g0, s0, tops, ms, ls)
            finish(j0, g0, ls)
            j2, g2 = following(j1, g1)
            t0 = score(j2, g2, s0)
            ms, ls = soft(j1, g1, s1, t1, ms, ls)
            finish(j1, g1, ls)
            return j2, g2, t0, ms, ls

        acc[...] = jnp.zeros(acc.shape, F32)
        z1 = (jnp.zeros((1, cw), F32),) * 2
        zero = jnp.int32(0)
        total = heads * n
        carry = (zero, zero, score(zero, zero, s0), z1, z1)
        at = 0
        for stop, here, point in points:
            stop = jnp.minimum(stop, total // 2)
            carry = lax.fori_loop(at, stop, pair, carry)
            pl.when(here)(point)
            at = stop
        j, g, tops, ms, ls = lax.fori_loop(at, total // 2, pair, carry)

        @pl.when(lax.rem(total, 2) == 1)
        def _():
            _, l2 = soft(j, g, s0, tops, ms, ls)
            finish(j, g, l2)

    def kv_wait(which):
        for dc in zpeers:
            cc = lax.rem(c + dc, ncp)
            gm = jnp.where(y == 0, cc, last - cc)
            go = last - gm
            if which == 0:
                parts = [(0, gm, at_k, rb), (1, gm, at_c, rb)]
            else:
                parts = [(2, go, at_k, hk), (3, go, pl.multiple_of(at_k + hk, hk), hk),
                         (4, go, at_c, hk), (5, go, pl.multiple_of(at_c + hk, hk), hk)]
            for i, g, at, n in parts:
                for cp_ in kv_copies(g, at, n, i, dc, False):
                    cp_.wait_recv()

    wo_first(0)

    for i in range(2):
        yx_in[i].wait_recv()
        fwd = rcopy(xs.at[t_y, half(i)], xs.at[t_y, half(i)], fx_s.at[i], fx_r.at[i], d, c, t_c)
        fwd.start()
        a0 = pl.multiple_of(at_k + i * hk, hk)
        kv_rows(other, a0, hk, xs[t_y, i * hk:(i + 1) * hk])
        kv_send(other, a0, hk, 2 + i)
        rcopy(xs.at[t_z, half(i)], xs.at[t_z, half(i)], fx_s.at[i], fx_r.at[i], d, c, t_c).wait_recv()
        a1 = pl.multiple_of(at_c + i * hk, hk)
        kv_rows(other, a1, hk, xs[t_z, i * hk:(i + 1) * hk])
        kv_send(other, a1, hk, 4 + i)
        if i == 0:
            wo_near(0)
    q_rows(q_b, at_k, xs[t_y])
    q_rows(q_b, at_c, xs[t_z])

    prefetch_w1()
    prefetch_w2()
    wo_ends(0)
    kv_wait(0)
    wo_first(1)
    kv_wait(1)
    points = [(4, wo_cross), (5, lambda: wo_near(1)), (13, wo_far), (20, lambda: wo_ends(1))]
    done = heads * (other + 1) // 2
    attend(1, other, [(stop, stop <= done, point) for stop, point in points])
    attend(0, mine, [(jnp.maximum(stop - done, 0), stop > done, point) for stop, point in points])

    def finish_rows():
        for cc in range(ncp):
            x_copy(cc, True, 0).wait_recv()
        loads[4].wait()
        for j in range(heads):
            o_copy(j).wait_recv()
        for i in range(2):
            rcopy(xs.at[t_y, half(i)], xs.at[t_y, half(i)], fx_s.at[i], fx_r.at[i], d, c, t_c).wait_send()
        ahead = early // 512
        lax.fori_loop(0, ahead + 1, give, 0)
        lax.fori_loop(0, ahead, keep, 0)
        dispatch([0])

        x_copy(far, True, 1).wait_recv()

        @pl.when(c == 0)
        def _():
            x_copy(2, True, 1).wait_recv()

        @pl.when(c == ncp - 1)
        def _():
            x_copy(ncp - 3, True, 1).wait_recv()

        @pl.when(c > 0)
        def _():
            up2_copy(c_dn, c_dn).wait_recv()

        @pl.when(c < ncp - 1)
        def _():
            dn2_copy(c_up, c_up).wait_recv()
        lax.fori_loop(ahead + 1, nc, give, 0)
        lax.fori_loop(ahead, nc, keep, 0)
        dispatch(range(1, len(cuts)))

    nc = hd // 512
    def p_copy(i):
        cols = pl.ds(pl.multiple_of(i * 512, 512), 512)
        return rcopy(part.at[lax.rem(i, 2)], pin.at[:, cols], p_ss.at[i], p_rs.at[i], d, c, t_c)

    def proj(at, cols):
        rows = pl.ds(at, rb)
        return dot(o_a[rows, :], wo_a[:, cols]) + dot(o_b[rows, :], wo_b[:, cols])

    def give(i, _):
        cols = pl.ds(pl.multiple_of(i * 512, 512), 512)
        v = proj(at_c, cols)

        @pl.when(i >= 2)
        def _():
            p_copy(i - 2).wait_send()
        part[lax.rem(i, 2)] = v
        p_copy(i).start()
        return 0

    def keep(i, _):
        cols = pl.ds(pl.multiple_of(i * 512, 512), 512)
        own = proj(at_k, cols)
        p_copy(i).wait_recv()
        h_ref[:, cols] = (xs[t, :, cols].astype(F32) + (own + pin[:, cols])).astype(BF)
        return 0


    finish_rows()

    for s in range(NCH):
        for n in range(len(cuts)):
            if cuts[n][0] == s:
                for dc, dt in peers:
                    in_copy(n, dc, dt).wait_recv()

        def up(i, _):
            for cp_ in w1_copies(i):
                cp_.wait()
            at = pl.multiple_of(lax.rem(i, 2) * 2 * f1, f1)
            xx = recv[s]
            gg = dot(xx, wq[:, pl.ds(at, f1)])
            uu = dot(xx, wq[:, pl.ds(pl.multiple_of(at + f1, f1), f1)])
            act[:, pl.ds(pl.multiple_of(i * f1, f1), f1)] = (gg * jax.nn.sigmoid(gg) * uu).astype(BF)

            @pl.when(i + 2 < n1)
            def _():
                for cp_ in w1_copies(i + 2):
                    cp_.start()
            return 0

        lax.fori_loop(0, n1, up, 0)
        if s + 1 < NCH:
            prefetch_w1()

        def down(i, _):
            w2_copy(i).wait()
            zb[s, :, pl.ds(pl.multiple_of(i * f2, f2), f2)] = dot(act[...], w2buf[lax.rem(i, 2)]).astype(BF)

            @pl.when(i + 2 < n2)
            def _():
                w2_copy(i + 2).start()
            return 0

        lax.fori_loop(0, n2, down, 0)
        if s + 1 < NCH:
            prefetch_w2()
        for dc, dt in peers:
            home_copy(s, dc, dt).start()
        bk[s, blk(self_e), :] = zb[s, blk(self_e), :]

    ci = lax.broadcasted_iota(jnp.int32, (rb, rows), 1)
    g0 = column(g_ref, 0)[:, 0:1]
    g1 = column(g_ref, 1)[:, 0:1]
    for s in range(NCH):
        sel0 = jnp.where(ci + s * rows == code_ref[:, 0:1], 1.0, 0.0).astype(BF)
        sel1 = jnp.where(ci + s * rows == code_ref[:, 1:2], 1.0, 0.0).astype(BF)
        for dc, dt in peers:
            got_copy(s, dc, dt).wait_recv()

        def combine(i, _):
            cols = pl.ds(pl.multiple_of(i * 512, 512), 512)
            v = g0 * dot(sel0, bk[s, :, cols]) + g1 * dot(sel1, bk[s, :, cols])
            if s > 0:
                v = pin[:, cols] + v
            if s + 1 < NCH:
                pin[:, cols] = v
            else:
                y_ref[:, cols] = (h_ref[:, cols].astype(F32) + v).astype(BF)
            return 0

        lax.fori_loop(0, nc, combine, 0)

    for o in others:
        dd, cc, tt = rel(*o)
        src = (dd * ncp + cc) * ntp + tt
        rcopy(top, cnt.at[src], n_s.at[0], n_r.at[src], dd, cc, tt).wait_recv()
    mx_ref[...] = jnp.max(cnt[...], axis=0)

    for v in range(2):
        wy[v].wait_send()
    cx.wait_send()
    for i in range(2):
        yx[i].wait_send()
    for i, o in enumerate(others):
        dd, cc, tt = rel(*o)
        rcopy(top, cnt.at[me], n_s.at[i], n_r.at[me], dd, cc, tt).wait_send()
    for dc in zpeers:
        for i, (g, at, n) in enumerate([(mine, at_k, rb), (mine, at_c, rb),
                                        (other, at_k, hk), (other, pl.multiple_of(at_k + hk, hk), hk),
                                        (other, at_c, hk), (other, pl.multiple_of(at_c + hk, hk), hk)]):
            for cp_ in kv_copies(g, at, n, i, dc, True):
                cp_.wait_send()
    for cc in range(ncp):
        x_copy(cc, False, 0).wait_send()
    x_copy(c, False, 1).wait_send()
    x_copy(far, False, 1).wait_send()

    @pl.when(c == 0)
    def _():
        x_copy(2, False, 1).wait_send()

    @pl.when(c == ncp - 1)
    def _():
        x_copy(ncp - 3, False, 1).wait_send()

    @pl.when(c < ncp - 1)
    def _():
        up2_copy(c, c_up).wait_send()

    @pl.when(c > 0)
    def _():
        dn2_copy(c, c_dn).wait_send()

    for v in range(2):

        @pl.when(c < ncp - 1)
        def _():
            up_copy(c, c_up, v).wait_send()

        @pl.when(c > 0)
        def _():
            dn_copy(c, c_dn, v).wait_send()

        @pl.when(c == ncp - 2)
        def _():
            up_copy(c_dn, c_up, v).wait_send()

        @pl.when(c == 1)
        def _():
            dn_copy(c_up, c_dn, v).wait_send()
    wf.wait_send()
    for j in range(heads):
        o_copy(j).wait_send()
    for i in (nc - 2, nc - 1):
        p_copy(i).wait_send()
    for j in range(NCH):
        for dc, dt in peers:
            home_copy(j, dc, dt).wait_send()
    for n in range(len(cuts)):
        for dc, dt in peers:
            out_copy(n, dc, dt).wait_send()


def layer(x, wq, wk, wv, wo, idx, gates, wg, wu, wd, *, nd, ncp, ntp, cid):
    rb, hd = x.shape
    ql = wq.shape[1]
    seg = 2 * rb
    heads = ql // HD
    nseg = 2 * ncp
    n_all = nd * ncp * ntp
    ne = ncp * ntp
    ff = wg.shape[1]
    hbm = pl.BlockSpec(memory_space=pl.ANY)
    vm = pl.BlockSpec(memory_space=pltpu.VMEM)
    dma = pltpu.SemaphoreType.DMA
    V = pltpu.VMEM
    return pl.pallas_call(
        functools.partial(layer_kernel, nd=nd, ncp=ncp, ntp=ntp, scale=HD ** -0.5),
        in_specs=[hbm, hbm, hbm, hbm, hbm, vm, vm, hbm, hbm, hbm],
        out_specs=[vm, vm, vm, vm],
        out_shape=[jax.ShapeDtypeStruct((rb, hd), BF), jax.ShapeDtypeStruct((rb, hd), BF), jax.ShapeDtypeStruct((rb, 128), jnp.int32), jax.ShapeDtypeStruct((8, 128), F32)],
        scratch_shapes=[
            V((ntp, rb, hd), BF), V((hd, 1024), BF), V((hd, 2 * HD), BF), V((ql, hd), BF), V((ql, hd), BF),
            V((2, seg, ql), BF), V((nseg, seg, HD), BF), V((nseg, HD, seg), BF),
            V((2, seg, ql), BF), V((seg, ql), BF), V((2, rb, 512), F32), V((rb, hd), F32),
            V((n_all, 8, 128), F32), V((8, 128), F32), V((seg, seg), F32), V((seg, seg), F32), V((2, seg, seg), F32), V((HD, seg), F32),
            V((NCH, ne * CH, hd), BF), V((NCH, ne * CH, hd), BF), V((ne * CH, ff), BF), V((2, ff, 256), BF),
            dma((5,)), dma(()), dma(()), dma((2,)), dma((2,)), dma((2,)), dma((2,)),
            dma((ncp, 12)), dma((ncp, 12)), dma((2,)), dma((2,)), dma((ncp, 2)), dma((ncp, 2)),
            dma((ncp, 2)), dma((ncp, 2)), dma((ncp, 2)), dma((ncp, 2)), dma(()), dma(()), dma((2,)), dma((2,)), dma((heads,)), dma((heads,)),
            dma((hd // 512,)), dma((hd // 512,)), dma((n_all - 1,)), dma((n_all,)),
            dma((NCH + 1, ne)), dma((NCH + 1, ne)), dma((NCH, ne)), dma((NCH, ne)), dma((2, 2)), dma((2,)),
        ],
        compiler_params=pltpu.CompilerParams(collective_id=cid, has_side_effects=True, vmem_limit_bytes=VMEM_LIMIT),
        name="layer",
        cost_estimate=pl.CostEstimate(flops=60_000_000_000, bytes_accessed=30_000_000, transcendentals=0),
    )(x, wq, wk, wv, wo, idx.T, gates.T, wg, wu, wd)


def moe_kernel(h_ref, dc_ref, g_ref, wg_hbm, wu_hbm, wd_hbm, y_ref,
               send, recv, zbuf, back, act, w1buf, w2buf,
               ssem, rsem, zsem, bsem, w1sem, w2sem, *, ncp, ntp, nch, f1, f2):
    ne = ncp * ntp
    rows = ne * CH
    t, hd = h_ref.shape
    ff = wg_hbm.shape[1]
    n1, n2 = ff // f1, hd // f2
    r1, r2 = w1buf.shape[0], w2buf.shape[0]
    dp = lax.axis_index("dp")
    c = lax.axis_index("cp")
    p = lax.axis_index("tp")
    me = c * ntp + p

    order = [2, 1, 3, 0]
    peers = [(dc, dt) for dc in order[:ncp] for dt in range(ntp) if (dc, dt) != (0, 0)]

    def peer(dc, dt):
        pc = lax.rem(c + dc, ncp)
        pt = lax.rem(p + dt, ntp)
        return pc, pt, pc * ntp + pt

    def blk(e):
        return pl.ds(pl.multiple_of(e * CH, CH), CH)

    def out_copy(j, dc, dt):
        pc, pt, e = peer(dc, dt)
        return pltpu.make_async_remote_copy(send.at[j, blk(e)], recv.at[j, blk(me)], ssem.at[j, e], rsem.at[j, me],
                                            device_id=(dp, pc, pt), device_id_type=MESH)

    def in_copy(j, dc, dt):
        pc, pt, e = peer(dc, dt)
        return pltpu.make_async_remote_copy(send.at[j, blk(e)], recv.at[j, blk(e)], ssem.at[j, e], rsem.at[j, e],
                                            device_id=(dp, pc, pt), device_id_type=MESH)

    def home_copy(j, dc, dt):
        pc, pt, e = peer(dc, dt)
        return pltpu.make_async_remote_copy(zbuf.at[j, blk(e)], back.at[j, blk(me)], zsem.at[j, e], bsem.at[j, me],
                                            device_id=(dp, pc, pt), device_id_type=MESH)

    def got_copy(j, dc, dt):
        pc, pt, e = peer(dc, dt)
        return pltpu.make_async_remote_copy(zbuf.at[j, blk(e)], back.at[j, blk(e)], zsem.at[j, e], bsem.at[j, e],
                                            device_id=(dp, pc, pt), device_id_type=MESH)

    def w1_copies(s):
        slot = lax.rem(s, r1)
        cols = pl.ds(pl.multiple_of(s * f1, f1), f1)
        return (pltpu.make_async_copy(wg_hbm.at[:, cols], w1buf.at[slot, 0], w1sem.at[slot, 0]),
                pltpu.make_async_copy(wu_hbm.at[:, cols], w1buf.at[slot, 1], w1sem.at[slot, 1]))

    def w2_copy(s):
        slot = lax.rem(s, r2)
        cols = pl.ds(pl.multiple_of(s * f2, f2), f2)
        return pltpu.make_async_copy(wd_hbm.at[:, cols], w2buf.at[slot], w2sem.at[slot])

    def start_w1(s):
        for cp_ in w1_copies(s):
            cp_.start()

    def prefetch_w1():
        for s in range(r1):
            start_w1(jnp.int32(s))

    def prefetch_w2():
        for s in range(r2):
            w2_copy(jnp.int32(s)).start()

    prefetch_w1()
    prefetch_w2()

    barrier = pltpu.get_barrier_semaphore()
    for dc, dt in peers:
        pc, pt, _ = peer(dc, dt)
        pl.semaphore_signal(barrier, inc=1, device_id=(dp, pc, pt), device_id_type=MESH)
    pl.semaphore_wait(barrier, ne - 1)

    codes = dc_ref[...].astype(F32).T.astype(jnp.int32)

    for j in range(nch):
        ri = lax.broadcasted_iota(jnp.int32, (rows, t), 0) + j * rows
        sel = jnp.where(ri == codes[0:1, :], 1.0, 0.0) + jnp.where(ri == codes[1:2, :], 1.0, 0.0)
        sel = sel.astype(BF)

        def pick(i, _):
            cols = pl.ds(pl.multiple_of(i * 512, 512), 512)
            send[j, :, cols] = dot(sel, h_ref[:, cols]).astype(BF)
            return 0

        lax.fori_loop(0, hd // 512, pick, 0)
        for dc, dt in peers:
            out_copy(j, dc, dt).start()
        recv[j, blk(me), :] = send[j, blk(me), :]

    for j in range(nch):
        for dc, dt in peers:
            in_copy(j, dc, dt).wait_recv()

        def up(s, _):
            slot = lax.rem(s, r1)
            for cp_ in w1_copies(s):
                cp_.wait()
            xx = recv[j]
            gg = dot(xx, w1buf[slot, 0])
            uu = dot(xx, w1buf[slot, 1])
            act[:, pl.ds(pl.multiple_of(s * f1, f1), f1)] = (gg * jax.nn.sigmoid(gg) * uu).astype(BF)

            @pl.when(s + r1 < n1)
            def _():
                start_w1(s + r1)
            return 0

        lax.fori_loop(0, n1, up, 0)
        if j + 1 < nch:
            prefetch_w1()

        def down(s, _):
            slot = lax.rem(s, r2)
            w2_copy(s).wait()
            zbuf[j, :, pl.ds(pl.multiple_of(s * f2, f2), f2)] = dot(act[...], w2buf[slot]).astype(BF)

            @pl.when(s + r2 < n2)
            def _():
                w2_copy(s + r2).start()
            return 0

        lax.fori_loop(0, n2, down, 0)
        if j + 1 < nch:
            prefetch_w2()
        for dc, dt in peers:
            home_copy(j, dc, dt).start()
        back[j, blk(me), :] = zbuf[j, blk(me), :]

    for j in range(nch):
        for dc, dt in peers:
            got_copy(j, dc, dt).wait_recv()

    ci = lax.broadcasted_iota(jnp.int32, (t, rows), 1)
    sel0 = [jnp.where(ci + j * rows == dc_ref[:, 0:1], 1.0, 0.0).astype(BF) for j in range(nch)]
    sel1 = [jnp.where(ci + j * rows == dc_ref[:, 1:2], 1.0, 0.0).astype(BF) for j in range(nch)]
    g0 = g_ref[:, 0:1]
    g1 = g_ref[:, 1:2]

    def combine(i, _):
        cols = pl.ds(pl.multiple_of(i * 512, 512), 512)
        z0 = sum(dot(sel0[j], back[j, :, cols]) for j in range(nch))
        z1 = sum(dot(sel1[j], back[j, :, cols]) for j in range(nch))
        y_ref[:, cols] = (h_ref[:, cols].astype(F32) + (g0 * z0 + g1 * z1)).astype(BF)
        return 0

    lax.fori_loop(0, hd // 512, combine, 0)

    for j in range(nch):
        for dc, dt in peers:
            out_copy(j, dc, dt).wait_send()
            home_copy(j, dc, dt).wait_send()


def moe(h, code, gates, wg, wu, wd, *, ncp, ntp, nch, cid):
    t, hd = h.shape
    ff = wg.shape[1]
    ne = ncp * ntp
    rows = ne * CH
    f1, f2, r1, r2 = 256, 512, 2, 2
    vm = pl.BlockSpec(memory_space=pltpu.VMEM)
    hbm = pl.BlockSpec(memory_space=pl.ANY)
    dma = pltpu.SemaphoreType.DMA
    return pl.pallas_call(
        functools.partial(moe_kernel, ncp=ncp, ntp=ntp, nch=nch, f1=f1, f2=f2),
        in_specs=[vm, vm, vm, hbm, hbm, hbm],
        out_specs=vm,
        out_shape=jax.ShapeDtypeStruct((t, hd), BF),
        scratch_shapes=[
            pltpu.VMEM((nch, rows, hd), BF), pltpu.VMEM((nch, rows, hd), BF),
            pltpu.VMEM((nch, rows, hd), BF), pltpu.VMEM((nch, rows, hd), BF),
            pltpu.VMEM((rows, ff), BF),
            pltpu.VMEM((r1, 2, hd, f1), BF), pltpu.VMEM((r2, ff, f2), BF),
            dma((nch, ne)), dma((nch, ne)), dma((nch, ne)), dma((nch, ne)),
            dma((r1, 2)), dma((r2,)),
        ],
        compiler_params=pltpu.CompilerParams(collective_id=cid, has_side_effects=True, vmem_limit_bytes=VMEM_LIMIT),
        name=f"moe{nch}",
        cost_estimate=pl.CostEstimate(flops=6 * nch * rows * hd * ff, bytes_accessed=6 * nch * hd * ff, transcendentals=0),
    )(h, code, gates, wg, wu, wd)


def solution(mesh):
    ncp = mesh.shape["cp"]
    ntp = mesh.shape["tp"]
    rows_spec = P(("dp", "cp", "tp"), None)
    exp_spec = P(("cp", "tp"), None, None)

    def local(x, idx, gates, wq, wk, wv, wo, w1g, w1u, w2):
        y, h, code, most = layer(x, wq, wk, wv, wo, idx, gates, w1g[0], w1u[0], w2[0], nd=mesh.shape["dp"], ncp=ncp, ntp=ntp, cid=3)

        def few(args):
            return y

        def many(args):
            return moe(*args, ncp=ncp, ntp=ntp, nch=4, cid=2)

        return lax.cond(most[0, 0] <= NCH * CH, few, many, (h, code, gates, w1g[0], w1u[0], w2[0]))

    return jax.shard_map(local, mesh=mesh, in_specs=(rows_spec, rows_spec, rows_spec, P(None, "tp"), P(None, "tp"), P(None, "tp"), P("tp", None), exp_spec, exp_spec, exp_spec), out_specs=rows_spec, check_vma=False)
```

```python
import functools

import jax
import jax.numpy as jnp
from jax import lax
from jax.experimental import pallas as pl
from jax.experimental.pallas import tpu as pltpu
from jax.sharding import PartitionSpec as P

HD = 128
NEG = -1e30
BF = jnp.bfloat16
F32 = jnp.float32
MESH = pl.DeviceIdType.MESH
VMEM_LIMIT = 67_000_000
CH = 16
NCH = 2


def dot(a, b):
    return jnp.dot(a, b, preferred_element_type=F32)


def layer_kernel(x_hbm, wq_hbm, wk_hbm, wv_hbm, wo_hbm, idx_ref, g_ref, wg_hbm, wu_hbm, wd_hbm,
                 y_ref, h_ref, code_ref, mx_ref,
               xs, wq, wkv, wo_a, wo_b, qq, kb, vt, oo, o_b, part, pin, cnt, top, s0, s1, bias, acc,
               send, recv, act, w2buf,
               lsem, cx_s, cx_r, yx_s, yx_r, fx_s, fx_r, kv_s, kv_r, wy_s, wy_r, wx_s, wx_r,
               wu_s, wu_r, wd_s, wd_r, wf_s, wf_r, wc_s, wc_r, o_ss, o_rs, p_ss, p_rs, n_s, n_r, ssem, rsem, zsem, bsem, w1sem, w2sem, *, nd, ncp, ntp, scale):
    d = lax.axis_index("dp")
    c = lax.axis_index("cp")
    t = lax.axis_index("tp")
    y = t // 2
    k = lax.rem(t, 2)
    t_c = 2 * y + 1 - k
    t_y = 2 * (1 - y) + k
    t_z = 2 * (1 - y) + 1 - k
    rb = xs.shape[1]
    hd = xs.shape[2]
    seg = 2 * rb
    hk = rb // 2
    heads = qq.shape[2] // HD
    q_a, q_b, o_a, o_s = qq.at[0], qq.at[1], oo.at[0], oo.at[1]
    pr = wo_a.shape[0] // (nd * ncp)
    last = 2 * ncp - 1
    mine = jnp.where(y == 0, c, last - c)
    other = last - mine
    me = (d * ncp + c) * ntp + t

    def rcopy(src, dst, ss, rs, dd, cc, tt):
        return pltpu.make_async_remote_copy(src, dst, ss, rs, device_id=(dd, cc, tt), device_id_type=MESH)

    loads = [
        pltpu.make_async_copy(wk_hbm, wkv.at[:, 0:HD], lsem.at[0]),
        pltpu.make_async_copy(wv_hbm, wkv.at[:, HD:2 * HD], lsem.at[1]),
        pltpu.make_async_copy(x_hbm, xs.at[t], lsem.at[2]),
        pltpu.make_async_copy(wq_hbm, wq.at[:, 0:wq_hbm.shape[1]], lsem.at[3]),
        pltpu.make_async_copy(wo_hbm, wo_a, lsem.at[4]),
    ]
    for cp_ in loads:
        cp_.start()

    n_all = nd * ncp * ntp
    others = [(a, b, e) for a in range(nd) for b in range(ncp) for e in range(ntp) if (a, b, e) != (0, 0, 0)]

    def rel(a, b, e):
        return lax.rem(d + a, nd), lax.rem(c + b, ncp), lax.rem(t + e, ntp)

    barrier = pltpu.get_barrier_semaphore()
    for o in others:
        pl.semaphore_signal(barrier, inc=1, device_id=rel(*o), device_id_type=MESH)
    pl.semaphore_wait(barrier, n_all - 1)

    def piece(dd, cc):
        return pl.ds(pl.multiple_of((dd * ncp + cc) * pr, pr), pr)

    def half(i):
        return pl.ds(i * hk, hk)

    def cols2(v):
        return pl.ds(v * (hd // 2), hd // 2)

    def wo_cut(ref, dd, cc, v):
        return ref.at[piece(dd, cc), cols2(v)]

    wy = [rcopy(wo_cut(wo_hbm, d, c, v), wo_cut(wo_b, d, c, v), wy_s.at[v], wy_r.at[v], d, c, t_y) for v in range(2)]
    yx = [rcopy(x_hbm.at[half(i)], xs.at[t, half(i)], yx_s.at[i], yx_r.at[i], d, c, t_y) for i in range(2)]
    yx_in = [rcopy(x_hbm.at[half(i)], xs.at[t_y, half(i)], yx_s.at[i], yx_r.at[i], d, c, t_y) for i in range(2)]
    far = jnp.where(c < ncp // 2, ncp - 1, 0)
    wf = rcopy(wo_hbm.at[piece(d, far)], wo_b.at[piece(d, far)], wf_s, wf_r, d, c, t_y)

    wy[0].start()
    for cp_ in yx:
        cp_.start()
    wy[1].start()
    wf.start()
    cx = rcopy(x_hbm, xs.at[t], cx_s, cx_r, d, c, t_c)
    cx_in = rcopy(x_hbm, xs.at[t_c], cx_s, cx_r, d, c, t_c)
    cx.start()

    ne = ncp * ntp
    lane = lax.broadcasted_iota(jnp.int32, (rb, 128), 1)

    def column(ref, i):
        return jnp.broadcast_to(ref[i:i + 1, :].astype(F32), (128, rb)).T

    e0, e1 = column(idx_ref, 0).astype(jnp.int32), column(idx_ref, 1).astype(jnp.int32)
    oh0 = jnp.where(lane == e0, 1.0, 0.0)
    oh1 = jnp.where(lane == e1, 1.0, 0.0)
    both = oh0 + oh1
    tri = jnp.where(lax.broadcasted_iota(jnp.int32, (rb, rb), 1) < lax.broadcasted_iota(jnp.int32, (rb, rb), 0), 1.0, 0.0)
    before = dot(tri.astype(BF), both.astype(BF))

    def place(oh, e):
        slot = jnp.sum(before * oh, axis=1, keepdims=True).astype(jnp.int32)
        ch = lax.shift_right_logical(slot, CH.bit_length() - 1)
        return ch * (ne * CH) + e * CH + (slot - ch * CH)

    code_ref[...] = jnp.where(lane == 0, place(oh0, e0), place(oh1, e1))
    top[...] = jnp.zeros(top.shape, F32) + jnp.max(jnp.sum(both, axis=0, keepdims=True), axis=1, keepdims=True)
    cnt[me] = top[...]
    for i, o in enumerate(others):
        dd, cc, tt = rel(*o)
        rcopy(top, cnt.at[me], n_s.at[i], n_r.at[me], dd, cc, tt).start()

    zpeers = list(range(1, ncp))

    def kv_copies(g, at, n, i, dc, here):
        cc = lax.rem(c + dc, ncp)
        src = c if here else cc
        rows = pl.ds(at, n)
        return (rcopy(kb.at[g, rows], kb.at[g, rows], kv_s.at[cc, 2 * i], kv_r.at[src, 2 * i], d, cc, t),
                rcopy(vt.at[g, :, rows], vt.at[g, :, rows], kv_s.at[cc, 2 * i + 1], kv_r.at[src, 2 * i + 1], d, cc, t))

    def kv_rows(g, at, n, src):
        r = dot(src, wkv[...])
        kb[g, pl.ds(at, n), :] = r[:, :HD].astype(BF)
        vt[g, :, pl.ds(at, n)] = r[:, HD:].astype(BF).T

    def kv_send(g, at, n, i):
        for dc in zpeers:
            for cp_ in kv_copies(g, at, n, i, dc, True):
                cp_.start()

    at_k = pl.multiple_of(k * rb, rb)
    at_c = pl.multiple_of((1 - k) * rb, rb)

    ki = lax.broadcasted_iota(jnp.int32, (seg, seg), 0)
    qi = lax.broadcasted_iota(jnp.int32, (seg, seg), 1)
    bias[0] = jnp.zeros((seg, seg), F32)
    bias[1] = jnp.where(ki <= qi, 0.0, NEG)

    for i in (0, 1, 2):
        loads[i].wait()
    kv_rows(mine, at_k, rb, xs[t])
    kv_send(mine, at_k, rb, 0)
    cx_in.wait_recv()
    kv_rows(mine, at_c, rb, xs[t_c])
    kv_send(mine, at_c, rb, 1)
    loads[3].wait()

    def q_rows(q_ref, at, src):
        for lo in range(0, heads * HD, 256):
            hi = min(lo + 256, heads * HD)
            q_ref[pl.ds(at, rb), lo:hi] = dot(src, wq[:, lo:hi]).astype(BF)

    q_rows(q_a, at_k, xs[t])
    q_rows(q_a, at_c, xs[t_c])

    def x_copy(cc, there, v):
        dd = 1 - d if there else d
        return rcopy(wo_cut(wo_b, dd, cc, v), wo_cut(wo_b, dd, cc, v), wx_s.at[cc, v], wx_r.at[cc, v], 1 - d, c, t)

    def up_copy(cc, to, v):
        return rcopy(wo_cut(wo_b, d, cc, v), wo_cut(wo_b, d, cc, v), wu_s.at[cc, v], wu_r.at[cc, v], d, to, t)

    def dn_copy(cc, to, v):
        return rcopy(wo_cut(wo_b, d, cc, v), wo_cut(wo_b, d, cc, v), wd_s.at[cc, v], wd_r.at[cc, v], d, to, t)

    def up2_copy(cc, to):
        return rcopy(wo_cut(wo_b, 1 - d, cc, 1), wo_cut(wo_b, 1 - d, cc, 1), wc_s.at[0], wc_r.at[0], d, to, t)

    def dn2_copy(cc, to):
        return rcopy(wo_cut(wo_b, 1 - d, cc, 1), wo_cut(wo_b, 1 - d, cc, 1), wc_s.at[1], wc_r.at[1], d, to, t)

    c_up = jnp.minimum(c + 1, ncp - 1)
    c_dn = jnp.maximum(c - 1, 0)

    def wo_first(v):
        wy[v].wait_recv()
        x_copy(c, False, v).start()

        @pl.when(c < ncp - 1)
        def _():
            up_copy(c, c_up, v).start()

        @pl.when(c > 0)
        def _():
            dn_copy(c, c_dn, v).start()

    def wo_near(v):
        @pl.when(c > 0)
        def _():
            up_copy(c_dn, c_dn, v).wait_recv()

            @pl.when(c == ncp - 2)
            def _():
                up_copy(c_dn, c_up, v).start()
            if v == 0:
                x_copy(c_dn, False, v).start()

        @pl.when(c < ncp - 1)
        def _():
            dn_copy(c_up, c_up, v).wait_recv()

            @pl.when(c == 1)
            def _():
                dn_copy(c_up, c_dn, v).start()
            if v == 0:
                x_copy(c_up, False, v).start()

    def wo_cross():
        x_copy(c, True, 1).wait_recv()

        @pl.when(c < ncp - 1)
        def _():
            up2_copy(c, c_up).start()

        @pl.when(c > 0)
        def _():
            dn2_copy(c, c_dn).start()

    def wo_ends(v):
        @pl.when(c == ncp - 1)
        def _():
            up_copy(ncp - 3, c_dn, v).wait_recv()
            x_copy(ncp - 3, False, v).start()

        @pl.when(c == 0)
        def _():
            dn_copy(2, c_up, v).wait_recv()
            x_copy(2, False, v).start()

    def wo_far():
        wf.wait_recv()
        for v in range(2):
            x_copy(far, False, v).start()


    zb, bk = xs.at[2:4], xs.at[0:2]
    ff = wg_hbm.shape[1]
    f1, f2 = wq.shape[1] // 4, w2buf.shape[2]
    n1, n2 = ff // f1, hd // f2
    self_e = c * ntp + t
    rows = ne * CH
    peers = [(dc, dt) for dc in [2, 1, 3, 0] for dt in range(ntp) if (dc, dt) != (0, 0)]

    def blk(e):
        return pl.ds(pl.multiple_of(e * CH, CH), CH)

    def peer(dc, dt):
        pc = lax.rem(c + dc, ncp)
        pt = lax.rem(t + dt, ntp)
        return pc, pt, pc * ntp + pt

    early = 1024
    cuts = [(0, 0, early), (0, early, hd)] + [(j, 0, hd) for j in range(1, NCH)]

    def out_copy(n, dc, dt):
        pc, pt, e = peer(dc, dt)
        j, lo, hi = cuts[n]
        return rcopy(send.at[j, blk(e), lo:hi], recv.at[j, blk(self_e), lo:hi], ssem.at[n, e], rsem.at[n, self_e], d, pc, pt)

    def in_copy(n, dc, dt):
        pc, pt, e = peer(dc, dt)
        j, lo, hi = cuts[n]
        return rcopy(send.at[j, blk(e), lo:hi], recv.at[j, blk(e), lo:hi], ssem.at[n, e], rsem.at[n, e], d, pc, pt)

    def home_copy(j, dc, dt):
        pc, pt, e = peer(dc, dt)
        return rcopy(zb.at[j, blk(e)], bk.at[j, blk(self_e)], zsem.at[j, e], bsem.at[j, self_e], d, pc, pt)

    def got_copy(j, dc, dt):
        pc, pt, e = peer(dc, dt)
        return rcopy(zb.at[j, blk(e)], bk.at[j, blk(e)], zsem.at[j, e], bsem.at[j, e], d, pc, pt)

    def w1_copies(s):
        slot = lax.rem(s, 2)
        cols = pl.ds(pl.multiple_of(s * f1, f1), f1)
        return (pltpu.make_async_copy(wg_hbm.at[:, cols], wq.at[:, pl.ds(pl.multiple_of(slot * 2 * f1, f1), f1)], w1sem.at[slot, 0]),
                pltpu.make_async_copy(wu_hbm.at[:, cols], wq.at[:, pl.ds(pl.multiple_of(slot * 2 * f1 + f1, f1), f1)], w1sem.at[slot, 1]))

    def w2_copy(s):
        slot = lax.rem(s, 2)
        cols = pl.ds(pl.multiple_of(s * f2, f2), f2)
        return pltpu.make_async_copy(wd_hbm.at[:, cols], w2buf.at[slot], w2sem.at[slot])

    def prefetch_w1():
        for s in range(2):
            for cp_ in w1_copies(jnp.int32(s)):
                cp_.start()

    def prefetch_w2():
        for s in range(2):
            w2_copy(jnp.int32(s)).start()

    def dispatch(ns):
        codes = code_ref[...].astype(F32).T.astype(jnp.int32)
        for n in ns:
            j, lo, hi = cuts[n]
            ri = lax.broadcasted_iota(jnp.int32, (rows, rb), 0) + j * rows
            sel = (jnp.where(ri == codes[0:1, :], 1.0, 0.0) + jnp.where(ri == codes[1:2, :], 1.0, 0.0)).astype(BF)

            def pick(i, _):
                cols = pl.ds(pl.multiple_of(i * 512, 512), 512)
                send[j, :, cols] = dot(sel, h_ref[:, cols]).astype(BF)
                return 0

            lax.fori_loop(lo // 512, hi // 512, pick, 0)
            for dc, dt in peers:
                out_copy(n, dc, dt).start()
            recv[j, blk(self_e), lo:hi] = send[j, blk(self_e), lo:hi]

    cw = seg // 2

    def o_copy(j):
        cols = pl.ds(pl.multiple_of(j * HD, HD), HD)
        return rcopy(o_s.at[:, cols], o_b.at[:, cols], o_ss.at[j], o_rs.at[j], d, c, t_y)

    def attend(hf, count, points):
        n = count + 1

        def following(j, g):
            wrap = g == n - 1
            return jnp.minimum(j + jnp.where(wrap, 1, 0), heads - 1), jnp.where(wrap, 0, g + 1)

        def score(j, g, s_ref):
            diag = jnp.where(g == n - 1, 1, 0)
            qb = qq[hf, :, pl.ds(pl.multiple_of(j * HD, HD), HD)]
            tops = []
            for lo in range(0, seg, cw):
                v = lax.dot_general(kb[g], qb[lo:lo + cw], (((1,), (1,)), ((), ())), preferred_element_type=F32) * scale
                v = v + bias[diag, :, lo:lo + cw]
                s_ref[:, lo:lo + cw] = v
                tops.append(jnp.max(v, axis=0, keepdims=True))
            return tuple(tops)

        def soft(j, g, s_ref, tops, ms, ls):
            first = g == 0
            nm, nl = [], []
            for n_, lo in enumerate(range(0, seg, cw)):
                m = jnp.where(first, NEG, ms[n_])
                mn = jnp.maximum(m, tops[n_])
                w = jnp.exp(s_ref[:, lo:lo + cw] - mn)
                a = jnp.exp(m - mn)
                nl.append(jnp.where(first, 0.0, ls[n_]) * a + jnp.sum(w, axis=0, keepdims=True))
                acc[:, lo:lo + cw] = acc[:, lo:lo + cw] * a + dot(vt[g], w.astype(BF))
                nm.append(mn)
            return tuple(nm), tuple(nl)

        def finish(j, g, ls):
            hcols = pl.ds(pl.multiple_of(j * HD, HD), HD)

            @pl.when(g == n - 1)
            def _():
                for n_, lo in enumerate(range(0, seg, cw)):
                    oo[hf, lo:lo + cw, hcols] = (acc[:, lo:lo + cw] / ls[n_]).T.astype(BF)

            @pl.when((g == n - 1) & (hf == 1))
            def _():
                o_copy(j).start()

        def pair(u, carry):
            j0, g0, tops, ms, ls = carry
            j1, g1 = following(j0, g0)
            t1 = score(j1, g1, s1)
            ms, ls = soft(j0, g0, s0, tops, ms, ls)
            finish(j0, g0, ls)
            j2, g2 = following(j1, g1)
            t0 = score(j2, g2, s0)
            ms, ls = soft(j1, g1, s1, t1, ms, ls)
            finish(j1, g1, ls)
            return j2, g2, t0, ms, ls

        acc[...] = jnp.zeros(acc.shape, F32)
        z1 = (jnp.zeros((1, cw), F32),) * 2
        zero = jnp.int32(0)
        total = heads * n
        carry = (zero, zero, score(zero, zero, s0), z1, z1)
        at = 0
        for stop, here, point in points:
            stop = jnp.minimum(stop, total // 2)
            carry = lax.fori_loop(at, stop, pair, carry)
            pl.when(here)(point)
            at = stop
        j, g, tops, ms, ls = lax.fori_loop(at, total // 2, pair, carry)

        @pl.when(lax.rem(total, 2) == 1)
        def _():
            _, l2 = soft(j, g, s0, tops, ms, ls)
            finish(j, g, l2)

    def kv_wait(which):
        for dc in zpeers:
            cc = lax.rem(c + dc, ncp)
            gm = jnp.where(y == 0, cc, last - cc)
            go = last - gm
            if which == 0:
                parts = [(0, gm, at_k, rb), (1, gm, at_c, rb)]
            else:
                parts = [(2, go, at_k, hk), (3, go, pl.multiple_of(at_k + hk, hk), hk),
                         (4, go, at_c, hk), (5, go, pl.multiple_of(at_c + hk, hk), hk)]
            for i, g, at, n in parts:
                for cp_ in kv_copies(g, at, n, i, dc, False):
                    cp_.wait_recv()

    wo_first(0)

    for i in range(2):
        yx_in[i].wait_recv()
        fwd = rcopy(xs.at[t_y, half(i)], xs.at[t_y, half(i)], fx_s.at[i], fx_r.at[i], d, c, t_c)
        fwd.start()
        a0 = pl.multiple_of(at_k + i * hk, hk)
        kv_rows(other, a0, hk, xs[t_y, i * hk:(i + 1) * hk])
        kv_send(other, a0, hk, 2 + i)
        rcopy(xs.at[t_z, half(i)], xs.at[t_z, half(i)], fx_s.at[i], fx_r.at[i], d, c, t_c).wait_recv()
        a1 = pl.multiple_of(at_c + i * hk, hk)
        kv_rows(other, a1, hk, xs[t_z, i * hk:(i + 1) * hk])
        kv_send(other, a1, hk, 4 + i)
        if i == 0:
            wo_near(0)
    q_rows(q_b, at_k, xs[t_y])
    q_rows(q_b, at_c, xs[t_z])

    prefetch_w1()
    prefetch_w2()
    wo_ends(0)
    kv_wait(0)
    wo_first(1)
    kv_wait(1)
    points = [(4, wo_cross), (5, lambda: wo_near(1)), (13, wo_far), (26, lambda: wo_ends(1))]
    done = heads * (other + 1) // 2
    attend(1, other, [(stop, stop <= done, point) for stop, point in points])
    attend(0, mine, [(jnp.maximum(stop - done, 0), stop > done, point) for stop, point in points])

    def finish_rows():
        for cc in range(ncp):
            x_copy(cc, True, 0).wait_recv()
        loads[4].wait()
        for j in range(heads):
            o_copy(j).wait_recv()
        for i in range(2):
            rcopy(xs.at[t_y, half(i)], xs.at[t_y, half(i)], fx_s.at[i], fx_r.at[i], d, c, t_c).wait_send()
        ahead = early // 512
        lax.fori_loop(0, ahead + 1, give, 0)
        lax.fori_loop(0, ahead, keep, 0)
        dispatch([0])

        x_copy(far, True, 1).wait_recv()

        @pl.when(c == 0)
        def _():
            x_copy(2, True, 1).wait_recv()

        @pl.when(c == ncp - 1)
        def _():
            x_copy(ncp - 3, True, 1).wait_recv()

        @pl.when(c > 0)
        def _():
            up2_copy(c_dn, c_dn).wait_recv()

        @pl.when(c < ncp - 1)
        def _():
            dn2_copy(c_up, c_up).wait_recv()
        lax.fori_loop(ahead + 1, nc, give, 0)
        lax.fori_loop(ahead, nc, keep, 0)
        dispatch(range(1, len(cuts)))

    nc = hd // 512
    def p_copy(i):
        cols = pl.ds(pl.multiple_of(i * 512, 512), 512)
        return rcopy(part.at[lax.rem(i, 2)], pin.at[:, cols], p_ss.at[i], p_rs.at[i], d, c, t_c)

    def proj(at, cols):
        rows = pl.ds(at, rb)
        return dot(o_a[rows, :], wo_a[:, cols]) + dot(o_b[rows, :], wo_b[:, cols])

    def give(i, _):
        cols = pl.ds(pl.multiple_of(i * 512, 512), 512)
        v = proj(at_c, cols)

        @pl.when(i >= 2)
        def _():
            p_copy(i - 2).wait_send()
        part[lax.rem(i, 2)] = v
        p_copy(i).start()
        return 0

    def keep(i, _):
        cols = pl.ds(pl.multiple_of(i * 512, 512), 512)
        own = proj(at_k, cols)
        p_copy(i).wait_recv()
        h_ref[:, cols] = (xs[t, :, cols].astype(F32) + (own + pin[:, cols])).astype(BF)
        return 0


    finish_rows()

    for s in range(NCH):
        for n in range(len(cuts)):
            if cuts[n][0] == s:
                for dc, dt in peers:
                    in_copy(n, dc, dt).wait_recv()

        def up(i, _):
            for cp_ in w1_copies(i):
                cp_.wait()
            at = pl.multiple_of(lax.rem(i, 2) * 2 * f1, f1)
            xx = recv[s]
            gg = dot(xx, wq[:, pl.ds(at, f1)])
            uu = dot(xx, wq[:, pl.ds(pl.multiple_of(at + f1, f1), f1)])
            act[:, pl.ds(pl.multiple_of(i * f1, f1), f1)] = (gg * jax.nn.sigmoid(gg) * uu).astype(BF)

            @pl.when(i + 2 < n1)
            def _():
                for cp_ in w1_copies(i + 2):
                    cp_.start()
            return 0

        lax.fori_loop(0, n1, up, 0)
        if s + 1 < NCH:
            prefetch_w1()

        def down(i, _):
            w2_copy(i).wait()
            zb[s, :, pl.ds(pl.multiple_of(i * f2, f2), f2)] = dot(act[...], w2buf[lax.rem(i, 2)]).astype(BF)

            @pl.when(i + 2 < n2)
            def _():
                w2_copy(i + 2).start()
            return 0

        lax.fori_loop(0, n2, down, 0)
        if s + 1 < NCH:
            prefetch_w2()
        for dc, dt in peers:
            home_copy(s, dc, dt).start()
        bk[s, blk(self_e), :] = zb[s, blk(self_e), :]

    ci = lax.broadcasted_iota(jnp.int32, (rb, rows), 1)
    g0 = column(g_ref, 0)[:, 0:1]
    g1 = column(g_ref, 1)[:, 0:1]
    for s in range(NCH):
        sel0 = jnp.where(ci + s * rows == code_ref[:, 0:1], 1.0, 0.0).astype(BF)
        sel1 = jnp.where(ci + s * rows == code_ref[:, 1:2], 1.0, 0.0).astype(BF)
        for dc, dt in peers:
            got_copy(s, dc, dt).wait_recv()

        def combine(i, _):
            cols = pl.ds(pl.multiple_of(i * 512, 512), 512)
            v = g0 * dot(sel0, bk[s, :, cols]) + g1 * dot(sel1, bk[s, :, cols])
            if s > 0:
                v = pin[:, cols] + v
            if s + 1 < NCH:
                pin[:, cols] = v
            else:
                y_ref[:, cols] = (h_ref[:, cols].astype(F32) + v).astype(BF)
            return 0

        lax.fori_loop(0, nc, combine, 0)

    for o in others:
        dd, cc, tt = rel(*o)
        src = (dd * ncp + cc) * ntp + tt
        rcopy(top, cnt.at[src], n_s.at[0], n_r.at[src], dd, cc, tt).wait_recv()
    mx_ref[...] = jnp.max(cnt[...], axis=0)

    for v in range(2):
        wy[v].wait_send()
    cx.wait_send()
    for i in range(2):
        yx[i].wait_send()
    for i, o in enumerate(others):
        dd, cc, tt = rel(*o)
        rcopy(top, cnt.at[me], n_s.at[i], n_r.at[me], dd, cc, tt).wait_send()
    for dc in zpeers:
        for i, (g, at, n) in enumerate([(mine, at_k, rb), (mine, at_c, rb),
                                        (other, at_k, hk), (other, pl.multiple_of(at_k + hk, hk), hk),
                                        (other, at_c, hk), (other, pl.multiple_of(at_c + hk, hk), hk)]):
            for cp_ in kv_copies(g, at, n, i, dc, True):
                cp_.wait_send()
    for cc in range(ncp):
        x_copy(cc, False, 0).wait_send()
    x_copy(c, False, 1).wait_send()
    x_copy(far, False, 1).wait_send()

    @pl.when(c == 0)
    def _():
        x_copy(2, False, 1).wait_send()

    @pl.when(c == ncp - 1)
    def _():
        x_copy(ncp - 3, False, 1).wait_send()

    @pl.when(c < ncp - 1)
    def _():
        up2_copy(c, c_up).wait_send()

    @pl.when(c > 0)
    def _():
        dn2_copy(c, c_dn).wait_send()

    for v in range(2):

        @pl.when(c < ncp - 1)
        def _():
            up_copy(c, c_up, v).wait_send()

        @pl.when(c > 0)
        def _():
            dn_copy(c, c_dn, v).wait_send()

        @pl.when(c == ncp - 2)
        def _():
            up_copy(c_dn, c_up, v).wait_send()

        @pl.when(c == 1)
        def _():
            dn_copy(c_up, c_dn, v).wait_send()
    wf.wait_send()
    for j in range(heads):
        o_copy(j).wait_send()
    for i in (nc - 2, nc - 1):
        p_copy(i).wait_send()
    for j in range(NCH):
        for dc, dt in peers:
            home_copy(j, dc, dt).wait_send()
    for n in range(len(cuts)):
        for dc, dt in peers:
            out_copy(n, dc, dt).wait_send()


def layer(x, wq, wk, wv, wo, idx, gates, wg, wu, wd, *, nd, ncp, ntp, cid):
    rb, hd = x.shape
    ql = wq.shape[1]
    seg = 2 * rb
    heads = ql // HD
    nseg = 2 * ncp
    n_all = nd * ncp * ntp
    ne = ncp * ntp
    ff = wg.shape[1]
    hbm = pl.BlockSpec(memory_space=pl.ANY)
    vm = pl.BlockSpec(memory_space=pltpu.VMEM)
    dma = pltpu.SemaphoreType.DMA
    V = pltpu.VMEM
    return pl.pallas_call(
        functools.partial(layer_kernel, nd=nd, ncp=ncp, ntp=ntp, scale=HD ** -0.5),
        in_specs=[hbm, hbm, hbm, hbm, hbm, vm, vm, hbm, hbm, hbm],
        out_specs=[vm, vm, vm, vm],
        out_shape=[jax.ShapeDtypeStruct((rb, hd), BF), jax.ShapeDtypeStruct((rb, hd), BF), jax.ShapeDtypeStruct((rb, 128), jnp.int32), jax.ShapeDtypeStruct((8, 128), F32)],
        scratch_shapes=[
            V((ntp, rb, hd), BF), V((hd, 1024), BF), V((hd, 2 * HD), BF), V((ql, hd), BF), V((ql, hd), BF),
            V((2, seg, ql), BF), V((nseg, seg, HD), BF), V((nseg, HD, seg), BF),
            V((2, seg, ql), BF), V((seg, ql), BF), V((2, rb, 512), F32), V((rb, hd), F32),
            V((n_all, 8, 128), F32), V((8, 128), F32), V((seg, seg), F32), V((seg, seg), F32), V((2, seg, seg), F32), V((HD, seg), F32),
            V((NCH, ne * CH, hd), BF), V((NCH, ne * CH, hd), BF), V((ne * CH, ff), BF), V((2, ff, 256), BF),
            dma((5,)), dma(()), dma(()), dma((2,)), dma((2,)), dma((2,)), dma((2,)),
            dma((ncp, 12)), dma((ncp, 12)), dma((2,)), dma((2,)), dma((ncp, 2)), dma((ncp, 2)),
            dma((ncp, 2)), dma((ncp, 2)), dma((ncp, 2)), dma((ncp, 2)), dma(()), dma(()), dma((2,)), dma((2,)), dma((heads,)), dma((heads,)),
            dma((hd // 512,)), dma((hd // 512,)), dma((n_all - 1,)), dma((n_all,)),
            dma((NCH + 1, ne)), dma((NCH + 1, ne)), dma((NCH, ne)), dma((NCH, ne)), dma((2, 2)), dma((2,)),
        ],
        compiler_params=pltpu.CompilerParams(collective_id=cid, has_side_effects=True, vmem_limit_bytes=VMEM_LIMIT),
        name="layer",
        cost_estimate=pl.CostEstimate(flops=60_000_000_000, bytes_accessed=30_000_000, transcendentals=0),
    )(x, wq, wk, wv, wo, idx.T, gates.T, wg, wu, wd)


def moe_kernel(h_ref, dc_ref, g_ref, wg_hbm, wu_hbm, wd_hbm, y_ref,
               send, recv, zbuf, back, act, w1buf, w2buf,
               ssem, rsem, zsem, bsem, w1sem, w2sem, *, ncp, ntp, nch, f1, f2):
    ne = ncp * ntp
    rows = ne * CH
    t, hd = h_ref.shape
    ff = wg_hbm.shape[1]
    n1, n2 = ff // f1, hd // f2
    r1, r2 = w1buf.shape[0], w2buf.shape[0]
    dp = lax.axis_index("dp")
    c = lax.axis_index("cp")
    p = lax.axis_index("tp")
    me = c * ntp + p

    order = [2, 1, 3, 0]
    peers = [(dc, dt) for dc in order[:ncp] for dt in range(ntp) if (dc, dt) != (0, 0)]

    def peer(dc, dt):
        pc = lax.rem(c + dc, ncp)
        pt = lax.rem(p + dt, ntp)
        return pc, pt, pc * ntp + pt

    def blk(e):
        return pl.ds(pl.multiple_of(e * CH, CH), CH)

    def out_copy(j, dc, dt):
        pc, pt, e = peer(dc, dt)
        return pltpu.make_async_remote_copy(send.at[j, blk(e)], recv.at[j, blk(me)], ssem.at[j, e], rsem.at[j, me],
                                            device_id=(dp, pc, pt), device_id_type=MESH)

    def in_copy(j, dc, dt):
        pc, pt, e = peer(dc, dt)
        return pltpu.make_async_remote_copy(send.at[j, blk(e)], recv.at[j, blk(e)], ssem.at[j, e], rsem.at[j, e],
                                            device_id=(dp, pc, pt), device_id_type=MESH)

    def home_copy(j, dc, dt):
        pc, pt, e = peer(dc, dt)
        return pltpu.make_async_remote_copy(zbuf.at[j, blk(e)], back.at[j, blk(me)], zsem.at[j, e], bsem.at[j, me],
                                            device_id=(dp, pc, pt), device_id_type=MESH)

    def got_copy(j, dc, dt):
        pc, pt, e = peer(dc, dt)
        return pltpu.make_async_remote_copy(zbuf.at[j, blk(e)], back.at[j, blk(e)], zsem.at[j, e], bsem.at[j, e],
                                            device_id=(dp, pc, pt), device_id_type=MESH)

    def w1_copies(s):
        slot = lax.rem(s, r1)
        cols = pl.ds(pl.multiple_of(s * f1, f1), f1)
        return (pltpu.make_async_copy(wg_hbm.at[:, cols], w1buf.at[slot, 0], w1sem.at[slot, 0]),
                pltpu.make_async_copy(wu_hbm.at[:, cols], w1buf.at[slot, 1], w1sem.at[slot, 1]))

    def w2_copy(s):
        slot = lax.rem(s, r2)
        cols = pl.ds(pl.multiple_of(s * f2, f2), f2)
        return pltpu.make_async_copy(wd_hbm.at[:, cols], w2buf.at[slot], w2sem.at[slot])

    def start_w1(s):
        for cp_ in w1_copies(s):
            cp_.start()

    def prefetch_w1():
        for s in range(r1):
            start_w1(jnp.int32(s))

    def prefetch_w2():
        for s in range(r2):
            w2_copy(jnp.int32(s)).start()

    prefetch_w1()
    prefetch_w2()

    barrier = pltpu.get_barrier_semaphore()
    for dc, dt in peers:
        pc, pt, _ = peer(dc, dt)
        pl.semaphore_signal(barrier, inc=1, device_id=(dp, pc, pt), device_id_type=MESH)
    pl.semaphore_wait(barrier, ne - 1)

    codes = dc_ref[...].astype(F32).T.astype(jnp.int32)

    for j in range(nch):
        ri = lax.broadcasted_iota(jnp.int32, (rows, t), 0) + j * rows
        sel = jnp.where(ri == codes[0:1, :], 1.0, 0.0) + jnp.where(ri == codes[1:2, :], 1.0, 0.0)
        sel = sel.astype(BF)

        def pick(i, _):
            cols = pl.ds(pl.multiple_of(i * 512, 512), 512)
            send[j, :, cols] = dot(sel, h_ref[:, cols]).astype(BF)
            return 0

        lax.fori_loop(0, hd // 512, pick, 0)
        for dc, dt in peers:
            out_copy(j, dc, dt).start()
        recv[j, blk(me), :] = send[j, blk(me), :]

    for j in range(nch):
        for dc, dt in peers:
            in_copy(j, dc, dt).wait_recv()

        def up(s, _):
            slot = lax.rem(s, r1)
            for cp_ in w1_copies(s):
                cp_.wait()
            xx = recv[j]
            gg = dot(xx, w1buf[slot, 0])
            uu = dot(xx, w1buf[slot, 1])
            act[:, pl.ds(pl.multiple_of(s * f1, f1), f1)] = (gg * jax.nn.sigmoid(gg) * uu).astype(BF)

            @pl.when(s + r1 < n1)
            def _():
                start_w1(s + r1)
            return 0

        lax.fori_loop(0, n1, up, 0)
        if j + 1 < nch:
            prefetch_w1()

        def down(s, _):
            slot = lax.rem(s, r2)
            w2_copy(s).wait()
            zbuf[j, :, pl.ds(pl.multiple_of(s * f2, f2), f2)] = dot(act[...], w2buf[slot]).astype(BF)

            @pl.when(s + r2 < n2)
            def _():
                w2_copy(s + r2).start()
            return 0

        lax.fori_loop(0, n2, down, 0)
        if j + 1 < nch:
            prefetch_w2()
        for dc, dt in peers:
            home_copy(j, dc, dt).start()
        back[j, blk(me), :] = zbuf[j, blk(me), :]

    for j in range(nch):
        for dc, dt in peers:
            got_copy(j, dc, dt).wait_recv()

    ci = lax.broadcasted_iota(jnp.int32, (t, rows), 1)
    sel0 = [jnp.where(ci + j * rows == dc_ref[:, 0:1], 1.0, 0.0).astype(BF) for j in range(nch)]
    sel1 = [jnp.where(ci + j * rows == dc_ref[:, 1:2], 1.0, 0.0).astype(BF) for j in range(nch)]
    g0 = g_ref[:, 0:1]
    g1 = g_ref[:, 1:2]

    def combine(i, _):
        cols = pl.ds(pl.multiple_of(i * 512, 512), 512)
        z0 = sum(dot(sel0[j], back[j, :, cols]) for j in range(nch))
        z1 = sum(dot(sel1[j], back[j, :, cols]) for j in range(nch))
        y_ref[:, cols] = (h_ref[:, cols].astype(F32) + (g0 * z0 + g1 * z1)).astype(BF)
        return 0

    lax.fori_loop(0, hd // 512, combine, 0)

    for j in range(nch):
        for dc, dt in peers:
            out_copy(j, dc, dt).wait_send()
            home_copy(j, dc, dt).wait_send()


def moe(h, code, gates, wg, wu, wd, *, ncp, ntp, nch, cid):
    t, hd = h.shape
    ff = wg.shape[1]
    ne = ncp * ntp
    rows = ne * CH
    f1, f2, r1, r2 = 256, 512, 2, 2
    vm = pl.BlockSpec(memory_space=pltpu.VMEM)
    hbm = pl.BlockSpec(memory_space=pl.ANY)
    dma = pltpu.SemaphoreType.DMA
    return pl.pallas_call(
        functools.partial(moe_kernel, ncp=ncp, ntp=ntp, nch=nch, f1=f1, f2=f2),
        in_specs=[vm, vm, vm, hbm, hbm, hbm],
        out_specs=vm,
        out_shape=jax.ShapeDtypeStruct((t, hd), BF),
        scratch_shapes=[
            pltpu.VMEM((nch, rows, hd), BF), pltpu.VMEM((nch, rows, hd), BF),
            pltpu.VMEM((nch, rows, hd), BF), pltpu.VMEM((nch, rows, hd), BF),
            pltpu.VMEM((rows, ff), BF),
            pltpu.VMEM((r1, 2, hd, f1), BF), pltpu.VMEM((r2, ff, f2), BF),
            dma((nch, ne)), dma((nch, ne)), dma((nch, ne)), dma((nch, ne)),
            dma((r1, 2)), dma((r2,)),
        ],
        compiler_params=pltpu.CompilerParams(collective_id=cid, has_side_effects=True, vmem_limit_bytes=VMEM_LIMIT),
        name=f"moe{nch}",
        cost_estimate=pl.CostEstimate(flops=6 * nch * rows * hd * ff, bytes_accessed=6 * nch * hd * ff, transcendentals=0),
    )(h, code, gates, wg, wu, wd)


def solution(mesh):
    ncp = mesh.shape["cp"]
    ntp = mesh.shape["tp"]
    rows_spec = P(("dp", "cp", "tp"), None)
    exp_spec = P(("cp", "tp"), None, None)

    def local(x, idx, gates, wq, wk, wv, wo, w1g, w1u, w2):
        y, h, code, most = layer(x, wq, wk, wv, wo, idx, gates, w1g[0], w1u[0], w2[0], nd=mesh.shape["dp"], ncp=ncp, ntp=ntp, cid=3)

        def few(args):
            return y

        def many(args):
            return moe(*args, ncp=ncp, ntp=ntp, nch=4, cid=2)

        return lax.cond(most[0, 0] <= NCH * CH, few, many, (h, code, gates, w1g[0], w1u[0], w2[0]))

    return jax.shard_map(local, mesh=mesh, in_specs=(rows_spec, rows_spec, rows_spec, P(None, "tp"), P(None, "tp"), P(None, "tp"), P("tp", None), exp_spec, exp_spec, exp_spec), out_specs=rows_spec, check_vma=False)
```
